32 devices in a mesh: dp: 4 (over y, z), dcp: 8 (over x, core).
Axes of the slice: x: 4, y: 2, z: 2, core: 2. Of those that a mesh axis runs over, the one named last changes fastest.
The devices are a block of a 4x4x8 slice.
Arguments:
- q_abs: bfloat16 [128, 2, 64, 576], P('dp', None, 'dcp'), parts along dimension 0
- kv_cache: bfloat16 [128, 16, 8, 64, 576], P('dp', None, 'dcp'), parts along dimension 0
- lengths: int32 [128], P('dp'), parts along dimension 0
Outputs:
- output: bfloat16 [128, 2, 64, 512], P('dp', None, 'dcp'), parts along dimension 0
There are 4 independent parts. The reference program is written for one: setup_inputs(seed, part) draws one part's arguments, and reference() takes and returns one part's arrays. A program takes and returns all parts, laid end to end along the dimension named above; each array names one.
All inputs are finite; a program needn't handle non-finite values.
Results may differ from the reference program's by a relative error of at most 0.00757035.
Values are sent between devices in bfloat16 or wider.
A program may use at most 768 MiB of HBM per device.

```python
import math
import jax
import jax.numpy as jnp
from jax import lax

BATCH = 32
MTP = 2
HEADS = 64
LATENT = 512
ROPE = 64
NOPE = 128
ROUNDS = 16
GROUP = 8
PAGE = 64

SEQ = ROUNDS * GROUP * PAGE
WIDTH = LATENT + ROPE


def setup_inputs(seed: int = 0, part: int = 0) -> dict:
    base_key = jax.random.fold_in(jax.random.key(seed), part)
    key_qlat, key_qrope, key_cache, key_len, key_pick = jax.random.split(base_key, 5)
    lat_scale = math.sqrt(SEQ / 256.0)
    q_lat = jax.random.normal(key_qlat, (BATCH, MTP, HEADS, LATENT), jnp.float32) * (math.sqrt(1.8 * (NOPE + ROPE) / LATENT) / lat_scale)
    q_rope = jax.random.normal(key_qrope, (BATCH, MTP, HEADS, ROPE), jnp.float32) * math.sqrt(1.8 * (NOPE + ROPE) / ROPE)
    q_abs = jnp.concatenate([q_lat, q_rope], axis=-1).astype(jnp.bfloat16)
    col_scale = jnp.where(jnp.arange(WIDTH) < LATENT, lat_scale, 1.0)
    kv_cache = (jax.random.normal(key_cache, (BATCH, ROUNDS, GROUP, PAGE, WIDTH), jnp.float32) * col_scale).astype(jnp.bfloat16)
    lengths = jax.random.randint(key_len, (BATCH,), SEQ // 2, SEQ + 1, dtype=jnp.int32)
    longest = jax.random.randint(key_pick, (), 0, BATCH, dtype=jnp.int32)
    lengths = jnp.where(jnp.arange(BATCH) == longest, SEQ, lengths).astype(jnp.int32)
    return {'q_abs': q_abs, 'kv_cache': kv_cache, 'lengths': lengths}


def reference(q_abs, kv_cache, lengths):
    keys_all = kv_cache.reshape(BATCH, SEQ, WIDTH)
    score_scale = (NOPE + ROPE) ** -0.5
    positions = jnp.arange(SEQ)
    offsets = jnp.arange(MTP) - MTP

    def one_seq(seq_args):
        q_seq, key_seq, length = seq_args
        key_f = key_seq.astype(jnp.float32)
        scores = jnp.einsum('thd,sd->ths', q_seq.astype(jnp.float32), key_f) * score_scale
        last_pos = length + offsets
        visible = positions[None, :] <= last_pos[:, None]
        scores = jnp.where(visible[:, None, :], scores, -jnp.inf)
        weights = jax.nn.softmax(scores, axis=-1)
        out_seq = jnp.einsum('ths,sc->thc', weights, key_f[:, :LATENT])
        return out_seq.astype(jnp.bfloat16)

    return lax.map(one_seq, (q_abs, keys_all, lengths))
```

```python
import functools
import math

import jax
import jax.numpy as jnp
from jax import lax
from jax.experimental import pallas as pl
from jax.experimental.pallas import tpu as pltpu
from jax.sharding import PartitionSpec as P

LATENT = 512
ROPE = 64
NOPE = 128
PAGE = 64
CORES = 2
CHUNK = 4
KV_SLOTS = 4
AHEAD = 3
LANES = 128


def wide(col, n):
    return jnp.concatenate([col] * (n // LANES), axis=1)


def merge(o_a, l_a, o_b, l_b):
    top = jnp.maximum(l_a, l_b)
    e_a = jnp.exp(l_a - top)
    e_b = jnp.exp(l_b - top)
    total = e_a + e_b
    inv = 1.0 / total
    n = o_a.shape[1]
    return o_a * wide(e_a * inv, n) + o_b * wide(e_b * inv, n), top + jnp.log(total)


def kernel(group, rounds, min_rounds, len_ref, q_hbm, kv_hbm, out_ref, q_all, kv_buf, rank, own_o, own_l, sib_o, sib_l,
           got_o, got_l, chip_o, chip_l, hop_o, hop_l, mid_o, mid_l, fin_o, fin_l,
           load_sem, kv_sem, q_send, q_recv, qs_send, qs_recv, s_send, s_recv, h_send, h_recv, f_send, f_recv):
    chunks, _, per, rows, width = q_all.shape
    half = per // 2
    keys = kv_buf.shape[2]
    chips = group // CORES
    side = chips * rows
    me = lax.axis_index('dcp')
    chip, core = me // CORES, me % CORES
    right = lax.rem(chip + 1, chips) * CORES + core
    left = lax.rem(chip + chips - 1, chips) * CORES + core
    twin = chip * CORES + (CORES - 1 - core)
    scale = (NOPE + ROPE) ** -0.5

    def remote(src, dst, send, recv, to):
        return pltpu.make_async_remote_copy(src_ref=src, dst_ref=dst, send_sem=send, recv_sem=recv,
                                            device_id={'dcp': to}, device_id_type=pl.DeviceIdType.MESH)

    def q_copy(c, kind):
        if kind == 0:
            src, dst, to = q_all.at[c, 0], q_all.at[c, 1], right
        elif kind == 1:
            src, dst, to = q_all.at[c, 0], q_all.at[c, 2], left
        elif kind == 2:
            src, dst, to = q_all.at[c, 1, pl.ds(0, half)], q_all.at[c, 3, pl.ds(0, half)], right
        else:
            src, dst, to = q_all.at[c, 2, pl.ds(half, half)], q_all.at[c, 3, pl.ds(half, half)], left
        return remote(src, dst, q_send.at[c, kind], q_recv.at[c, kind], to)

    def q_twin(c):
        return remote(q_all.at[c, pl.ds(0, chips)], q_all.at[c, pl.ds(chips, chips)], qs_send.at[c], qs_recv.at[c], twin)

    def part_twin(c, what):
        src, dst = ((sib_o, got_o), (sib_l, got_l))[what]
        return remote(src.at[c], dst.at[c], s_send.at[c, what], s_recv.at[c, what], twin)

    def hop_copy(c, h, what):
        src = (chip_o.at[c, h, 3], chip_l.at[c, h])[what]
        dst = (hop_o.at[c, h], hop_l.at[c, h])[what]
        return remote(src, dst, h_send.at[c, h, what], h_recv.at[c, h, what], (right, left)[h])

    def fin_copy(c, s, h, what):
        if s == h:
            src = (mid_o.at[c, h], mid_l.at[c, h])[what]
        else:
            src = (chip_o.at[c, h, 2 - s], chip_l.at[c, h])[what]
        dst = (fin_o.at[c, s, h], fin_l.at[c, s, h])[what]
        return remote(src, dst, f_send.at[c, s, h, what], f_recv.at[c, s, h, what], (right, left)[s])

    def kv_copy(c, b):
        slot = lax.rem(c, KV_SLOTS)
        return pltpu.make_async_copy(kv_hbm.at[c * per + b], kv_buf.at[slot, b], kv_sem.at[slot, b])

    load = pltpu.make_async_copy(q_hbm, q_all.at[:, 0], load_sem)
    load.start()
    for c in range(min(KV_SLOTS, chunks)):
        for b in range(per):
            kv_copy(c, b).start()

    barrier = pltpu.get_barrier_semaphore()
    for peer in (left, right, twin):
        pl.semaphore_signal(barrier, inc=1, device_id={'dcp': peer}, device_id_type=pl.DeviceIdType.MESH)

    r_id = lax.broadcasted_iota(jnp.int32, (rows, keys), 0)
    k_id = lax.broadcasted_iota(jnp.int32, (rows, keys), 1)
    tokens = 2
    rank[...] = (k_id // PAGE * group + me) * PAGE + k_id % PAGE - r_id // (rows // tokens)

    load.wait()
    pl.semaphore_wait(barrier, 3)
    for c in range(min(AHEAD, chunks)):
        for kind in (0, 1):
            q_copy(c, kind).start()

    free_keys = (min_rounds * PAGE) // LANES * LANES

    def attend(c):
        slot = lax.rem(c, KV_SLOTS)
        for b in range(per):
            kv_copy(c, b).wait()
        for b in range(per):
            q = q_all[c, :, b].reshape(group * rows, width)
            kv = kv_buf.at[slot, b]
            s = lax.dot_general(q, kv[...], (((1,), (1,)), ((), ())), preferred_element_type=jnp.float32)
            tail = s[:, free_keys:].reshape(group, rows, keys - free_keys)
            limit = len_ref[c * per + b] - tokens
            seen = jnp.broadcast_to(rank[:, free_keys:][None], tail.shape) <= limit
            tail = jnp.where(seen, tail, -jnp.inf).reshape(group * rows, keys - free_keys)
            s = jnp.concatenate([s[:, :free_keys], tail], axis=1)
            top = jnp.max(s, axis=1, keepdims=True)
            p = jnp.exp2((s - top) * (scale * math.log2(math.e)))
            total = jnp.sum(p, axis=1, keepdims=True)
            o = jnp.dot(p.astype(jnp.bfloat16), kv[:, :LATENT], preferred_element_type=jnp.float32)
            o = o * (1.0 / total)
            lse = jnp.broadcast_to(top * scale + jnp.log(total), (group * rows, LANES))
            own_o[b] = o[:side]
            own_l[b] = lse[:side]
            sib_o[c, b] = o[side:].astype(jnp.bfloat16)
            sib_l[c, b] = lse[side:]

    lane_s = lax.broadcasted_iota(jnp.int32, (side, LANES), 1)
    row_s = lax.broadcasted_iota(jnp.int32, (side, LANES), 0)
    block = half * rows
    lane_b = lax.broadcasted_iota(jnp.int32, (block, LANES), 1)
    row_b = lax.broadcasted_iota(jnp.int32, (block, LANES), 0)

    def column(row, slot):
        picked = jnp.where(lane_b == row_b + slot * block, jnp.broadcast_to(row, (block, LANES)), 0.0)
        return jnp.broadcast_to(jnp.sum(picked, axis=1, keepdims=True), (block, LANES))

    def join_cores(c):
        for h in range(2):
            packed = jnp.zeros((1, LANES), jnp.float32)
            for n in range(half):
                b = h * half + n
                o, lse = merge(own_o[b], own_l[b], got_o[c, b].astype(jnp.float32), got_l[c, b])
                o = o.astype(jnp.bfloat16)
                for slot in range(chips):
                    chip_o[c, h, slot, n * rows:(n + 1) * rows] = o[slot * rows:(slot + 1) * rows]
                at = row_s // rows * block + n * rows + row_s % rows
                packed = packed + jnp.sum(jnp.where(lane_s == at, lse, 0.0), axis=0, keepdims=True)
            chip_l[c, h] = packed

    def join_hop(c):
        for h in range(2):
            slot = 2 - h
            row = chip_l[c, h]
            o, lse = merge(chip_o[c, h, slot].astype(jnp.float32), column(row, slot),
                           hop_o[c, h].astype(jnp.float32), column(hop_l[c, h], 3))
            mid_o[c, h] = o.astype(jnp.bfloat16)
            mid_l[c, h] = jnp.sum(jnp.where(lane_b == row_b + slot * block, lse, 0.0), axis=0, keepdims=True)

    def join_last(c):
        for h in range(2):
            parts = [(chip_o[c, h, 0], column(chip_l[c, h], 0))]
            for s in range(2):
                parts.append((fin_o[c, s, h], column(fin_l[c, s, h], 2 - s)))
            top = functools.reduce(jnp.maximum, [l for _, l in parts])
            weights = [jnp.exp(l - top) for _, l in parts]
            inv = 1.0 / functools.reduce(jnp.add, weights)
            o = functools.reduce(jnp.add, [part.astype(jnp.float32) * wide(w * inv, LATENT) for (part, _), w in zip(parts, weights)])
            o = o.astype(jnp.bfloat16)
            for n in range(half):
                out_ref[c * per + h * half + n] = o[n * rows:(n + 1) * rows]

    def stage(t, lag, fn):
        c = t - lag

        @pl.when(jnp.logical_and(c >= 0, c < chunks))
        def _():
            fn(c)

    def spread(c):
        for kind in (0, 1):
            q_copy(c, kind).wait_recv()
        for kind in (2, 3):
            q_copy(c, kind).start()

    def to_twin(c):
        for kind in (2, 3):
            q_copy(c, kind).wait_recv()
        q_twin(c).start()

    def send_own(c):
        for kind in (0, 1):
            q_copy(c, kind).start()

    def cores(c):
        for what in range(2):
            part_twin(c, what).wait_recv()
        join_cores(c)
        for what in range(2):
            for h in range(2):
                hop_copy(c, h, what).start()
            for s in range(2):
                fin_copy(c, s, 1 - s, what).start()

    def hop(c):
        for what in range(2):
            for h in range(2):
                hop_copy(c, h, what).wait_recv()
        join_hop(c)
        for what in range(2):
            for s in range(2):
                fin_copy(c, s, s, what).start()

    def last(c):
        for what in range(2):
            for s in range(2):
                for h in range(2):
                    fin_copy(c, s, h, what).wait_recv()
        join_last(c)

    def work(c):
        q_twin(c).wait_recv()
        attend(c)
        for what in range(2):
            part_twin(c, what).start()

        @pl.when(c + KV_SLOTS < chunks)
        def _():
            for b in range(per):
                kv_copy(c + KV_SLOTS, b).start()

    def step(t, carry):
        stage(t, -AHEAD, send_own)
        stage(t, 0, spread)
        stage(t, 1, to_twin)
        stage(t, 3, cores)
        stage(t, 4, hop)
        stage(t, 5, last)
        stage(t, 2, work)
        return carry

    lax.fori_loop(0, chunks + 5, step, 0)

    def drain(c, carry):
        for kind in range(4):
            q_copy(c, kind).wait_send()
        q_twin(c).wait_send()
        for what in range(2):
            part_twin(c, what).wait_send()
            for h in range(2):
                hop_copy(c, h, what).wait_send()
                for s in range(2):
                    fin_copy(c, s, h, what).wait_send()
        return carry

    lax.fori_loop(0, chunks, drain, 0)


def solution(mesh):
    group = mesh.shape['dcp']
    chips = group // CORES

    def local_step(q_blk, kv_blk, len_blk):
        batch, tokens, heads, width = q_blk.shape
        rounds = kv_blk.shape[1]
        keys = rounds * PAGE
        rows = tokens * heads
        chunks = batch // CHUNK
        half = CHUNK // 2
        block = half * rows
        side = chips * rows
        bf, f32 = jnp.bfloat16, jnp.float32
        scratch = [
            pltpu.VMEM((chunks, group, CHUNK, rows, width), bf),
            pltpu.VMEM((KV_SLOTS, CHUNK, keys, width), bf),
            pltpu.VMEM((rows, keys), jnp.int32),
            pltpu.VMEM((CHUNK, side, LATENT), f32),
            pltpu.VMEM((CHUNK, side, LANES), f32),
            pltpu.VMEM((chunks, CHUNK, side, LATENT), bf),
            pltpu.VMEM((chunks, CHUNK, side, LANES), f32),
            pltpu.VMEM((chunks, CHUNK, side, LATENT), bf),
            pltpu.VMEM((chunks, CHUNK, side, LANES), f32),
            pltpu.VMEM((chunks, 2, chips, block, LATENT), bf),
            pltpu.VMEM((chunks, 2, 1, LANES), f32),
            pltpu.VMEM((chunks, 2, block, LATENT), bf),
            pltpu.VMEM((chunks, 2, 1, LANES), f32),
            pltpu.VMEM((chunks, 2, block, LATENT), bf),
            pltpu.VMEM((chunks, 2, 1, LANES), f32),
            pltpu.VMEM((chunks, 2, 2, block, LATENT), bf),
            pltpu.VMEM((chunks, 2, 2, 1, LANES), f32),
            pltpu.SemaphoreType.DMA,
            pltpu.SemaphoreType.DMA((KV_SLOTS, CHUNK)),
        ]
        for shape in ((chunks, 4), (chunks,), (chunks, 2), (chunks, 2, 2), (chunks, 2, 2, 2)):
            scratch += [pltpu.SemaphoreType.DMA(shape)] * 2
        flops = 2 * batch * group * rows * keys * (width + LATENT)
        o = pl.pallas_call(
            functools.partial(kernel, group, rounds, rounds // 2 - 1),
            out_shape=jax.ShapeDtypeStruct((batch, rows, LATENT), bf),
            in_specs=[pl.BlockSpec(memory_space=pltpu.SMEM), pl.BlockSpec(memory_space=pl.ANY), pl.BlockSpec(memory_space=pl.ANY)],
            out_specs=pl.BlockSpec(memory_space=pltpu.VMEM),
            scratch_shapes=scratch,
            compiler_params=pltpu.CompilerParams(collective_id=0, has_side_effects=True, vmem_limit_bytes=62 * 2**20),
            cost_estimate=pl.CostEstimate(flops=flops, bytes_accessed=kv_blk.size * 2, transcendentals=batch * group * rows * keys),
        )(len_blk, q_blk.reshape(chunks, CHUNK, rows, width), kv_blk.reshape(batch, keys, width))
        return o.reshape(batch, tokens, heads, LATENT)

    return jax.shard_map(local_step, mesh=mesh, in_specs=(P('dp', None, 'dcp', None), P('dp', None, 'dcp', None, None), P('dp')), out_specs=P('dp', None, 'dcp', None), check_vma=False)
```

```python
import functools
import math

import jax
import jax.numpy as jnp
from jax import lax
from jax.experimental import pallas as pl
from jax.experimental.pallas import tpu as pltpu
from jax.sharding import PartitionSpec as P

LATENT = 512
ROPE = 64
NOPE = 128
PAGE = 64
CORES = 2
CHUNK = 2
KV_SLOTS = 8
AHEAD = 4
LAG = 2
KEPT = LAG
LANES = 128


def wide(col, n):
    return jnp.concatenate([col] * (n // LANES), axis=1)


def merge(o_a, l_a, o_b, l_b):
    top = jnp.maximum(l_a, l_b)
    e_a = jnp.exp(l_a - top)
    e_b = jnp.exp(l_b - top)
    total = e_a + e_b
    inv = 1.0 / total
    n = o_a.shape[1]
    return o_a * wide(e_a * inv, n) + o_b * wide(e_b * inv, n), top + jnp.log(total)


def kernel(group, min_rounds, len_ref, q_hbm, kv_hbm, out_ref, q_all, kv_buf, rank, own_o, own_l, sib_o, sib_l,
           got_o, got_l, chip_o, chip_l, hop_o, hop_l, mid_o, mid_l, fin_o, fin_l,
           load_sem, kv_sem, q_send, q_recv, s_send, s_recv, h_send, h_recv, f_send, f_recv):
    chunks, _, per, rows, width = q_all.shape
    keys = kv_buf.shape[2]
    chips = group // CORES
    side = chips * rows
    block = per * rows
    me = lax.axis_index('dcp')
    chip, core = me // CORES, me % CORES
    right = lax.rem(chip + 1, chips) * CORES + core
    left = lax.rem(chip + chips - 1, chips) * CORES + core
    twin = chip * CORES + (CORES - 1 - core)
    scale = (NOPE + ROPE) ** -0.5

    def remote(src, dst, send, recv, to):
        return pltpu.make_async_remote_copy(src_ref=src, dst_ref=dst, send_sem=send, recv_sem=recv,
                                            device_id={'dcp': to}, device_id_type=pl.DeviceIdType.MESH)

    def way(c):
        return lax.rem(c, 2)

    def toward(d):
        return jnp.where(d == 0, right, left)

    def q_copy(c, kind):
        if kind == 0:
            src, dst, to = q_all.at[c, 0], q_all.at[c, 1], right
        elif kind == 1:
            src, dst, to = q_all.at[c, 0], q_all.at[c, 2], left
        elif kind == 2:
            src, dst, to = q_all.at[c, 1 + way(c)], q_all.at[c, 3], toward(way(c))
        else:
            src, dst, to = q_all.at[c, pl.ds(0, chips)], q_all.at[c, pl.ds(chips, chips)], twin
        return remote(src, dst, q_send.at[c, kind], q_recv.at[c, kind], to)

    def part_twin(c, what):
        src, dst = ((sib_o, got_o), (sib_l, got_l))[what]
        return remote(src.at[c], dst.at[c], s_send.at[c, what], s_recv.at[c, what], twin)

    def hop_copy(c, what):
        src = (chip_o.at[c, 3], chip_l.at[c])[what]
        dst = (hop_o.at[c], hop_l.at[c])[what]
        return remote(src, dst, h_send.at[c, what], h_recv.at[c, what], toward(way(c)))

    def fin_copy(c, kind, what):
        if kind == 0:
            src, to = (mid_o.at[c], mid_l.at[c])[what], toward(way(c))
        else:
            src, to = (chip_o.at[c, 1 + way(c)], chip_l.at[c])[what], toward(1 - way(c))
        dst = (fin_o.at[c, kind], fin_l.at[c, kind])[what]
        return remote(src, dst, f_send.at[c, kind, what], f_recv.at[c, kind, what], to)

    def kv_copy(c, b):
        slot = lax.rem(c, KV_SLOTS)
        return pltpu.make_async_copy(kv_hbm.at[c * per + b], kv_buf.at[slot, b], kv_sem.at[slot, b])

    load = pltpu.make_async_copy(q_hbm, q_all.at[:, 0], load_sem)
    load.start()
    for c in range(min(KV_SLOTS, chunks)):
        for b in range(per):
            kv_copy(c, b).start()

    barrier = pltpu.get_barrier_semaphore()
    for peer in (left, right, twin):
        pl.semaphore_signal(barrier, inc=1, device_id={'dcp': peer}, device_id_type=pl.DeviceIdType.MESH)

    r_id = lax.broadcasted_iota(jnp.int32, (rows, keys), 0)
    k_id = lax.broadcasted_iota(jnp.int32, (rows, keys), 1)
    tokens = 2
    rank[...] = (k_id // PAGE * group + me) * PAGE + k_id % PAGE - r_id // (rows // tokens)

    load.wait()
    pl.semaphore_wait(barrier, 3)
    for c in range(min(AHEAD, chunks)):
        for kind in (0, 1):
            q_copy(c, kind).start()

    free_keys = (min_rounds * PAGE) // LANES * LANES

    def attend(c):
        slot = lax.rem(c, KV_SLOTS)
        for b in range(per):
            kv_copy(c, b).wait()
        for b in range(per):
            q = q_all[c, :, b].reshape(group * rows, width)
            kv = kv_buf.at[slot, b]
            s = lax.dot_general(q, kv[...], (((1,), (1,)), ((), ())), preferred_element_type=jnp.float32)
            tail = s[:, free_keys:].reshape(group, rows, keys - free_keys)
            limit = len_ref[c * per + b] - tokens
            seen = jnp.broadcast_to(rank[:, free_keys:][None], tail.shape) <= limit
            tail = jnp.where(seen, tail, -jnp.inf).reshape(group * rows, keys - free_keys)
            s = jnp.concatenate([s[:, :free_keys], tail], axis=1)
            top = jnp.max(s, axis=1, keepdims=True)
            p = jnp.exp2((s - top) * (scale * math.log2(math.e)))
            total = jnp.sum(p, axis=1, keepdims=True)
            o = jnp.dot(p.astype(jnp.bfloat16), kv[:, :LATENT], preferred_element_type=jnp.float32)
            o = o * (1.0 / total)
            lse = jnp.broadcast_to(top * scale + jnp.log(total), (group * rows, LANES))
            keep = lax.rem(c, KEPT)
            own_o[keep, b] = o[:side]
            own_l[keep, b] = lse[:side]
            sib_o[c, b] = o[side:].astype(jnp.bfloat16)
            sib_l[c, b] = lse[side:]

    lane_s = lax.broadcasted_iota(jnp.int32, (side, LANES), 1)
    row_s = lax.broadcasted_iota(jnp.int32, (side, LANES), 0)
    lane_b = lax.broadcasted_iota(jnp.int32, (block, LANES), 1)
    row_b = lax.broadcasted_iota(jnp.int32, (block, LANES), 0)

    def column(row, slot):
        picked = jnp.where(lane_b == row_b + slot * block, jnp.broadcast_to(row, (block, LANES)), 0.0)
        return jnp.broadcast_to(jnp.sum(picked, axis=1, keepdims=True), (block, LANES))

    def join_cores(c):
        packed = jnp.zeros((1, LANES), jnp.float32)
        keep = lax.rem(c, KEPT)
        for b in range(per):
            o, lse = merge(own_o[keep, b], own_l[keep, b], got_o[c, b].astype(jnp.float32), got_l[c, b])
            o = o.astype(jnp.bfloat16)
            for slot in range(chips):
                chip_o[c, slot, b * rows:(b + 1) * rows] = o[slot * rows:(slot + 1) * rows]
            at = row_s // rows * block + b * rows + row_s % rows
            packed = packed + jnp.sum(jnp.where(lane_s == at, lse, 0.0), axis=0, keepdims=True)
        chip_l[c] = packed

    def join_hop(c):
        slot = 2 - way(c)
        o, lse = merge(chip_o[c, slot].astype(jnp.float32), column(chip_l[c], slot), hop_o[c].astype(jnp.float32), column(hop_l[c], 3))
        mid_o[c] = o.astype(jnp.bfloat16)
        mid_l[c] = jnp.sum(jnp.where(lane_b == row_b, lse, 0.0), axis=0, keepdims=True)

    def join_last(c):
        parts = [(chip_o[c, 0], column(chip_l[c], 0)), (fin_o[c, 0], column(fin_l[c, 0], 0)),
                 (fin_o[c, 1], column(fin_l[c, 1], 1 + way(c)))]
        top = functools.reduce(jnp.maximum, [l for _, l in parts])
        weights = [jnp.exp(l - top) for _, l in parts]
        inv = 1.0 / functools.reduce(jnp.add, weights)
        o = functools.reduce(jnp.add, [part.astype(jnp.float32) * wide(w * inv, LATENT) for (part, _), w in zip(parts, weights)])
        o = o.astype(jnp.bfloat16)
        for b in range(per):
            out_ref[c * per + b] = o[b * rows:(b + 1) * rows]

    def stage(t, lag, fn):
        c = t - lag

        @pl.when(jnp.logical_and(c >= 0, c < chunks))
        def _():
            fn(c)

    def send_own(c):
        for kind in (0, 1):
            q_copy(c, kind).start()

    def spread(c):
        for kind in (0, 1):
            q_copy(c, kind).wait_recv()
        q_copy(c, 2).start()

    def to_twin(c):
        q_copy(c, 2).wait_recv()
        q_copy(c, 3).start()

    def work(c):
        q_copy(c, 3).wait_recv()
        attend(c)
        for what in range(2):
            part_twin(c, what).start()

        @pl.when(c + KV_SLOTS < chunks)
        def _():
            for b in range(per):
                kv_copy(c + KV_SLOTS, b).start()

    def cores(c):
        for what in range(2):
            part_twin(c, what).wait_recv()
        join_cores(c)
        for what in range(2):
            hop_copy(c, what).start()
            fin_copy(c, 1, what).start()

    def hop(c):
        for what in range(2):
            hop_copy(c, what).wait_recv()
        join_hop(c)
        for what in range(2):
            fin_copy(c, 0, what).start()

    def last(c):
        for what in range(2):
            for kind in range(2):
                fin_copy(c, kind, what).wait_recv()
        join_last(c)

    def sent(c):
        for kind in range(4):
            q_copy(c, kind).wait_send()
        for what in range(2):
            part_twin(c, what).wait_send()
            hop_copy(c, what).wait_send()
            for kind in range(2):
                fin_copy(c, kind, what).wait_send()

    def step(t, carry):
        stage(t, -AHEAD, send_own)
        stage(t, 0, spread)
        stage(t, LAG, to_twin)
        stage(t, 3 * LAG, cores)
        stage(t, 4 * LAG, hop)
        stage(t, 5 * LAG, last)
        stage(t, 5 * LAG + 1, sent)
        stage(t, 2 * LAG, work)
        return carry

    lax.fori_loop(0, chunks + 5 * LAG + 1, step, 0)


def solution(mesh):
    group = mesh.shape['dcp']
    chips = group // CORES

    def local_step(q_blk, kv_blk, len_blk):
        batch, tokens, heads, width = q_blk.shape
        rounds = kv_blk.shape[1]
        keys = rounds * PAGE
        rows = tokens * heads
        chunks = batch // CHUNK
        block = CHUNK * rows
        side = chips * rows
        bf, f32 = jnp.bfloat16, jnp.float32
        scratch = [
            pltpu.VMEM((chunks, group, CHUNK, rows, width), bf),
            pltpu.VMEM((KV_SLOTS, CHUNK, keys, width), bf),
            pltpu.VMEM((rows, keys), jnp.int32),
            pltpu.VMEM((KEPT, CHUNK, side, LATENT), f32),
            pltpu.VMEM((KEPT, CHUNK, side, LANES), f32),
            pltpu.VMEM((chunks, CHUNK, side, LATENT), bf),
            pltpu.VMEM((chunks, CHUNK, side, LANES), f32),
            pltpu.VMEM((chunks, CHUNK, side, LATENT), bf),
            pltpu.VMEM((chunks, CHUNK, side, LANES), f32),
            pltpu.VMEM((chunks, chips, block, LATENT), bf),
            pltpu.VMEM((chunks, 1, LANES), f32),
            pltpu.VMEM((chunks, block, LATENT), bf),
            pltpu.VMEM((chunks, 1, LANES), f32),
            pltpu.VMEM((chunks, block, LATENT), bf),
            pltpu.VMEM((chunks, 1, LANES), f32),
            pltpu.VMEM((chunks, 2, block, LATENT), bf),
            pltpu.VMEM((chunks, 2, 1, LANES), f32),
            pltpu.SemaphoreType.DMA,
            pltpu.SemaphoreType.DMA((KV_SLOTS, CHUNK)),
        ]
        for shape in ((chunks, 4), (chunks, 2), (chunks, 2), (chunks, 2, 2)):
            scratch += [pltpu.SemaphoreType.DMA(shape)] * 2
        flops = 2 * batch * group * rows * keys * (width + LATENT)
        o = pl.pallas_call(
            functools.partial(kernel, group, rounds // 2 - 1),
            out_shape=jax.ShapeDtypeStruct((batch, rows, LATENT), bf),
            in_specs=[pl.BlockSpec(memory_space=pltpu.SMEM), pl.BlockSpec(memory_space=pl.ANY), pl.BlockSpec(memory_space=pl.ANY)],
            out_specs=pl.BlockSpec(memory_space=pltpu.VMEM),
            scratch_shapes=scratch,
            compiler_params=pltpu.CompilerParams(collective_id=0, has_side_effects=True, vmem_limit_bytes=62 * 2**20),
            cost_estimate=pl.CostEstimate(flops=flops, bytes_accessed=kv_blk.size * 2, transcendentals=batch * group * rows * keys),
        )(len_blk, q_blk.reshape(chunks, CHUNK, rows, width), kv_blk.reshape(batch, keys, width))
        return o.reshape(batch, tokens, heads, LATENT)

    return jax.shard_map(local_step, mesh=mesh, in_specs=(P('dp', None, 'dcp', None), P('dp', None, 'dcp', None, None), P('dp')), out_specs=P('dp', None, 'dcp', None), check_vma=False)
```

```python
import functools
import math

import jax
import jax.numpy as jnp
from jax import lax
from jax.experimental import pallas as pl
from jax.experimental.pallas import tpu as pltpu
from jax.sharding import PartitionSpec as P

LATENT = 512
ROPE = 64
NOPE = 128
PAGE = 64
CORES = 2
CHUNK = 2
KV_SLOTS = 8
AHEAD = 6
LAG = 3
KEPT = LAG
LANES = 128


def wide(col, n):
    return jnp.concatenate([col] * (n // LANES), axis=1)


def merge(o_a, l_a, o_b, l_b):
    top = jnp.maximum(l_a, l_b)
    e_a = jnp.exp(l_a - top)
    e_b = jnp.exp(l_b - top)
    total = e_a + e_b
    inv = 1.0 / total
    n = o_a.shape[1]
    return o_a * wide(e_a * inv, n) + o_b * wide(e_b * inv, n), top + jnp.log(total)


def kernel(group, min_rounds, len_ref, q_hbm, kv_hbm, out_ref, q_all, kv_buf, rank, own_o, own_l, sib_o, sib_l,
           got_o, got_l, chip_o, chip_l, hop_o, hop_l, mid_o, mid_l, fin_o, fin_l,
           load_sem, kv_sem, q_send, q_recv, s_send, s_recv, h_send, h_recv, f_send, f_recv):
    chunks, _, per, rows, width = q_all.shape
    keys = kv_buf.shape[2]
    chips = group // CORES
    side = chips * rows
    block = per * rows
    me = lax.axis_index('dcp')
    chip, core = me // CORES, me % CORES
    right = lax.rem(chip + 1, chips) * CORES + core
    left = lax.rem(chip + chips - 1, chips) * CORES + core
    twin = chip * CORES + (CORES - 1 - core)
    scale = (NOPE + ROPE) ** -0.5

    def remote(src, dst, send, recv, to):
        return pltpu.make_async_remote_copy(src_ref=src, dst_ref=dst, send_sem=send, recv_sem=recv,
                                            device_id={'dcp': to}, device_id_type=pl.DeviceIdType.MESH)

    def way(c):
        return lax.rem(c, 2)

    def toward(d):
        return jnp.where(d == 0, right, left)

    def q_copy(c, kind):
        if kind == 0:
            src, dst, to = q_all.at[c, 0], q_all.at[c, 1], right
        elif kind == 1:
            src, dst, to = q_all.at[c, 0], q_all.at[c, 2], left
        elif kind == 2:
            src, dst, to = q_all.at[c, 1 + way(c)], q_all.at[c, 3], toward(way(c))
        else:
            src, dst, to = q_all.at[c, pl.ds(0, chips)], q_all.at[c, pl.ds(chips, chips)], twin
        return remote(src, dst, q_send.at[c, kind], q_recv.at[c, kind], to)

    def part_twin(c, what):
        src, dst = ((sib_o, got_o), (sib_l, got_l))[what]
        return remote(src.at[c], dst.at[c], s_send.at[c, what], s_recv.at[c, what], twin)

    def hop_copy(c, what):
        src = (chip_o.at[c, 3], chip_l.at[c])[what]
        dst = (hop_o.at[c], hop_l.at[c])[what]
        return remote(src, dst, h_send.at[c, what], h_recv.at[c, what], toward(way(c)))

    def fin_copy(c, kind, what):
        if kind == 0:
            src, to = (mid_o.at[c], mid_l.at[c])[what], toward(way(c))
        else:
            src, to = (chip_o.at[c, 1 + way(c)], chip_l.at[c])[what], toward(1 - way(c))
        dst = (fin_o.at[c, kind], fin_l.at[c, kind])[what]
        return remote(src, dst, f_send.at[c, kind, what], f_recv.at[c, kind, what], to)

    def kv_copy(c, b):
        slot = lax.rem(c, KV_SLOTS)
        return pltpu.make_async_copy(kv_hbm.at[c * per + b], kv_buf.at[slot, b], kv_sem.at[slot, b])

    load = pltpu.make_async_copy(q_hbm, q_all.at[:, 0], load_sem)
    load.start()
    for c in range(min(KV_SLOTS, chunks)):
        for b in range(per):
            kv_copy(c, b).start()

    barrier = pltpu.get_barrier_semaphore()
    for peer in (left, right, twin):
        pl.semaphore_signal(barrier, inc=1, device_id={'dcp': peer}, device_id_type=pl.DeviceIdType.MESH)

    r_id = lax.broadcasted_iota(jnp.int32, (rows, keys), 0)
    k_id = lax.broadcasted_iota(jnp.int32, (rows, keys), 1)
    tokens = 2
    rank[...] = (k_id // PAGE * group + me) * PAGE + k_id % PAGE - r_id // (rows // tokens)

    load.wait()
    pl.semaphore_wait(barrier, 3)
    for c in range(min(AHEAD, chunks)):
        for kind in (0, 1):
            q_copy(c, kind).start()

    free_keys = (min_rounds * PAGE) // LANES * LANES

    def attend(c):
        slot = lax.rem(c, KV_SLOTS)
        for b in range(per):
            kv_copy(c, b).wait()
        for b in range(per):
            q = q_all[c, :, b].reshape(group * rows, width)
            kv = kv_buf.at[slot, b]
            s = lax.dot_general(q, kv[...], (((1,), (1,)), ((), ())), preferred_element_type=jnp.float32)
            tail = s[:, free_keys:].reshape(group, rows, keys - free_keys)
            limit = len_ref[c * per + b] - tokens
            seen = jnp.broadcast_to(rank[:, free_keys:][None], tail.shape) <= limit
            tail = jnp.where(seen, tail, -jnp.inf).reshape(group * rows, keys - free_keys)
            s = jnp.concatenate([s[:, :free_keys], tail], axis=1)
            top = jnp.max(s, axis=1, keepdims=True)
            p = jnp.exp2((s - top) * (scale * math.log2(math.e)))
            total = jnp.sum(p, axis=1, keepdims=True)
            o = jnp.dot(p.astype(jnp.bfloat16), kv[:, :LATENT], preferred_element_type=jnp.float32)
            o = o * (1.0 / total)
            lse = jnp.broadcast_to(top * scale + jnp.log(total), (group * rows, LANES))
            keep = lax.rem(c, KEPT)
            own_o[keep, b] = o[:side]
            own_l[keep, b] = lse[:side]
            sib_o[c, b] = o[side:].astype(jnp.bfloat16)
            sib_l[c, b] = lse[side:]

    lane_s = lax.broadcasted_iota(jnp.int32, (side, LANES), 1)
    row_s = lax.broadcasted_iota(jnp.int32, (side, LANES), 0)
    lane_b = lax.broadcasted_iota(jnp.int32, (block, LANES), 1)
    row_b = lax.broadcasted_iota(jnp.int32, (block, LANES), 0)

    def column(row, slot):
        picked = jnp.where(lane_b == row_b + slot * block, jnp.broadcast_to(row, (block, LANES)), 0.0)
        return jnp.broadcast_to(jnp.sum(picked, axis=1, keepdims=True), (block, LANES))

    def join_cores(c):
        packed = jnp.zeros((1, LANES), jnp.float32)
        keep = lax.rem(c, KEPT)
        for b in range(per):
            o, lse = merge(own_o[keep, b], own_l[keep, b], got_o[c, b].astype(jnp.float32), got_l[c, b])
            o = o.astype(jnp.bfloat16)
            for slot in range(chips):
                chip_o[c, slot, b * rows:(b + 1) * rows] = o[slot * rows:(slot + 1) * rows]
            at = row_s // rows * block + b * rows + row_s % rows
            packed = packed + jnp.sum(jnp.where(lane_s == at, lse, 0.0), axis=0, keepdims=True)
        chip_l[c] = packed

    def join_hop(c):
        slot = 2 - way(c)
        o, lse = merge(chip_o[c, slot].astype(jnp.float32), column(chip_l[c], slot), hop_o[c].astype(jnp.float32), column(hop_l[c], 3))
        mid_o[c] = o.astype(jnp.bfloat16)
        mid_l[c] = jnp.sum(jnp.where(lane_b == row_b, lse, 0.0), axis=0, keepdims=True)

    def join_last(c):
        parts = [(chip_o[c, 0], column(chip_l[c], 0)), (fin_o[c, 0], column(fin_l[c, 0], 0)),
                 (fin_o[c, 1], column(fin_l[c, 1], 1 + way(c)))]
        top = functools.reduce(jnp.maximum, [l for _, l in parts])
        weights = [jnp.exp(l - top) for _, l in parts]
        inv = 1.0 / functools.reduce(jnp.add, weights)
        o = functools.reduce(jnp.add, [part.astype(jnp.float32) * wide(w * inv, LATENT) for (part, _), w in zip(parts, weights)])
        o = o.astype(jnp.bfloat16)
        for b in range(per):
            out_ref[c * per + b] = o[b * rows:(b + 1) * rows]

    def stage(t, lag, fn):
        c = t - lag

        @pl.when(jnp.logical_and(c >= 0, c < chunks))
        def _():
            fn(c)

    def send_own(c):
        for kind in (0, 1):
            q_copy(c, kind).start()

    def spread(c):
        for kind in (0, 1):
            q_copy(c, kind).wait_recv()
        q_copy(c, 2).start()

    def to_twin(c):
        q_copy(c, 2).wait_recv()
        q_copy(c, 3).start()

    def work(c):
        q_copy(c, 3).wait_recv()
        attend(c)
        for what in range(2):
            part_twin(c, what).start()

        @pl.when(c + KV_SLOTS < chunks)
        def _():
            for b in range(per):
                kv_copy(c + KV_SLOTS, b).start()

    def cores(c):
        for what in range(2):
            part_twin(c, what).wait_recv()
        join_cores(c)
        for what in range(2):
            hop_copy(c, what).start()
            fin_copy(c, 1, what).start()

    def hop(c):
        for what in range(2):
            hop_copy(c, what).wait_recv()
        join_hop(c)
        for what in range(2):
            fin_copy(c, 0, what).start()

    def last(c):
        for what in range(2):
            for kind in range(2):
                fin_copy(c, kind, what).wait_recv()
        join_last(c)

    def sent(c):
        for kind in range(4):
            q_copy(c, kind).wait_send()
        for what in range(2):
            part_twin(c, what).wait_send()
            hop_copy(c, what).wait_send()
            for kind in range(2):
                fin_copy(c, kind, what).wait_send()

    def step(t, carry):
        stage(t, -AHEAD, send_own)
        stage(t, 0, spread)
        stage(t, LAG, to_twin)
        stage(t, 3 * LAG, cores)
        stage(t, 4 * LAG, hop)
        stage(t, 5 * LAG, last)
        stage(t, 5 * LAG + 1, sent)
        stage(t, 2 * LAG, work)
        return carry

    lax.fori_loop(0, chunks + 5 * LAG + 1, step, 0)


def solution(mesh):
    group = mesh.shape['dcp']
    chips = group // CORES

    def local_step(q_blk, kv_blk, len_blk):
        batch, tokens, heads, width = q_blk.shape
        rounds = kv_blk.shape[1]
        keys = rounds * PAGE
        rows = tokens * heads
        chunks = batch // CHUNK
        block = CHUNK * rows
        side = chips * rows
        bf, f32 = jnp.bfloat16, jnp.float32
        scratch = [
            pltpu.VMEM((chunks, group, CHUNK, rows, width), bf),
            pltpu.VMEM((KV_SLOTS, CHUNK, keys, width), bf),
            pltpu.VMEM((rows, keys), jnp.int32),
            pltpu.VMEM((KEPT, CHUNK, side, LATENT), f32),
            pltpu.VMEM((KEPT, CHUNK, side, LANES), f32),
            pltpu.VMEM((chunks, CHUNK, side, LATENT), bf),
            pltpu.VMEM((chunks, CHUNK, side, LANES), f32),
            pltpu.VMEM((chunks, CHUNK, side, LATENT), bf),
            pltpu.VMEM((chunks, CHUNK, side, LANES), f32),
            pltpu.VMEM((chunks, chips, block, LATENT), bf),
            pltpu.VMEM((chunks, 1, LANES), f32),
            pltpu.VMEM((chunks, block, LATENT), bf),
            pltpu.VMEM((chunks, 1, LANES), f32),
            pltpu.VMEM((chunks, block, LATENT), bf),
            pltpu.VMEM((chunks, 1, LANES), f32),
            pltpu.VMEM((chunks, 2, block, LATENT), bf),
            pltpu.VMEM((chunks, 2, 1, LANES), f32),
            pltpu.SemaphoreType.DMA,
            pltpu.SemaphoreType.DMA((KV_SLOTS, CHUNK)),
        ]
        for shape in ((chunks, 4), (chunks, 2), (chunks, 2), (chunks, 2, 2)):
            scratch += [pltpu.SemaphoreType.DMA(shape)] * 2
        flops = 2 * batch * group * rows * keys * (width + LATENT)
        o = pl.pallas_call(
            functools.partial(kernel, group, rounds // 2 - 1),
            out_shape=jax.ShapeDtypeStruct((batch, rows, LATENT), bf),
            in_specs=[pl.BlockSpec(memory_space=pltpu.SMEM), pl.BlockSpec(memory_space=pl.ANY), pl.BlockSpec(memory_space=pl.ANY)],
            out_specs=pl.BlockSpec(memory_space=pltpu.VMEM),
            scratch_shapes=scratch,
            compiler_params=pltpu.CompilerParams(collective_id=0, has_side_effects=True, vmem_limit_bytes=62 * 2**20),
            cost_estimate=pl.CostEstimate(flops=flops, bytes_accessed=kv_blk.size * 2, transcendentals=batch * group * rows * keys),
        )(len_blk, q_blk.reshape(chunks, CHUNK, rows, width), kv_blk.reshape(batch, keys, width))
        return o.reshape(batch, tokens, heads, LATENT)

    return jax.shard_map(local_step, mesh=mesh, in_specs=(P('dp', None, 'dcp', None), P('dp', None, 'dcp', None, None), P('dp')), out_specs=P('dp', None, 'dcp', None), check_vma=False)
```

```python
import functools
import math

import jax
import jax.numpy as jnp
from jax import lax
from jax.experimental import pallas as pl
from jax.experimental.pallas import tpu as pltpu
from jax.sharding import PartitionSpec as P

LATENT = 512
ROPE = 64
NOPE = 128
PAGE = 64
CORES = 2
CHUNK = 4
KV_SLOTS = 4
AHEAD = 3
KEPT = 2
SENDS = 4
LANES = 128


def wide(col, n):
    return jnp.concatenate([col] * (n // LANES), axis=1)


def merge(o_a, l_a, o_b, l_b):
    top = jnp.maximum(l_a, l_b)
    e_a = jnp.exp(l_a - top)
    e_b = jnp.exp(l_b - top)
    total = e_a + e_b
    inv = 1.0 / total
    n = o_a.shape[1]
    return o_a * wide(e_a * inv, n) + o_b * wide(e_b * inv, n), top + jnp.log(total)


def kernel(group, min_rounds, len_ref, q_hbm, kv_hbm, out_ref, q_all, kv_buf, rank, own_o, own_l, sib_o, sib_l,
           got_o, got_l, chip_o, chip_l, hop_o, hop_l, mid_o, mid_l, fin_o, fin_l,
           load_sem, kv_sem, q_send, q_recv, s_send, s_recv, h_send, h_recv, f_send, f_recv):
    chunks, _, per, rows, width = q_all.shape
    keys = kv_buf.shape[2]
    chips = group // CORES
    side = chips * rows
    block = per * rows
    lot = LANES // block
    me = lax.axis_index('dcp')
    chip, core = me // CORES, me % CORES
    right = lax.rem(chip + 1, chips) * CORES + core
    left = lax.rem(chip + chips - 1, chips) * CORES + core
    twin = chip * CORES + (CORES - 1 - core)
    scale = (NOPE + ROPE) ** -0.5

    def remote(src, dst, send, recv, to):
        return pltpu.make_async_remote_copy(src_ref=src, dst_ref=dst, send_sem=send, recv_sem=recv,
                                            device_id={'dcp': to}, device_id_type=pl.DeviceIdType.MESH)

    def way(c):
        return lax.rem(c, 2)

    def toward(d):
        return jnp.where(d == 0, right, left)

    def q_copy(c, kind):
        if kind == 0:
            src, dst, to = q_all.at[c, 0], q_all.at[c, 1], right
        elif kind == 1:
            src, dst, to = q_all.at[c, 0], q_all.at[c, 2], left
        elif kind == 2:
            src, dst, to = q_all.at[c, 1 + way(c)], q_all.at[c, 3], toward(way(c))
        else:
            src, dst, to = q_all.at[c, pl.ds(0, chips)], q_all.at[c, pl.ds(chips, chips)], twin
        return remote(src, dst, q_send.at[lax.rem(c, SENDS), kind], q_recv.at[c, kind], to)

    def part_twin(c, what):
        src, dst = ((sib_o, got_o), (sib_l, got_l))[what]
        return remote(src.at[c], dst.at[c], s_send.at[lax.rem(c, SENDS), what], s_recv.at[c, what], twin)

    def hop_copy(c, what):
        src = (chip_o.at[c, 3], chip_l.at[c, 3 // lot])[what]
        dst = (hop_o.at[c], hop_l.at[c])[what]
        return remote(src, dst, h_send.at[lax.rem(c, SENDS), what], h_recv.at[c, what], toward(way(c)))

    def fin_copy(c, kind, what):
        if kind == 0:
            src, to = (mid_o.at[c], mid_l.at[c])[what], toward(way(c))
        else:
            slot = 1 + way(c)
            src, to = (chip_o.at[c, slot], chip_l.at[c, slot // lot])[what], toward(1 - way(c))
        dst = (fin_o.at[c, kind], fin_l.at[c, kind])[what]
        return remote(src, dst, f_send.at[lax.rem(c, SENDS), kind, what], f_recv.at[c, kind, what], to)

    def kv_copy(c, b):
        slot = lax.rem(c, KV_SLOTS)
        return pltpu.make_async_copy(kv_hbm.at[c * per + b], kv_buf.at[slot, b], kv_sem.at[slot, b])

    def go(make, c, *which):
        @pl.when(c >= SENDS)
        def _():
            make(c - SENDS, *which).wait_send()

        make(c, *which).start()

    def send_own(c):
        for kind in (0, 1):
            go(q_copy, c, kind)

    load = pltpu.make_async_copy(q_hbm, q_all.at[:, 0], load_sem)
    load.start()
    barrier = pltpu.get_barrier_semaphore()
    for peer in (left, right, twin):
        pl.semaphore_signal(barrier, inc=1, device_id={'dcp': peer}, device_id_type=pl.DeviceIdType.MESH)

    r_id = lax.broadcasted_iota(jnp.int32, (rows, keys), 0)
    k_id = lax.broadcasted_iota(jnp.int32, (rows, keys), 1)
    tokens = 2
    rank[...] = (k_id // PAGE * group + me) * PAGE + k_id % PAGE - r_id // (rows // tokens)

    load.wait()
    pl.semaphore_wait(barrier, 3)
    for c in range(min(AHEAD, chunks)):
        send_own(jnp.int32(c))
    for c in range(min(KV_SLOTS, chunks)):
        for b in range(per):
            kv_copy(c, b).start()

    free_keys = (min_rounds * PAGE) // LANES * LANES

    def attend(c):
        slot = lax.rem(c, KV_SLOTS)
        for b in range(per):
            kv_copy(c, b).wait()
        for b in range(per):
            q = q_all[c, :, b].reshape(group * rows, width)
            kv = kv_buf.at[slot, b]
            s = lax.dot_general(q, kv[...], (((1,), (1,)), ((), ())), preferred_element_type=jnp.float32)
            tail = s[:, free_keys:].reshape(group, rows, keys - free_keys)
            limit = len_ref[c * per + b] - tokens
            seen = jnp.broadcast_to(rank[:, free_keys:][None], tail.shape) <= limit
            tail = jnp.where(seen, tail, -jnp.inf).reshape(group * rows, keys - free_keys)
            s = jnp.concatenate([s[:, :free_keys], tail], axis=1)
            top = jnp.max(s, axis=1, keepdims=True)
            p = jnp.exp2((s - top) * (scale * math.log2(math.e)))
            total = jnp.sum(p, axis=1, keepdims=True)
            o = jnp.dot(p.astype(jnp.bfloat16), kv[:, :LATENT], preferred_element_type=jnp.float32)
            o = o * (1.0 / total)
            lse = jnp.broadcast_to(top * scale + jnp.log(total), (group * rows, LANES))
            keep = lax.rem(c, KEPT)
            own_o[keep, b] = o[:side]
            own_l[keep, b] = lse[:side]
            sib_o[c, b] = o[side:].astype(jnp.bfloat16)
            sib_l[c, b] = lse[side:]

    lane_s = lax.broadcasted_iota(jnp.int32, (lot * rows, LANES), 1)
    row_s = lax.broadcasted_iota(jnp.int32, (lot * rows, LANES), 0)
    lane_b = lax.broadcasted_iota(jnp.int32, (block, LANES), 1)
    row_b = lax.broadcasted_iota(jnp.int32, (block, LANES), 0)

    def column(row, slot):
        picked = jnp.where(lane_b == row_b + lax.rem(slot, lot) * block, jnp.broadcast_to(row, (block, LANES)), 0.0)
        return jnp.broadcast_to(jnp.sum(picked, axis=1, keepdims=True), (block, LANES))

    def join_cores(c):
        packed = [jnp.zeros((1, LANES), jnp.float32) for _ in range(chips // lot)]
        keep = lax.rem(c, KEPT)
        for b in range(per):
            o, lse = merge(own_o[keep, b], own_l[keep, b], got_o[c, b].astype(jnp.float32), got_l[c, b])
            o = o.astype(jnp.bfloat16)
            for slot in range(chips):
                chip_o[c, slot, b * rows:(b + 1) * rows] = o[slot * rows:(slot + 1) * rows]
            at = row_s // rows * block + b * rows + row_s % rows
            for j in range(chips // lot):
                part = lse[j * lot * rows:(j + 1) * lot * rows]
                packed[j] = packed[j] + jnp.sum(jnp.where(lane_s == at, part, 0.0), axis=0, keepdims=True)
        for j in range(chips // lot):
            chip_l[c, j] = packed[j]

    def join_hop(c):
        slot = 2 - way(c)
        o, lse = merge(chip_o[c, slot].astype(jnp.float32), column(chip_l[c, slot // lot], slot),
                       hop_o[c].astype(jnp.float32), column(hop_l[c], jnp.int32(3)))
        mid_o[c] = o.astype(jnp.bfloat16)
        mid_l[c] = jnp.sum(jnp.where(lane_b == row_b, lse, 0.0), axis=0, keepdims=True)

    def join_last(c):
        parts = [(chip_o[c, 0], column(chip_l[c, 0], jnp.int32(0))), (fin_o[c, 0], column(fin_l[c, 0], jnp.int32(0))),
                 (fin_o[c, 1], column(fin_l[c, 1], 1 + way(c)))]
        top = functools.reduce(jnp.maximum, [l for _, l in parts])
        weights = [jnp.exp(l - top) for _, l in parts]
        inv = 1.0 / functools.reduce(jnp.add, weights)
        o = functools.reduce(jnp.add, [part.astype(jnp.float32) * wide(w * inv, LATENT) for (part, _), w in zip(parts, weights)])
        o = o.astype(jnp.bfloat16)
        for b in range(per):
            out_ref[c * per + b] = o[b * rows:(b + 1) * rows]

    def stage(t, lag, fn):
        c = t - lag

        @pl.when(jnp.logical_and(c >= 0, c < chunks))
        def _():
            fn(c)

    def spread(c):
        for kind in (0, 1):
            q_copy(c, kind).wait_recv()
        go(q_copy, c, 2)

    def to_twin(c):
        q_copy(c, 2).wait_recv()
        go(q_copy, c, 3)

    def work(c):
        q_copy(c, 3).wait_recv()
        attend(c)
        for what in range(2):
            go(part_twin, c, what)

        @pl.when(c + KV_SLOTS < chunks)
        def _():
            for b in range(per):
                kv_copy(c + KV_SLOTS, b).start()

    def cores(c):
        for what in range(2):
            part_twin(c, what).wait_recv()
        join_cores(c)
        for what in range(2):
            go(hop_copy, c, what)
            go(fin_copy, c, 1, what)

    def hop(c):
        for what in range(2):
            hop_copy(c, what).wait_recv()
        join_hop(c)
        for what in range(2):
            go(fin_copy, c, 0, what)

    def last(c):
        for what in range(2):
            for kind in range(2):
                fin_copy(c, kind, what).wait_recv()
        join_last(c)

    def step(t, carry):
        stage(t, -AHEAD, send_own)
        stage(t, 0, spread)
        stage(t, 1, to_twin)
        stage(t, 4, cores)
        stage(t, 6, hop)
        stage(t, 8, last)
        stage(t, 2, work)
        return carry

    lax.fori_loop(0, chunks + 8, step, 0)
    for c in range(max(chunks - SENDS, 0), chunks):
        c = jnp.int32(c)
        for kind in range(4):
            q_copy(c, kind).wait_send()
        for what in range(2):
            part_twin(c, what).wait_send()
            hop_copy(c, what).wait_send()
            for kind in range(2):
                fin_copy(c, kind, what).wait_send()


def solution(mesh):
    group = mesh.shape['dcp']
    chips = group // CORES

    def local_step(q_blk, kv_blk, len_blk):
        batch, tokens, heads, width = q_blk.shape
        rounds = kv_blk.shape[1]
        keys = rounds * PAGE
        rows = tokens * heads
        chunks = batch // CHUNK
        block = CHUNK * rows
        side = chips * rows
        bf, f32 = jnp.bfloat16, jnp.float32
        scratch = [
            pltpu.VMEM((chunks, group, CHUNK, rows, width), bf),
            pltpu.VMEM((KV_SLOTS, CHUNK, keys, width), bf),
            pltpu.VMEM((rows, keys), jnp.int32),
            pltpu.VMEM((KEPT, CHUNK, side, LATENT), f32),
            pltpu.VMEM((KEPT, CHUNK, side, LANES), f32),
            pltpu.VMEM((chunks, CHUNK, side, LATENT), bf),
            pltpu.VMEM((chunks, CHUNK, side, LANES), f32),
            pltpu.VMEM((chunks, CHUNK, side, LATENT), bf),
            pltpu.VMEM((chunks, CHUNK, side, LANES), f32),
            pltpu.VMEM((chunks, chips, block, LATENT), bf),
            pltpu.VMEM((chunks, chips * block // LANES, 1, LANES), f32),
            pltpu.VMEM((chunks, block, LATENT), bf),
            pltpu.VMEM((chunks, 1, LANES), f32),
            pltpu.VMEM((chunks, block, LATENT), bf),
            pltpu.VMEM((chunks, 1, LANES), f32),
            pltpu.VMEM((chunks, 2, block, LATENT), bf),
            pltpu.VMEM((chunks, 2, 1, LANES), f32),
            pltpu.SemaphoreType.DMA,
            pltpu.SemaphoreType.DMA((KV_SLOTS, CHUNK)),
        ]
        for shape in ((4,), (2,), (2,), (2, 2)):
            scratch += [pltpu.SemaphoreType.DMA((SENDS, *shape)), pltpu.SemaphoreType.DMA((chunks, *shape))]
        flops = 2 * batch * group * rows * keys * (width + LATENT)
        o = pl.pallas_call(
            functools.partial(kernel, group, rounds // 2 - 1),
            out_shape=jax.ShapeDtypeStruct((batch, rows, LATENT), bf),
            in_specs=[pl.BlockSpec(memory_space=pltpu.SMEM), pl.BlockSpec(memory_space=pl.ANY), pl.BlockSpec(memory_space=pl.ANY)],
            out_specs=pl.BlockSpec(memory_space=pltpu.VMEM),
            scratch_shapes=scratch,
            compiler_params=pltpu.CompilerParams(collective_id=0, has_side_effects=True, vmem_limit_bytes=62 * 2**20),
            cost_estimate=pl.CostEstimate(flops=flops, bytes_accessed=kv_blk.size * 2, transcendentals=batch * group * rows * keys),
        )(len_blk, q_blk.reshape(chunks, CHUNK, rows, width), kv_blk.reshape(batch, keys, width))
        return o.reshape(batch, tokens, heads, LATENT)

    return jax.shard_map(local_step, mesh=mesh, in_specs=(P('dp', None, 'dcp', None), P('dp', None, 'dcp', None, None), P('dp')), out_specs=P('dp', None, 'dcp', None), check_vma=False)
```

```python
import functools
import math

import jax
import jax.numpy as jnp
from jax import lax
from jax.experimental import pallas as pl
from jax.experimental.pallas import tpu as pltpu
from jax.sharding import PartitionSpec as P

LATENT = 512
ROPE = 64
NOPE = 128
PAGE = 64
CORES = 2
CHUNK = 2
KV_SLOTS = 8
AHEAD = 2
KEPT = 4
SENDS = 4
LANES = 128


def wide(col, n):
    return jnp.concatenate([col] * (n // LANES), axis=1)


def merge(o_a, l_a, o_b, l_b):
    top = jnp.maximum(l_a, l_b)
    e_a = jnp.exp(l_a - top)
    e_b = jnp.exp(l_b - top)
    total = e_a + e_b
    inv = 1.0 / total
    n = o_a.shape[1]
    return o_a * wide(e_a * inv, n) + o_b * wide(e_b * inv, n), top + jnp.log(total)


def kernel(group, min_rounds, len_ref, q_hbm, kv_hbm, out_hbm, q_all, kv_buf, rank, own, sib, got, chip_o, chip_l, hop_o, hop_l, mid_o, mid_l, fin_o, fin_l,
           out_buf, load_sem, kv_sem, out_sem, q_send, q_recv, s_send, s_recv, h_send, h_recv, f_send, f_recv):
    chunks, _, per, rows, width = q_all.shape
    keys = kv_buf.shape[2]
    chips = group // CORES
    side = chips * rows
    block = per * rows
    lot = LANES // block
    me = lax.axis_index('dcp')
    chip, core = me // CORES, me % CORES
    right = lax.rem(chip + 1, chips) * CORES + core
    left = lax.rem(chip + chips - 1, chips) * CORES + core
    twin = chip * CORES + (CORES - 1 - core)
    scale = (NOPE + ROPE) ** -0.5

    def remote(src, dst, send, recv, to):
        return pltpu.make_async_remote_copy(src_ref=src, dst_ref=dst, send_sem=send, recv_sem=recv,
                                            device_id={'dcp': to}, device_id_type=pl.DeviceIdType.MESH)

    def way(c):
        return lax.rem(c, 2)

    def toward(d):
        return jnp.where(d == 0, right, left)

    def q_copy(c, kind):
        if kind == 0:
            src, dst, to = q_all.at[c, 0], q_all.at[c, 1], right
        elif kind == 1:
            src, dst, to = q_all.at[c, 0], q_all.at[c, 2], left
        elif kind == 2:
            src, dst, to = q_all.at[c, 1 + way(c)], q_all.at[c, 3], toward(way(c))
        else:
            src, dst, to = q_all.at[c, pl.ds(0, chips)], q_all.at[c, pl.ds(chips, chips)], twin
        return remote(src, dst, q_send.at[lax.rem(c, SENDS), kind], q_recv.at[c, kind], to)

    def part_twin(c):
        return remote(sib.at[c], got.at[c], s_send.at[lax.rem(c, SENDS)], s_recv.at[c], twin)

    def hop_copy(c, what):
        src = (chip_o.at[c, 3], chip_l.at[c, 3 // lot])[what]
        dst = (hop_o.at[c], hop_l.at[c])[what]
        return remote(src, dst, h_send.at[lax.rem(c, SENDS), what], h_recv.at[c, what], toward(way(c)))

    def fin_copy(c, kind, what):
        if kind == 0:
            src, to = (mid_o.at[c], mid_l.at[c])[what], toward(way(c))
        else:
            slot = 1 + way(c)
            src, to = (chip_o.at[c, slot], chip_l.at[c, slot // lot])[what], toward(1 - way(c))
        dst = (fin_o.at[c, kind], fin_l.at[c, kind])[what]
        return remote(src, dst, f_send.at[lax.rem(c, SENDS), kind, what], f_recv.at[c, kind, what], to)

    def out_copy(c):
        return pltpu.make_async_copy(out_buf.at[c], out_hbm.at[c], out_sem.at[lax.rem(c, SENDS)])

    def kv_copy(c, b):
        slot = lax.rem(c, KV_SLOTS)
        return pltpu.make_async_copy(kv_hbm.at[c * per + b], kv_buf.at[slot, b], kv_sem.at[slot, b])

    def go(make, c, *which):
        @pl.when(c >= SENDS)
        def _():
            make(c - SENDS, *which).wait_send()

        make(c, *which).start()

    def send_own(c):
        for kind in (0, 1):
            go(q_copy, c, kind)

    load = pltpu.make_async_copy(q_hbm, q_all.at[:, 0], load_sem)
    load.start()
    barrier = pltpu.get_barrier_semaphore()
    for peer in (left, right, twin):
        pl.semaphore_signal(barrier, inc=1, device_id={'dcp': peer}, device_id_type=pl.DeviceIdType.MESH)

    r_id = lax.broadcasted_iota(jnp.int32, (rows, keys), 0)
    k_id = lax.broadcasted_iota(jnp.int32, (rows, keys), 1)
    tokens = 2
    rank[...] = (k_id // PAGE * group + me) * PAGE + k_id % PAGE - r_id // (rows // tokens)

    load.wait()
    pl.semaphore_wait(barrier, 3)
    for c in range(min(AHEAD, chunks)):
        send_own(jnp.int32(c))
    for c in range(min(KV_SLOTS, chunks)):
        for b in range(per):
            kv_copy(c, b).start()

    free_keys = (min_rounds * PAGE) // LANES * LANES

    def scores(c, b):
        q = q_all[c, :, b].reshape(group * rows, width)
        s = lax.dot_general(q, kv_buf[lax.rem(c, KV_SLOTS), b], (((1,), (1,)), ((), ())), preferred_element_type=jnp.float32)
        tail = s[:, free_keys:].reshape(group, rows, keys - free_keys)
        limit = len_ref[c * per + b] - tokens
        seen = jnp.broadcast_to(rank[:, free_keys:][None], tail.shape) <= limit
        tail = jnp.where(seen, tail, -jnp.inf).reshape(group * rows, keys - free_keys)
        return jnp.concatenate([s[:, :free_keys], tail], axis=1)

    def values(c, b, s):
        top = jnp.max(s, axis=1, keepdims=True)
        p = jnp.exp2((s - top) * (scale * math.log2(math.e)))
        total = jnp.sum(p, axis=1, keepdims=True)
        o = jnp.dot(p.astype(jnp.bfloat16), kv_buf[lax.rem(c, KV_SLOTS), b, :, :LATENT], preferred_element_type=jnp.float32)
        o = o * (1.0 / total)
        lse = jnp.broadcast_to(top * scale + jnp.log(total), (group * rows, LANES))
        keep = lax.rem(c, KEPT)
        own[keep, b, :, :LATENT] = o[:side]
        own[keep, b, :, LATENT:] = lse[:side]
        sib[c, b, :, :LATENT] = o[side:]
        sib[c, b, :, LATENT:] = lse[side:]

    def attend(c):
        ahead = scores(c, 0)
        for b in range(per):
            now = ahead
            if b + 1 < per:
                ahead = scores(c, b + 1)
            values(c, b, now)

    lane_s = lax.broadcasted_iota(jnp.int32, (lot * rows, LANES), 1)
    row_s = lax.broadcasted_iota(jnp.int32, (lot * rows, LANES), 0)
    lane_b = lax.broadcasted_iota(jnp.int32, (block, LANES), 1)
    row_b = lax.broadcasted_iota(jnp.int32, (block, LANES), 0)

    def column(row, slot):
        picked = jnp.where(lane_b == row_b + lax.rem(slot, lot) * block, jnp.broadcast_to(row, (block, LANES)), 0.0)
        return jnp.broadcast_to(jnp.sum(picked, axis=1, keepdims=True), (block, LANES))

    def join_cores(c):
        packed = [jnp.zeros((1, LANES), jnp.float32) for _ in range(chips // lot)]
        keep = lax.rem(c, KEPT)
        for b in range(per):
            o, lse = merge(own[keep, b, :, :LATENT], own[keep, b, :, LATENT:], got[c, b, :, :LATENT], got[c, b, :, LATENT:])
            o = o.astype(jnp.bfloat16)
            for slot in range(chips):
                chip_o[c, slot, b * rows:(b + 1) * rows] = o[slot * rows:(slot + 1) * rows]
            at = row_s // rows * block + b * rows + row_s % rows
            for j in range(chips // lot):
                part = lse[j * lot * rows:(j + 1) * lot * rows]
                packed[j] = packed[j] + jnp.sum(jnp.where(lane_s == at, part, 0.0), axis=0, keepdims=True)
        for j in range(chips // lot):
            chip_l[c, j] = packed[j]

    def join_hop(c):
        slot = 2 - way(c)
        o, lse = merge(chip_o[c, slot].astype(jnp.float32), column(chip_l[c, slot // lot], slot),
                       hop_o[c].astype(jnp.float32), column(hop_l[c], jnp.int32(3)))
        mid_o[c] = o.astype(jnp.bfloat16)
        mid_l[c] = jnp.sum(jnp.where(lane_b == row_b, lse, 0.0), axis=0, keepdims=True)

    def join_last(c):
        parts = [(chip_o[c, 0], column(chip_l[c, 0], jnp.int32(0))), (fin_o[c, 0], column(fin_l[c, 0], jnp.int32(0))),
                 (fin_o[c, 1], column(fin_l[c, 1], 1 + way(c)))]
        top = functools.reduce(jnp.maximum, [l for _, l in parts])
        weights = [jnp.exp(l - top) for _, l in parts]
        inv = 1.0 / functools.reduce(jnp.add, weights)
        o = functools.reduce(jnp.add, [part.astype(jnp.float32) * wide(w * inv, LATENT) for (part, _), w in zip(parts, weights)])
        o = o.astype(jnp.bfloat16)
        for b in range(per):
            out_buf[c, b] = o[b * rows:(b + 1) * rows]

    def stage(t, lag, fn):
        c = t - lag

        @pl.when(jnp.logical_and(c >= 0, c < chunks))
        def _():
            fn(c)

    def spread(c):
        for kind in (0, 1):
            q_copy(c, kind).wait_recv()
        go(q_copy, c, 2)

    def to_twin(c):
        q_copy(c, 2).wait_recv()
        go(q_copy, c, 3)

    def cores_in(c):
        part_twin(c).wait_recv()

    def cores_out(c):
        for what in range(2):
            go(hop_copy, c, what)
            go(fin_copy, c, 1, what)

    def hop_in(c):
        for what in range(2):
            hop_copy(c, what).wait_recv()

    def hop_out(c):
        for what in range(2):
            go(fin_copy, c, 0, what)

    def last_in(c):
        for what in range(2):
            for kind in range(2):
                fin_copy(c, kind, what).wait_recv()

    def last_out(c):
        @pl.when(c >= SENDS)
        def _():
            out_copy(c - SENDS).wait()

        out_copy(c).start()

    joins = ((13, last_in, join_last, last_out), (10, hop_in, join_hop, hop_out), (7, cores_in, join_cores, cores_out))
    lag = 4

    def step(t, carry):
        c = t - lag
        busy = jnp.logical_and(c >= 0, c < chunks)

        @pl.when(busy)
        def _():
            for late, ready, _, _ in joins:
                stage(t, late, ready)
            q_copy(c, 3).wait_recv()
            for b in range(per):
                kv_copy(c, b).wait()
            for late, _, join, _ in joins:
                old = t - late
                join(jnp.where(old >= 0, old, chunks))
            attend(c)
            go(part_twin, c)
            for late, _, _, pass_on in joins:
                stage(t, late, pass_on)

            @pl.when(c + KV_SLOTS < chunks)
            def _():
                for b in range(per):
                    kv_copy(c + KV_SLOTS, b).start()

        @pl.when(jnp.logical_not(busy))
        def _():
            for late, ready, join, pass_on in joins[::-1]:
                def all_of(c, ready=ready, join=join, pass_on=pass_on):
                    ready(c)
                    join(c)
                    pass_on(c)

                stage(t, late, all_of)

        stage(t, -AHEAD, send_own)
        stage(t, 0, spread)
        stage(t, 2, to_twin)
        return carry

    lax.fori_loop(0, chunks + joins[0][0], step, 0)
    for c in range(max(chunks - SENDS, 0), chunks):
        c = jnp.int32(c)
        for kind in range(4):
            q_copy(c, kind).wait_send()
        part_twin(c).wait_send()
        for what in range(2):
            hop_copy(c, what).wait_send()
            for kind in range(2):
                fin_copy(c, kind, what).wait_send()
        out_copy(c).wait()


def solution(mesh):
    group = mesh.shape['dcp']
    chips = group // CORES

    def local_step(q_blk, kv_blk, len_blk):
        batch, tokens, heads, width = q_blk.shape
        rounds = kv_blk.shape[1]
        keys = rounds * PAGE
        rows = tokens * heads
        chunks = batch // CHUNK
        block = CHUNK * rows
        side = chips * rows
        bf, f32 = jnp.bfloat16, jnp.float32
        scratch = [
            pltpu.VMEM((chunks, group, CHUNK, rows, width), bf),
            pltpu.VMEM((KV_SLOTS, CHUNK, keys, width), bf),
            pltpu.VMEM((rows, keys), jnp.int32),
            pltpu.VMEM((KEPT, CHUNK, side, LATENT + LANES), f32),
            pltpu.VMEM((chunks, CHUNK, side, LATENT + LANES), f32),
            pltpu.VMEM((chunks + 1, CHUNK, side, LATENT + LANES), f32),
            pltpu.VMEM((chunks + 1, chips, block, LATENT), bf),
            pltpu.VMEM((chunks + 1, chips * block // LANES, 1, LANES), f32),
            pltpu.VMEM((chunks + 1, block, LATENT), bf),
            pltpu.VMEM((chunks + 1, 1, LANES), f32),
            pltpu.VMEM((chunks + 1, block, LATENT), bf),
            pltpu.VMEM((chunks + 1, 1, LANES), f32),
            pltpu.VMEM((chunks + 1, 2, block, LATENT), bf),
            pltpu.VMEM((chunks + 1, 2, 1, LANES), f32),
            pltpu.VMEM((chunks + 1, CHUNK, rows, LATENT), bf),
            pltpu.SemaphoreType.DMA,
            pltpu.SemaphoreType.DMA((KV_SLOTS, CHUNK)),
            pltpu.SemaphoreType.DMA((SENDS,)),
        ]
        for shape in ((4,), (), (2,), (2, 2)):
            scratch += [pltpu.SemaphoreType.DMA((SENDS, *shape)), pltpu.SemaphoreType.DMA((chunks, *shape))]
        flops = 2 * batch * group * rows * keys * (width + LATENT)
        o = pl.pallas_call(
            functools.partial(kernel, group, rounds // 2 - 1),
            out_shape=jax.ShapeDtypeStruct((chunks, CHUNK, rows, LATENT), bf),
            in_specs=[pl.BlockSpec(memory_space=pltpu.SMEM), pl.BlockSpec(memory_space=pl.ANY), pl.BlockSpec(memory_space=pl.ANY)],
            out_specs=pl.BlockSpec(memory_space=pl.ANY),
            scratch_shapes=scratch,
            compiler_params=pltpu.CompilerParams(collective_id=0, has_side_effects=True, vmem_limit_bytes=62 * 2**20),
            cost_estimate=pl.CostEstimate(flops=flops, bytes_accessed=kv_blk.size * 2, transcendentals=batch * group * rows * keys),
        )(len_blk, q_blk.reshape(chunks, CHUNK, rows, width), kv_blk.reshape(batch, keys, width))
        return o.reshape(batch, tokens, heads, LATENT)

    return jax.shard_map(local_step, mesh=mesh, in_specs=(P('dp', None, 'dcp', None), P('dp', None, 'dcp', None, None), P('dp')), out_specs=P('dp', None, 'dcp', None), check_vma=False)
```

```python
import functools
import math

import jax
import jax.numpy as jnp
from jax import lax
from jax.experimental import pallas as pl
from jax.experimental.pallas import tpu as pltpu
from jax.sharding import PartitionSpec as P

LATENT = 512
ROPE = 64
NOPE = 128
PAGE = 64
CORES = 2
CHUNK = 4
KV_SLOTS = 4
AHEAD = 2
KEPT = 3
SENDS = 4
STRAIGHT = 1
LANES = 128


def wide(col, n):
    return jnp.concatenate([col] * (n // LANES), axis=1)


def merge(o_a, l_a, o_b, l_b):
    top = jnp.maximum(l_a, l_b)
    e_a = jnp.exp(l_a - top)
    e_b = jnp.exp(l_b - top)
    total = e_a + e_b
    inv = 1.0 / total
    n = o_a.shape[1]
    return o_a * wide(e_a * inv, n) + o_b * wide(e_b * inv, n), top + jnp.log(total)


def kernel(group, min_rounds, len_hbm, q_hbm, kv_hbm, out_hbm, q_all, kv_buf, rank, own, sib, got, chip_o, chip_l, hop_o, hop_l, mid_o, mid_l, fin_o, fin_l,
           out_buf, len_ref, load_sem, len_sem, kv_sem, out_sem, q_send, q_recv, s_send, s_recv, h_send, h_recv, f_send, f_recv):
    chunks, _, per, rows, width = q_all.shape
    keys = kv_buf.shape[2]
    chips = group // CORES
    side = chips * rows
    block = per * rows
    relayed = chunks - STRAIGHT
    lot = LANES // block
    me = lax.axis_index('dcp')
    chip, core = me // CORES, me % CORES
    right = lax.rem(chip + 1, chips) * CORES + core
    left = lax.rem(chip + chips - 1, chips) * CORES + core
    far = lax.rem(chip + 2, chips) * CORES + core
    twin = chip * CORES + (CORES - 1 - core)
    scale = (NOPE + ROPE) ** -0.5

    def remote(src, dst, send, recv, to):
        return pltpu.make_async_remote_copy(src_ref=src, dst_ref=dst, send_sem=send, recv_sem=recv,
                                            device_id={'dcp': to}, device_id_type=pl.DeviceIdType.MESH)

    def way(c):
        return lax.rem(c, 2)

    def toward(d):
        return jnp.where(d == 0, right, left)

    def q_copy(c, kind):
        if kind == 0:
            src, dst, to = q_all.at[c, 0], q_all.at[c, 1], right
        elif kind == 1:
            src, dst, to = q_all.at[c, 0], q_all.at[c, 2], left
        elif kind == 2:
            src, dst, to = q_all.at[c, 1 + way(c)], q_all.at[c, 3], toward(way(c))
        else:
            src, dst, to = q_all.at[c, pl.ds(0, chips)], q_all.at[c, pl.ds(chips, chips)], twin
        return remote(src, dst, q_send.at[lax.rem(c, SENDS), kind], q_recv.at[c, kind], to)

    def part_twin(c):
        return remote(sib.at[c], got.at[c], s_send.at[lax.rem(c, SENDS)], s_recv.at[c], twin)

    def hop_copy(c, what):
        src = (chip_o.at[c, 3], chip_l.at[c, 3 // lot])[what]
        dst = (hop_o.at[c], hop_l.at[c])[what]
        return remote(src, dst, h_send.at[lax.rem(c, SENDS), what], h_recv.at[c, what], jnp.where(c >= relayed, far, toward(way(c))))

    def fin_copy(c, kind, what):
        if kind == 0:
            src, to = (mid_o.at[c], mid_l.at[c])[what], toward(way(c))
        else:
            slot = 1 + way(c)
            src, to = (chip_o.at[c, slot], chip_l.at[c, slot // lot])[what], toward(1 - way(c))
        dst = (fin_o.at[c, kind], fin_l.at[c, kind])[what]
        return remote(src, dst, f_send.at[lax.rem(c, SENDS), kind, what], f_recv.at[c, kind, what], to)

    def fin_straight(c, what):
        slot = 2 - way(c)
        src = (chip_o.at[c, slot], chip_l.at[c, slot // lot])[what]
        dst = (fin_o.at[c, 0], fin_l.at[c, 0])[what]
        return remote(src, dst, f_send.at[lax.rem(c, SENDS), 0, what], f_recv.at[c, 0, what], toward(way(c)))

    def out_copy(c):
        return pltpu.make_async_copy(out_buf.at[c], out_hbm.at[c], out_sem.at[lax.rem(c, SENDS)])

    def kv_copy(c, b):
        slot = lax.rem(c, KV_SLOTS)
        return pltpu.make_async_copy(kv_hbm.at[c * per + b], kv_buf.at[slot, b], kv_sem.at[slot, b])

    def go(make, c, *which):
        @pl.when(c >= SENDS)
        def _():
            make(c - SENDS, *which).wait_send()

        make(c, *which).start()

    def send_own(c):
        for kind in (0, 1):
            go(q_copy, c, kind)

    load = pltpu.make_async_copy(q_hbm, q_all.at[:, 0], load_sem)
    load.start()
    lengths = pltpu.make_async_copy(len_hbm, len_ref, len_sem)
    lengths.start()
    barrier = pltpu.get_barrier_semaphore()
    for peer in (left, right, far, twin):
        pl.semaphore_signal(barrier, inc=1, device_id={'dcp': peer}, device_id_type=pl.DeviceIdType.MESH)

    r_id = lax.broadcasted_iota(jnp.int32, (rows, keys), 0)
    k_id = lax.broadcasted_iota(jnp.int32, (rows, keys), 1)
    tokens = 2
    rank[...] = (k_id // PAGE * group + me) * PAGE + k_id % PAGE - r_id // (rows // tokens)

    load.wait()
    pl.semaphore_wait(barrier, 4)
    for c in range(min(AHEAD, chunks)):
        send_own(jnp.int32(c))
    for c in range(min(KV_SLOTS, chunks)):
        for b in range(per):
            kv_copy(c, b).start()

    free_keys = (min_rounds * PAGE) // LANES * LANES

    def scores(c, b):
        q = q_all[c, :, b].reshape(group * rows, width)
        s = lax.dot_general(q, kv_buf[lax.rem(c, KV_SLOTS), b], (((1,), (1,)), ((), ())), preferred_element_type=jnp.float32)
        tail = s[:, free_keys:].reshape(group, rows, keys - free_keys)
        limit = len_ref[c * per + b] - tokens
        seen = jnp.broadcast_to(rank[:, free_keys:][None], tail.shape) <= limit
        tail = jnp.where(seen, tail, -jnp.inf).reshape(group * rows, keys - free_keys)
        return jnp.concatenate([s[:, :free_keys], tail], axis=1)

    def values(c, b, s):
        top = jnp.max(s, axis=1, keepdims=True)
        p = jnp.exp2((s - top) * (scale * math.log2(math.e)))
        total = jnp.sum(p, axis=1, keepdims=True)
        o = jnp.dot(p.astype(jnp.bfloat16), kv_buf[lax.rem(c, KV_SLOTS), b, :, :LATENT], preferred_element_type=jnp.float32)
        o = o * (1.0 / total)
        lse = jnp.broadcast_to(top * scale + jnp.log(total), (group * rows, LANES))
        keep = lax.rem(c, KEPT)
        own[keep, b, :, :LATENT] = o[:side]
        own[keep, b, :, LATENT:] = lse[:side]
        sib[c, b, :, :LATENT] = o[side:]
        sib[c, b, :, LATENT:] = lse[side:]

    def attend(c):
        ahead = scores(c, 0)
        for b in range(per):
            now = ahead
            if b + 1 < per:
                ahead = scores(c, b + 1)
            values(c, b, now)

    lane_s = lax.broadcasted_iota(jnp.int32, (lot * rows, LANES), 1)
    row_s = lax.broadcasted_iota(jnp.int32, (lot * rows, LANES), 0)
    lane_b = lax.broadcasted_iota(jnp.int32, (block, LANES), 1)
    row_b = lax.broadcasted_iota(jnp.int32, (block, LANES), 0)

    def column(row, slot):
        picked = jnp.where(lane_b == row_b + lax.rem(slot, lot) * block, jnp.broadcast_to(row, (block, LANES)), 0.0)
        return jnp.broadcast_to(jnp.sum(picked, axis=1, keepdims=True), (block, LANES))

    def join_cores(c):
        packed = [jnp.zeros((1, LANES), jnp.float32) for _ in range(chips // lot)]
        keep = lax.rem(c, KEPT)
        for b in range(per):
            o, lse = merge(own[keep, b, :, :LATENT], own[keep, b, :, LATENT:], got[c, b, :, :LATENT], got[c, b, :, LATENT:])
            o = o.astype(jnp.bfloat16)
            for slot in range(chips):
                chip_o[c, slot, b * rows:(b + 1) * rows] = o[slot * rows:(slot + 1) * rows]
            at = row_s // rows * block + b * rows + row_s % rows
            for j in range(chips // lot):
                part = lse[j * lot * rows:(j + 1) * lot * rows]
                packed[j] = packed[j] + jnp.sum(jnp.where(lane_s == at, part, 0.0), axis=0, keepdims=True)
        for j in range(chips // lot):
            chip_l[c, j] = packed[j]

    def join_hop(c):
        slot = 2 - way(c)
        o, lse = merge(chip_o[c, slot].astype(jnp.float32), column(chip_l[c, slot // lot], slot),
                       hop_o[c].astype(jnp.float32), column(hop_l[c], jnp.int32(3)))
        mid_o[c] = o.astype(jnp.bfloat16)
        mid_l[c] = jnp.sum(jnp.where(lane_b == row_b, lse, 0.0), axis=0, keepdims=True)

    def finish(c, parts):
        top = functools.reduce(jnp.maximum, [l for _, l in parts])
        weights = [jnp.exp(l - top) for _, l in parts]
        inv = 1.0 / functools.reduce(jnp.add, weights)
        o = functools.reduce(jnp.add, [part.astype(jnp.float32) * wide(w * inv, LATENT) for (part, _), w in zip(parts, weights)])
        o = o.astype(jnp.bfloat16)
        for b in range(per):
            out_buf[c, b] = o[b * rows:(b + 1) * rows]

    def join_last(c):
        finish(c, [(chip_o[c, 0], column(chip_l[c, 0], jnp.int32(0))), (fin_o[c, 0], column(fin_l[c, 0], jnp.int32(0))),
                   (fin_o[c, 1], column(fin_l[c, 1], 1 + way(c)))])

    def join_straight(c):
        finish(c, [(chip_o[c, 0], column(chip_l[c, 0], jnp.int32(0))), (fin_o[c, 0], column(fin_l[c, 0], 2 - way(c))),
                   (fin_o[c, 1], column(fin_l[c, 1], 1 + way(c))), (hop_o[c], column(hop_l[c], jnp.int32(3)))])

    def stage(t, lag, fn, start=0, stop=chunks):
        c = t - lag

        @pl.when(jnp.logical_and(c >= start, c < stop))
        def _():
            fn(c)

    def spread(c):
        for kind in (0, 1):
            q_copy(c, kind).wait_recv()
        go(q_copy, c, 2)

    def to_twin(c):
        q_copy(c, 2).wait_recv()
        go(q_copy, c, 3)

    def cores_in(c):
        part_twin(c).wait_recv()

    def cores_out(c):
        for what in range(2):
            go(hop_copy, c, what)
            go(fin_copy, c, 1, what)

    def hop_in(c):
        for what in range(2):
            hop_copy(c, what).wait_recv()

    def hop_out(c):
        for what in range(2):
            go(fin_copy, c, 0, what)

    def last_in(c):
        for what in range(2):
            for kind in range(2):
                fin_copy(c, kind, what).wait_recv()

    def last_out(c):
        @pl.when(c >= SENDS)
        def _():
            out_copy(c - SENDS).wait()

        out_copy(c).start()

    joins = ((11, last_in, join_last, last_out), (8, hop_in, join_hop, hop_out), (5, cores_in, join_cores, cores_out))
    lag = 3

    def step(t, carry):
        stage(t, -AHEAD, send_own)
        stage(t, 0, spread)
        stage(t, 2, to_twin)
        c = t - lag
        busy = jnp.logical_and(c >= 0, c < chunks)

        @pl.when(busy)
        def _():
            for late, ready, _, _ in joins:
                stage(t, late, ready)
            q_copy(c, 3).wait_recv()
            for b in range(per):
                kv_copy(c, b).wait()
            for late, _, join, _ in joins:
                old = t - late
                join(jnp.where(old >= 0, old, chunks))
            attend(c)
            go(part_twin, c)
            for late, _, _, pass_on in joins:
                stage(t, late, pass_on)

            @pl.when(c + KV_SLOTS < chunks)
            def _():
                for b in range(per):
                    kv_copy(c + KV_SLOTS, b).start()

        @pl.when(jnp.logical_not(busy))
        def _():
            def cores(c):
                cores_in(c)
                join_cores(c)
                cores_out(c)

            def cores_straight(c):
                cores(c)
                for what in range(2):
                    go(fin_straight, c, what)

            def hop(c):
                hop_in(c)
                join_hop(c)
                hop_out(c)

            def last(c):
                last_in(c)
                join_last(c)
                last_out(c)

            def last_straight(c):
                last_in(c)
                hop_in(c)
                join_straight(c)
                last_out(c)

            stage(t, joins[2][0], cores, stop=relayed)
            stage(t, joins[2][0], cores_straight, start=relayed)
            stage(t, joins[1][0], hop, stop=relayed)
            stage(t, joins[0][0], last, stop=relayed)
            stage(t, joins[0][0], last_straight, start=relayed)

        return carry

    lengths.wait()
    lax.fori_loop(0, chunks + joins[0][0], step, 0)
    for c in range(max(chunks - SENDS, 0), chunks):
        c = jnp.int32(c)
        for kind in range(4):
            q_copy(c, kind).wait_send()
        part_twin(c).wait_send()
        for what in range(2):
            hop_copy(c, what).wait_send()
            for kind in range(2):
                fin_copy(c, kind, what).wait_send()
        out_copy(c).wait()


def solution(mesh):
    group = mesh.shape['dcp']
    chips = group // CORES

    def local_step(q_blk, kv_blk, len_blk):
        batch, tokens, heads, width = q_blk.shape
        rounds = kv_blk.shape[1]
        keys = rounds * PAGE
        rows = tokens * heads
        chunks = batch // CHUNK
        block = CHUNK * rows
        side = chips * rows
        bf, f32 = jnp.bfloat16, jnp.float32
        scratch = [
            pltpu.VMEM((chunks, group, CHUNK, rows, width), bf),
            pltpu.VMEM((KV_SLOTS, CHUNK, keys, width), bf),
            pltpu.VMEM((rows, keys), jnp.int32),
            pltpu.VMEM((KEPT, CHUNK, side, LATENT + LANES), f32),
            pltpu.VMEM((chunks, CHUNK, side, LATENT + LANES), f32),
            pltpu.VMEM((chunks + 1, CHUNK, side, LATENT + LANES), f32),
            pltpu.VMEM((chunks + 1, chips, block, LATENT), bf),
            pltpu.VMEM((chunks + 1, chips * block // LANES, 1, LANES), f32),
            pltpu.VMEM((chunks + 1, block, LATENT), bf),
            pltpu.VMEM((chunks + 1, 1, LANES), f32),
            pltpu.VMEM((chunks + 1, block, LATENT), bf),
            pltpu.VMEM((chunks + 1, 1, LANES), f32),
            pltpu.VMEM((chunks + 1, 2, block, LATENT), bf),
            pltpu.VMEM((chunks + 1, 2, 1, LANES), f32),
            pltpu.VMEM((chunks + 1, CHUNK, rows, LATENT), bf),
            pltpu.SMEM((batch,), jnp.int32),
            pltpu.SemaphoreType.DMA,
            pltpu.SemaphoreType.DMA,
            pltpu.SemaphoreType.DMA((KV_SLOTS, CHUNK)),
            pltpu.SemaphoreType.DMA((SENDS,)),
        ]
        for shape in ((4,), (), (2,), (2, 2)):
            scratch += [pltpu.SemaphoreType.DMA((SENDS, *shape)), pltpu.SemaphoreType.DMA((chunks, *shape))]
        flops = 2 * batch * group * rows * keys * (width + LATENT)
        o = pl.pallas_call(
            functools.partial(kernel, group, rounds // 2 - 1),
            out_shape=jax.ShapeDtypeStruct((chunks, CHUNK, rows, LATENT), bf),
            in_specs=[pl.BlockSpec(memory_space=pl.ANY), pl.BlockSpec(memory_space=pl.ANY), pl.BlockSpec(memory_space=pl.ANY)],
            out_specs=pl.BlockSpec(memory_space=pl.ANY),
            scratch_shapes=scratch,
            compiler_params=pltpu.CompilerParams(collective_id=0, has_side_effects=True, vmem_limit_bytes=62 * 2**20),
            cost_estimate=pl.CostEstimate(flops=flops, bytes_accessed=kv_blk.size * 2, transcendentals=batch * group * rows * keys),
        )(len_blk, q_blk.reshape(chunks, CHUNK, rows, width), kv_blk.reshape(batch, keys, width))
        return o.reshape(batch, tokens, heads, LATENT)

    return jax.shard_map(local_step, mesh=mesh, in_specs=(P('dp', None, 'dcp', None), P('dp', None, 'dcp', None, None), P('dp')), out_specs=P('dp', None, 'dcp', None), check_vma=False)
```

```python
import functools
import math

import jax
import jax.numpy as jnp
from jax import lax
from jax.experimental import pallas as pl
from jax.experimental.pallas import tpu as pltpu
from jax.sharding import PartitionSpec as P

LATENT = 512
ROPE = 64
NOPE = 128
PAGE = 64
TOKENS = 2
CORES = 2
CHUNK = 4
KV_SLOTS = 4
AHEAD = 2
KEPT = 3
SENDS = 4
STRAIGHT = 1
LANES = 128


def wide(col, n):
    return jnp.concatenate([col] * (n // LANES), axis=1)


def merge(o_a, l_a, o_b, l_b):
    top = jnp.maximum(l_a, l_b)
    e_a = jnp.exp(l_a - top)
    e_b = jnp.exp(l_b - top)
    total = e_a + e_b
    inv = 1.0 / total
    n = o_a.shape[1]
    return o_a * wide(e_a * inv, n) + o_b * wide(e_b * inv, n), top + jnp.log(total)


def kernel(group, min_rounds, len_hbm, q_hbm, kv_hbm, out_hbm, q_raw, q_all, kv_buf, rank, own, sib, got, chip_o, chip_l, hop_o, hop_l, mid_o, mid_l, fin_o, fin_l,
           out_buf, len_ref, load_sem, len_sem, kv_sem, out_sem, q_send, q_recv, s_send, s_recv, h_send, h_recv, f_send, f_recv):
    chunks, per, rows, width = q_raw.shape
    half = per // 2
    heads = rows // TOKENS
    tiles = LATENT // LANES
    keys = kv_buf.shape[2]
    chips = group // CORES
    side = chips * rows
    block = per * rows
    relayed = chunks - STRAIGHT
    lot = LANES // block
    me = lax.axis_index('dcp')
    chip, core = me // CORES, me % CORES
    right = lax.rem(chip + 1, chips) * CORES + core
    left = lax.rem(chip + chips - 1, chips) * CORES + core
    far = lax.rem(chip + 2, chips) * CORES + core
    twin = chip * CORES + (CORES - 1 - core)
    scale = (NOPE + ROPE) ** -0.5

    def remote(src, dst, send, recv, to):
        return pltpu.make_async_remote_copy(src_ref=src, dst_ref=dst, send_sem=send, recv_sem=recv,
                                            device_id={'dcp': to}, device_id_type=pl.DeviceIdType.MESH)

    def way(c):
        return lax.rem(c, 2)

    def toward(d):
        return jnp.where(d == 0, right, left)

    def q_copy(c, kind):
        if kind == 0:
            src, dst, to = q_all.at[c, 0], q_all.at[c, 1], right
        elif kind == 1:
            src, dst, to = q_all.at[c, 0], q_all.at[c, 2], left
        elif kind == 2:
            src, dst, to = q_all.at[c, 1, 0], q_all.at[c, 3, 0], right
        elif kind == 3:
            src, dst, to = q_all.at[c, 2, 1], q_all.at[c, 3, 1], left
        else:
            src, dst, to = q_all.at[c, pl.ds(0, chips)], q_all.at[c, pl.ds(chips, chips)], twin
        return remote(src, dst, q_send.at[lax.rem(c, SENDS), kind], q_recv.at[c, kind], to)

    def part_twin(c):
        return remote(sib.at[c], got.at[c], s_send.at[lax.rem(c, SENDS)], s_recv.at[c], twin)

    def hop_copy(c, what):
        src = (chip_o.at[c, 3], chip_l.at[c, 3 // lot])[what]
        dst = (hop_o.at[c], hop_l.at[c])[what]
        return remote(src, dst, h_send.at[lax.rem(c, SENDS), what], h_recv.at[c, what], jnp.where(c >= relayed, far, toward(way(c))))

    def fin_copy(c, kind, what):
        if kind == 0:
            src, to = (mid_o.at[c], mid_l.at[c])[what], toward(way(c))
        else:
            slot = 1 + way(c)
            src, to = (chip_o.at[c, slot], chip_l.at[c, slot // lot])[what], toward(1 - way(c))
        dst = (fin_o.at[c, kind], fin_l.at[c, kind])[what]
        return remote(src, dst, f_send.at[lax.rem(c, SENDS), kind, what], f_recv.at[c, kind, what], to)

    def fin_straight(c, what):
        slot = 2 - way(c)
        src = (chip_o.at[c, slot], chip_l.at[c, slot // lot])[what]
        dst = (fin_o.at[c, 0], fin_l.at[c, 0])[what]
        return remote(src, dst, f_send.at[lax.rem(c, SENDS), 0, what], f_recv.at[c, 0, what], toward(way(c)))

    def out_copy(c):
        return pltpu.make_async_copy(out_buf.at[c], out_hbm.at[c], out_sem.at[lax.rem(c, SENDS)])

    def kv_copy(c, b):
        slot = lax.rem(c, KV_SLOTS)
        return pltpu.make_async_copy(kv_hbm.at[c * per + b], kv_buf.at[slot, b], kv_sem.at[slot, b])

    def go(make, c, *which):
        @pl.when(c >= SENDS)
        def _():
            make(c - SENDS, *which).wait_send()

        make(c, *which).start()

    def pack(c):
        for b in range(per):
            h, n = b // half, b % half
            for k in range(tiles):
                at = (k * half + n) * rows
                q_all[c, 0, h, at:at + rows] = q_raw[c, b, :, k * LANES:(k + 1) * LANES]
            turn = q_raw[c, b, :, LATENT:].astype(jnp.float32)
            at = tiles * half * rows + n * heads
            both = jnp.concatenate([turn[t * heads:(t + 1) * heads] for t in range(TOKENS)], axis=1)
            q_all[c, 0, h, at:at + heads] = both.astype(jnp.bfloat16)

    def send_own(c):
        for kind in (0, 1):
            go(q_copy, c, kind)

    load = pltpu.make_async_copy(q_hbm, q_raw, load_sem)
    load.start()
    lengths = pltpu.make_async_copy(len_hbm, len_ref, len_sem)
    lengths.start()
    barrier = pltpu.get_barrier_semaphore()
    for peer in (left, right, twin):
        pl.semaphore_signal(barrier, inc=1, device_id={'dcp': peer}, device_id_type=pl.DeviceIdType.MESH)

    r_id = lax.broadcasted_iota(jnp.int32, (rows, keys), 0)
    k_id = lax.broadcasted_iota(jnp.int32, (rows, keys), 1)
    rank[...] = (k_id // PAGE * group + me) * PAGE + k_id % PAGE - r_id // heads

    load.wait()
    for c in range(min(AHEAD, chunks)):
        pack(c)
    pl.semaphore_wait(barrier, 3)
    for c in range(min(AHEAD, chunks)):
        send_own(jnp.int32(c))
    for c in range(min(KV_SLOTS, chunks)):
        for b in range(per):
            kv_copy(c, b).start()
    for c in range(min(AHEAD, chunks), chunks):
        pack(c)

    free_keys = (min_rounds * PAGE) // LANES * LANES

    def scores(c, b):
        h, n = b // half, b % half
        latent = [q_all[c, :, h, (k * half + n) * rows:(k * half + n + 1) * rows] for k in range(tiles)]
        latent = jnp.concatenate([x.reshape(group * rows, LANES) for x in latent], axis=1)
        at = tiles * half * rows + n * heads
        both = q_all[c, :, h, at:at + heads].astype(jnp.float32).reshape(group * heads, LANES)
        turn = jnp.stack([both.reshape(group, heads, LANES), pltpu.roll(both, ROPE, 1).reshape(group, heads, LANES)], axis=1)
        turn = turn.reshape(group * rows, LANES).astype(jnp.bfloat16)[:, :ROPE]
        kv = kv_buf.at[lax.rem(c, KV_SLOTS), b]
        over = (((1,), (1,)), ((), ()))
        s = lax.dot_general(latent, kv[:, :LATENT], over, preferred_element_type=jnp.float32)
        s = s + lax.dot_general(turn, kv[:, LATENT:], over, preferred_element_type=jnp.float32)
        tail = s[:, free_keys:].reshape(group, rows, keys - free_keys)
        limit = len_ref[c * per + b] - TOKENS
        seen = jnp.broadcast_to(rank[:, free_keys:][None], tail.shape) <= limit
        tail = jnp.where(seen, tail, -jnp.inf).reshape(group * rows, keys - free_keys)
        return jnp.concatenate([s[:, :free_keys], tail], axis=1)

    def values(c, b, s):
        top = jnp.max(s, axis=1, keepdims=True)
        p = jnp.exp2((s - top) * (scale * math.log2(math.e)))
        total = jnp.sum(p, axis=1, keepdims=True)
        o = jnp.dot(p.astype(jnp.bfloat16), kv_buf[lax.rem(c, KV_SLOTS), b, :, :LATENT], preferred_element_type=jnp.float32)
        o = o * (1.0 / total)
        lse = jnp.broadcast_to(top * scale + jnp.log(total), (group * rows, LANES))
        keep = lax.rem(c, KEPT)
        own[keep, b, :, :LATENT] = o[:side]
        own[keep, b, :, LATENT:] = lse[:side]
        sib[c, b, :, :LATENT] = o[side:]
        sib[c, b, :, LATENT:] = lse[side:]

    def attend(c):
        ahead = scores(c, 0)
        for b in range(per):
            now = ahead
            if b + 1 < per:
                ahead = scores(c, b + 1)
            values(c, b, now)

    lane_s = lax.broadcasted_iota(jnp.int32, (lot * rows, LANES), 1)
    row_s = lax.broadcasted_iota(jnp.int32, (lot * rows, LANES), 0)
    lane_b = lax.broadcasted_iota(jnp.int32, (block, LANES), 1)
    row_b = lax.broadcasted_iota(jnp.int32, (block, LANES), 0)

    def column(row, slot):
        picked = jnp.where(lane_b == row_b + lax.rem(slot, lot) * block, jnp.broadcast_to(row, (block, LANES)), 0.0)
        return jnp.broadcast_to(jnp.sum(picked, axis=1, keepdims=True), (block, LANES))

    def join_cores(c):
        packed = [jnp.zeros((1, LANES), jnp.float32) for _ in range(chips // lot)]
        keep = lax.rem(c, KEPT)
        for b in range(per):
            o, lse = merge(own[keep, b, :, :LATENT], own[keep, b, :, LATENT:], got[c, b, :, :LATENT], got[c, b, :, LATENT:])
            o = o.astype(jnp.bfloat16)
            for slot in range(chips):
                chip_o[c, slot, b * rows:(b + 1) * rows] = o[slot * rows:(slot + 1) * rows]
            at = row_s // rows * block + b * rows + row_s % rows
            for j in range(chips // lot):
                part = lse[j * lot * rows:(j + 1) * lot * rows]
                packed[j] = packed[j] + jnp.sum(jnp.where(lane_s == at, part, 0.0), axis=0, keepdims=True)
        for j in range(chips // lot):
            chip_l[c, j] = packed[j]

    def join_hop(c):
        slot = 2 - way(c)
        o, lse = merge(chip_o[c, slot].astype(jnp.float32), column(chip_l[c, slot // lot], slot),
                       hop_o[c].astype(jnp.float32), column(hop_l[c], jnp.int32(3)))
        mid_o[c] = o.astype(jnp.bfloat16)
        mid_l[c] = jnp.sum(jnp.where(lane_b == row_b, lse, 0.0), axis=0, keepdims=True)

    def finish(c, parts):
        top = functools.reduce(jnp.maximum, [l for _, l in parts])
        weights = [jnp.exp(l - top) for _, l in parts]
        inv = 1.0 / functools.reduce(jnp.add, weights)
        o = functools.reduce(jnp.add, [part.astype(jnp.float32) * wide(w * inv, LATENT) for (part, _), w in zip(parts, weights)])
        o = o.astype(jnp.bfloat16)
        for b in range(per):
            out_buf[c, b] = o[b * rows:(b + 1) * rows]

    def join_last(c):
        finish(c, [(chip_o[c, 0], column(chip_l[c, 0], jnp.int32(0))), (fin_o[c, 0], column(fin_l[c, 0], jnp.int32(0))),
                   (fin_o[c, 1], column(fin_l[c, 1], 1 + way(c)))])

    def join_straight(c):
        finish(c, [(chip_o[c, 0], column(chip_l[c, 0], jnp.int32(0))), (fin_o[c, 0], column(fin_l[c, 0], 2 - way(c))),
                   (fin_o[c, 1], column(fin_l[c, 1], 1 + way(c))), (hop_o[c], column(hop_l[c], jnp.int32(3)))])

    def stage(t, lag, fn, start=0, stop=chunks):
        c = t - lag

        @pl.when(jnp.logical_and(c >= start, c < stop))
        def _():
            fn(c)

    def spread(c):
        for kind in (0, 1):
            q_copy(c, kind).wait_recv()
        for kind in (2, 3):
            go(q_copy, c, kind)

    def to_twin(c):
        for kind in (2, 3):
            q_copy(c, kind).wait_recv()
        go(q_copy, c, 4)

    def cores_in(c):
        part_twin(c).wait_recv()

    def cores_out(c):
        for what in range(2):
            go(hop_copy, c, what)
            go(fin_copy, c, 1, what)

    def hop_in(c):
        for what in range(2):
            hop_copy(c, what).wait_recv()

    def hop_out(c):
        for what in range(2):
            go(fin_copy, c, 0, what)

    def last_in(c):
        for what in range(2):
            for kind in range(2):
                fin_copy(c, kind, what).wait_recv()

    def last_out(c):
        @pl.when(c >= SENDS)
        def _():
            out_copy(c - SENDS).wait()

        out_copy(c).start()

    joins = ((11, last_in, join_last, last_out), (8, hop_in, join_hop, hop_out), (5, cores_in, join_cores, cores_out))
    lag = 3

    def step(t, carry):
        stage(t, -AHEAD, send_own)
        stage(t, 0, spread)
        stage(t, 2, to_twin)
        c = t - lag
        busy = jnp.logical_and(c >= 0, c < chunks)

        @pl.when(busy)
        def _():
            for late, ready, _, _ in joins:
                stage(t, late, ready)
            q_copy(c, 4).wait_recv()
            for b in range(per):
                kv_copy(c, b).wait()
            for late, _, join, _ in joins:
                old = t - late
                join(jnp.where(old >= 0, old, chunks))
            attend(c)
            go(part_twin, c)
            for late, _, _, pass_on in joins:
                stage(t, late, pass_on)

            @pl.when(c + KV_SLOTS < chunks)
            def _():
                for b in range(per):
                    kv_copy(c + KV_SLOTS, b).start()

        @pl.when(jnp.logical_not(busy))
        def _():
            def cores(c):
                cores_in(c)
                join_cores(c)
                cores_out(c)

            def cores_straight(c):
                cores(c)
                for what in range(2):
                    go(fin_straight, c, what)

            def hop(c):
                hop_in(c)
                join_hop(c)
                hop_out(c)

            def last(c):
                last_in(c)
                join_last(c)
                last_out(c)

            def last_straight(c):
                last_in(c)
                hop_in(c)
                join_straight(c)
                last_out(c)

            stage(t, joins[2][0], cores, stop=relayed)
            stage(t, joins[2][0], cores_straight, start=relayed)
            stage(t, joins[1][0], hop, stop=relayed)
            stage(t, joins[0][0], last, stop=relayed)
            stage(t, joins[0][0], last_straight, start=relayed)

        return carry

    lengths.wait()
    lax.fori_loop(0, chunks + joins[0][0], step, 0)
    for c in range(max(chunks - SENDS, 0), chunks):
        c = jnp.int32(c)
        for kind in range(5):
            q_copy(c, kind).wait_send()
        part_twin(c).wait_send()
        for what in range(2):
            hop_copy(c, what).wait_send()
            for kind in range(2):
                fin_copy(c, kind, what).wait_send()
        out_copy(c).wait()


def solution(mesh):
    group = mesh.shape['dcp']
    chips = group // CORES

    def local_step(q_blk, kv_blk, len_blk):
        batch, tokens, heads, width = q_blk.shape
        rounds = kv_blk.shape[1]
        keys = rounds * PAGE
        rows = tokens * heads
        chunks = batch // CHUNK
        block = CHUNK * rows
        side = chips * rows
        bf, f32 = jnp.bfloat16, jnp.float32
        scratch = [
            pltpu.VMEM((chunks, CHUNK, rows, width), bf),
            pltpu.VMEM((chunks, group, 2, CHUNK // 2 * rows * width // LANES, LANES), bf),
            pltpu.VMEM((KV_SLOTS, CHUNK, keys, width), bf),
            pltpu.VMEM((rows, keys), jnp.int32),
            pltpu.VMEM((KEPT, CHUNK, side, LATENT + LANES), f32),
            pltpu.VMEM((chunks, CHUNK, side, LATENT + LANES), f32),
            pltpu.VMEM((chunks + 1, CHUNK, side, LATENT + LANES), f32),
            pltpu.VMEM((chunks + 1, chips, block, LATENT), bf),
            pltpu.VMEM((chunks + 1, chips * block // LANES, 1, LANES), f32),
            pltpu.VMEM((chunks + 1, block, LATENT), bf),
            pltpu.VMEM((chunks + 1, 1, LANES), f32),
            pltpu.VMEM((chunks + 1, block, LATENT), bf),
            pltpu.VMEM((chunks + 1, 1, LANES), f32),
            pltpu.VMEM((chunks + 1, 2, block, LATENT), bf),
            pltpu.VMEM((chunks + 1, 2, 1, LANES), f32),
            pltpu.VMEM((chunks + 1, CHUNK, rows, LATENT), bf),
            pltpu.SMEM((batch,), jnp.int32),
            pltpu.SemaphoreType.DMA,
            pltpu.SemaphoreType.DMA,
            pltpu.SemaphoreType.DMA((KV_SLOTS, CHUNK)),
            pltpu.SemaphoreType.DMA((SENDS,)),
        ]
        for shape in ((5,), (), (2,), (2, 2)):
            scratch += [pltpu.SemaphoreType.DMA((SENDS, *shape)), pltpu.SemaphoreType.DMA((chunks, *shape))]
        flops = 2 * batch * group * rows * keys * (width + LATENT)
        o = pl.pallas_call(
            functools.partial(kernel, group, rounds // 2 - 1),
            out_shape=jax.ShapeDtypeStruct((chunks, CHUNK, rows, LATENT), bf),
            in_specs=[pl.BlockSpec(memory_space=pl.ANY), pl.BlockSpec(memory_space=pl.ANY), pl.BlockSpec(memory_space=pl.ANY)],
            out_specs=pl.BlockSpec(memory_space=pl.ANY),
            scratch_shapes=scratch,
            compiler_params=pltpu.CompilerParams(collective_id=0, has_side_effects=True, vmem_limit_bytes=62 * 2**20),
            cost_estimate=pl.CostEstimate(flops=flops, bytes_accessed=kv_blk.size * 2, transcendentals=batch * group * rows * keys),
        )(len_blk, q_blk.reshape(chunks, CHUNK, rows, width), kv_blk.reshape(batch, keys, width))
        return o.reshape(batch, tokens, heads, LATENT)

    return jax.shard_map(local_step, mesh=mesh, in_specs=(P('dp', None, 'dcp', None), P('dp', None, 'dcp', None, None), P('dp')), out_specs=P('dp', None, 'dcp', None), check_vma=False)
```

```python
import functools
import math

import jax
import jax.numpy as jnp
from jax import lax
from jax.experimental import pallas as pl
from jax.experimental.pallas import tpu as pltpu
from jax.sharding import PartitionSpec as P

LATENT = 512
ROPE = 64
NOPE = 128
PAGE = 64
TOKENS = 2
CORES = 2
CHUNK = 4
KV_SLOTS = 3
AHEAD = 2
KEPT = 3
SENDS = 2
STRAIGHT = 1
LANES = 128


def wide(col, n):
    return jnp.concatenate([col] * (n // LANES), axis=1)


def merge(o_a, l_a, o_b, l_b):
    top = jnp.maximum(l_a, l_b)
    e_a = jnp.exp(l_a - top)
    e_b = jnp.exp(l_b - top)
    total = e_a + e_b
    inv = 1.0 / total
    n = o_a.shape[1]
    return o_a * wide(e_a * inv, n) + o_b * wide(e_b * inv, n), top + jnp.log(total)


def kernel(group, min_rounds, len_hbm, q_hbm, kv_hbm, out_ref, q_raw, q_all, kv_buf, rank, own, sib, got, chip_o, chip_l, hop_o, hop_l, mid_o, mid_l, fin_o, fin_l,
           len_ref, load_sem, len_sem, kv_sem, q_send, q_recv, s_send, s_recv, h_send, h_recv, f_send, f_recv):
    chunks, per, rows, width = q_raw.shape
    half = per // 2
    heads = rows // TOKENS
    tiles = LATENT // LANES
    keys = kv_buf.shape[2]
    chips = group // CORES
    side = chips * rows
    block = per * rows
    relayed = chunks - STRAIGHT
    lot = LANES // block
    me = lax.axis_index('dcp')
    chip, core = me // CORES, me % CORES
    right = lax.rem(chip + 1, chips) * CORES + core
    left = lax.rem(chip + chips - 1, chips) * CORES + core
    far = lax.rem(chip + 2, chips) * CORES + core
    twin = chip * CORES + (CORES - 1 - core)
    scale = (NOPE + ROPE) ** -0.5

    def remote(src, dst, send, recv, to):
        return pltpu.make_async_remote_copy(src_ref=src, dst_ref=dst, send_sem=send, recv_sem=recv,
                                            device_id={'dcp': to}, device_id_type=pl.DeviceIdType.MESH)

    def way(c):
        return lax.rem(c, 2)

    def toward(d):
        return jnp.where(d == 0, right, left)

    def q_copy(c, kind):
        if kind == 0:
            src, dst, to = q_all.at[c, 0], q_all.at[c, 1], right
        elif kind == 1:
            src, dst, to = q_all.at[c, 0], q_all.at[c, 2], left
        elif kind == 2:
            src, dst, to = q_all.at[c, 1, 0], q_all.at[c, 3, 0], right
        elif kind == 3:
            src, dst, to = q_all.at[c, 2, 1], q_all.at[c, 3, 1], left
        else:
            src, dst, to = q_all.at[c, pl.ds(0, chips)], q_all.at[c, pl.ds(chips, chips)], twin
        return remote(src, dst, q_send.at[lax.rem(c, SENDS), kind], q_recv.at[c, kind], to)

    def part_twin(c):
        return remote(sib.at[c], got.at[c], s_send.at[lax.rem(c, SENDS)], s_recv.at[c], twin)

    def hop_copy(c, what):
        src = (chip_o.at[c, 3], chip_l.at[c, 3 // lot])[what]
        dst = (hop_o.at[c], hop_l.at[c])[what]
        return remote(src, dst, h_send.at[lax.rem(c, SENDS), what], h_recv.at[c, what], jnp.where(c >= relayed, far, toward(way(c))))

    def fin_copy(c, kind, what):
        if kind == 0:
            src, to = (mid_o.at[c], mid_l.at[c])[what], toward(way(c))
        else:
            slot = 1 + way(c)
            src, to = (chip_o.at[c, slot], chip_l.at[c, slot // lot])[what], toward(1 - way(c))
        dst = (fin_o.at[c, kind], fin_l.at[c, kind])[what]
        return remote(src, dst, f_send.at[lax.rem(c, SENDS), kind, what], f_recv.at[c, kind, what], to)

    def fin_straight(c, what):
        slot = 2 - way(c)
        src = (chip_o.at[c, slot], chip_l.at[c, slot // lot])[what]
        dst = (fin_o.at[c, 0], fin_l.at[c, 0])[what]
        return remote(src, dst, f_send.at[lax.rem(c, SENDS), 0, what], f_recv.at[c, 0, what], toward(way(c)))

    def kv_copy(c, b):
        slot = lax.rem(c, KV_SLOTS)
        return pltpu.make_async_copy(kv_hbm.at[c * per + b], kv_buf.at[slot, b], kv_sem.at[slot, b])

    def go(make, c, *which):
        @pl.when(c >= SENDS)
        def _():
            make(c - SENDS, *which).wait_send()

        make(c, *which).start()

    def pack(c):
        for b in range(per):
            h, n = b // half, b % half
            for k in range(tiles):
                at = (k * half + n) * rows
                q_all[c, 0, h, at:at + rows] = q_raw[c, b, :, k * LANES:(k + 1) * LANES]
            turn = q_raw[c, b, :, LATENT:].astype(jnp.float32)
            at = tiles * half * rows + n * heads
            both = jnp.concatenate([turn[t * heads:(t + 1) * heads] for t in range(TOKENS)], axis=1)
            q_all[c, 0, h, at:at + heads] = both.astype(jnp.bfloat16)

    def send_own(c):
        for kind in (0, 1):
            go(q_copy, c, kind)

    load = pltpu.make_async_copy(q_hbm, q_raw, load_sem)
    load.start()
    lengths = pltpu.make_async_copy(len_hbm, len_ref, len_sem)
    lengths.start()
    barrier = pltpu.get_barrier_semaphore()
    for peer in (left, right, twin):
        pl.semaphore_signal(barrier, inc=1, device_id={'dcp': peer}, device_id_type=pl.DeviceIdType.MESH)

    r_id = lax.broadcasted_iota(jnp.int32, (rows, keys), 0)
    k_id = lax.broadcasted_iota(jnp.int32, (rows, keys), 1)
    rank[...] = (k_id // PAGE * group + me) * PAGE + k_id % PAGE - r_id // heads

    load.wait()
    for c in range(min(AHEAD, chunks)):
        pack(c)
    pl.semaphore_wait(barrier, 3)
    for c in range(min(AHEAD, chunks)):
        send_own(jnp.int32(c))
    for c in range(min(KV_SLOTS, chunks)):
        for b in range(per):
            kv_copy(c, b).start()
    for c in range(min(AHEAD, chunks), chunks):
        pack(c)

    free_keys = (min_rounds * PAGE) // LANES * LANES

    def scores(c, b):
        h, n = b // half, b % half
        latent = [q_all[c, :, h, (k * half + n) * rows:(k * half + n + 1) * rows] for k in range(tiles)]
        latent = jnp.concatenate([x.reshape(group * rows, LANES) for x in latent], axis=1)
        at = tiles * half * rows + n * heads
        both = q_all[c, :, h, at:at + heads].astype(jnp.float32).reshape(group * heads, LANES)
        turn = jnp.stack([both.reshape(group, heads, LANES), pltpu.roll(both, ROPE, 1).reshape(group, heads, LANES)], axis=1)
        turn = turn.reshape(group * rows, LANES).astype(jnp.bfloat16)[:, :ROPE]
        kv = kv_buf.at[lax.rem(c, KV_SLOTS), b]
        over = (((1,), (1,)), ((), ()))
        s = lax.dot_general(latent, kv[:, :LATENT], over, preferred_element_type=jnp.float32)
        s = s + lax.dot_general(turn, kv[:, LATENT:], over, preferred_element_type=jnp.float32)
        tail = s[:, free_keys:].reshape(group, rows, keys - free_keys)
        limit = len_ref[c * per + b] - TOKENS
        seen = jnp.broadcast_to(rank[:, free_keys:][None], tail.shape) <= limit
        tail = jnp.where(seen, tail, -jnp.inf).reshape(group * rows, keys - free_keys)
        return jnp.concatenate([s[:, :free_keys], tail], axis=1)

    def values(c, b, s):
        top = jnp.max(s, axis=1, keepdims=True)
        p = jnp.exp2((s - top) * (scale * math.log2(math.e)))
        total = jnp.sum(p, axis=1, keepdims=True)
        o = jnp.dot(p.astype(jnp.bfloat16), kv_buf[lax.rem(c, KV_SLOTS), b, :, :LATENT], preferred_element_type=jnp.float32)
        o = o * (1.0 / total)
        lse = jnp.broadcast_to(top * scale + jnp.log(total), (group * rows, LANES))
        keep = lax.rem(c, KEPT)
        own[keep, b, :, :LATENT] = o[:side]
        own[keep, b, :, LATENT:] = lse[:side]
        sib[c, b, :, :LATENT] = o[side:]
        sib[c, b, :, LATENT:] = lse[side:]

    def attend(c):
        ahead = scores(c, 0)
        for b in range(per):
            now = ahead
            if b + 1 < per:
                ahead = scores(c, b + 1)
            values(c, b, now)

    lane_s = lax.broadcasted_iota(jnp.int32, (lot * rows, LANES), 1)
    row_s = lax.broadcasted_iota(jnp.int32, (lot * rows, LANES), 0)
    lane_b = lax.broadcasted_iota(jnp.int32, (block, LANES), 1)
    row_b = lax.broadcasted_iota(jnp.int32, (block, LANES), 0)

    def column(row, slot):
        picked = jnp.where(lane_b == row_b + lax.rem(slot, lot) * block, jnp.broadcast_to(row, (block, LANES)), 0.0)
        return jnp.broadcast_to(jnp.sum(picked, axis=1, keepdims=True), (block, LANES))

    def join_cores(c):
        packed = [jnp.zeros((1, LANES), jnp.float32) for _ in range(chips // lot)]
        keep = lax.rem(c, KEPT)
        for b in range(per):
            o, lse = merge(own[keep, b, :, :LATENT], own[keep, b, :, LATENT:], got[c, b, :, :LATENT], got[c, b, :, LATENT:])
            o = o.astype(jnp.bfloat16)
            for slot in range(chips):
                chip_o[c, slot, b * rows:(b + 1) * rows] = o[slot * rows:(slot + 1) * rows]
            at = row_s // rows * block + b * rows + row_s % rows
            for j in range(chips // lot):
                part = lse[j * lot * rows:(j + 1) * lot * rows]
                packed[j] = packed[j] + jnp.sum(jnp.where(lane_s == at, part, 0.0), axis=0, keepdims=True)
        for j in range(chips // lot):
            chip_l[c, j] = packed[j]

    def join_hop(c):
        slot = 2 - way(c)
        o, lse = merge(chip_o[c, slot].astype(jnp.float32), column(chip_l[c, slot // lot], slot),
                       hop_o[c].astype(jnp.float32), column(hop_l[c], jnp.int32(3)))
        mid_o[c] = o.astype(jnp.bfloat16)
        mid_l[c] = jnp.sum(jnp.where(lane_b == row_b, lse, 0.0), axis=0, keepdims=True)

    def finish(c, parts):
        top = functools.reduce(jnp.maximum, [l for _, l in parts])
        weights = [jnp.exp(l - top) for _, l in parts]
        inv = 1.0 / functools.reduce(jnp.add, weights)
        o = functools.reduce(jnp.add, [part.astype(jnp.float32) * wide(w * inv, LATENT) for (part, _), w in zip(parts, weights)])
        o = o.astype(jnp.bfloat16)
        for b in range(per):
            out_ref[c, b] = o[b * rows:(b + 1) * rows]

    def join_last(c):
        finish(c, [(chip_o[c, 0], column(chip_l[c, 0], jnp.int32(0))), (fin_o[c, 0], column(fin_l[c, 0], jnp.int32(0))),
                   (fin_o[c, 1], column(fin_l[c, 1], 1 + way(c)))])

    def join_straight(c):
        finish(c, [(chip_o[c, 0], column(chip_l[c, 0], jnp.int32(0))), (fin_o[c, 0], column(fin_l[c, 0], 2 - way(c))),
                   (fin_o[c, 1], column(fin_l[c, 1], 1 + way(c))), (hop_o[c], column(hop_l[c], jnp.int32(3)))])

    def stage(t, lag, fn, start=0, stop=chunks):
        c = t - lag

        @pl.when(jnp.logical_and(c >= start, c < stop))
        def _():
            fn(c)

    def spread(c):
        for kind in (0, 1):
            q_copy(c, kind).wait_recv()
        for kind in (2, 3):
            go(q_copy, c, kind)

    def to_twin(c):
        for kind in (2, 3):
            q_copy(c, kind).wait_recv()
        go(q_copy, c, 4)

    def cores_in(c):
        part_twin(c).wait_recv()

    def cores_out(c):
        for what in range(2):
            go(hop_copy, c, what)
            go(fin_copy, c, 1, what)

    def hop_in(c):
        for what in range(2):
            hop_copy(c, what).wait_recv()

    def hop_out(c):
        for what in range(2):
            go(fin_copy, c, 0, what)

    def last_in(c):
        for what in range(2):
            for kind in range(2):
                fin_copy(c, kind, what).wait_recv()

    lag = 3
    joins = ((8, hop_in, join_hop, hop_out), (5, cores_in, join_cores, cores_out))
    final = chunks + lag

    def step(t, carry):
        stage(t, 0, spread)
        stage(t, -AHEAD, send_own)
        stage(t, 2, to_twin)
        c = t - lag
        busy = jnp.logical_and(c >= 0, c < chunks)

        @pl.when(busy)
        def _():
            for late, ready, _, _ in joins:
                stage(t, late, ready)
            q_copy(c, 4).wait_recv()
            for b in range(per):
                kv_copy(c, b).wait()
            for late, _, join, _ in joins:
                old = t - late
                join(jnp.where(old >= 0, old, chunks))
            attend(c)
            go(part_twin, c)
            for late, _, _, pass_on in joins:
                stage(t, late, pass_on)

            @pl.when(c + KV_SLOTS < chunks)
            def _():
                for b in range(per):
                    kv_copy(c + KV_SLOTS, b).start()

        @pl.when(jnp.logical_not(busy))
        def _():
            def cores(c):
                cores_in(c)
                join_cores(c)
                cores_out(c)

            def cores_straight(c):
                cores(c)
                for what in range(2):
                    go(fin_straight, c, what)

            def hop(c):
                hop_in(c)
                join_hop(c)
                hop_out(c)

            def last(c):
                last_in(c)
                join_last(c)

            def last_straight(c):
                last_in(c)
                hop_in(c)
                join_straight(c)

            stage(t, joins[1][0], cores, stop=relayed)
            stage(t, joins[1][0], cores_straight, start=relayed)
            stage(t, joins[0][0], hop, stop=relayed)
            stage(t, final, last, stop=relayed)
            stage(t, final, last_straight, start=relayed)

        return carry

    lengths.wait()
    lax.fori_loop(0, chunks + final, step, 0)
    for c in range(max(chunks - SENDS, 0), chunks):
        c = jnp.int32(c)
        for kind in range(5):
            q_copy(c, kind).wait_send()
        part_twin(c).wait_send()
        for what in range(2):
            hop_copy(c, what).wait_send()
            for kind in range(2):
                fin_copy(c, kind, what).wait_send()


def solution(mesh):
    group = mesh.shape['dcp']
    chips = group // CORES

    def local_step(q_blk, kv_blk, len_blk):
        batch, tokens, heads, width = q_blk.shape
        rounds = kv_blk.shape[1]
        keys = rounds * PAGE
        rows = tokens * heads
        chunks = batch // CHUNK
        block = CHUNK * rows
        side = chips * rows
        bf, f32 = jnp.bfloat16, jnp.float32
        scratch = [
            pltpu.VMEM((chunks, CHUNK, rows, width), bf),
            pltpu.VMEM((chunks, group, 2, CHUNK // 2 * rows * width // LANES, LANES), bf),
            pltpu.VMEM((KV_SLOTS, CHUNK, keys, width), bf),
            pltpu.VMEM((rows, keys), jnp.int32),
            pltpu.VMEM((KEPT, CHUNK, side, LATENT + LANES), f32),
            pltpu.VMEM((chunks, CHUNK, side, LATENT + LANES), f32),
            pltpu.VMEM((chunks + 1, CHUNK, side, LATENT + LANES), f32),
            pltpu.VMEM((chunks + 1, chips, block, LATENT), bf),
            pltpu.VMEM((chunks + 1, chips * block // LANES, 1, LANES), f32),
            pltpu.VMEM((chunks + 1, block, LATENT), bf),
            pltpu.VMEM((chunks + 1, 1, LANES), f32),
            pltpu.VMEM((chunks + 1, block, LATENT), bf),
            pltpu.VMEM((chunks + 1, 1, LANES), f32),
            pltpu.VMEM((chunks + 1, 2, block, LATENT), bf),
            pltpu.VMEM((chunks + 1, 2, 1, LANES), f32),
            pltpu.SMEM((batch,), jnp.int32),
            pltpu.SemaphoreType.DMA,
            pltpu.SemaphoreType.DMA,
            pltpu.SemaphoreType.DMA((KV_SLOTS, CHUNK)),
        ]
        for shape in ((5,), (), (2,), (2, 2)):
            scratch += [pltpu.SemaphoreType.DMA((SENDS, *shape)), pltpu.SemaphoreType.DMA((chunks, *shape))]
        flops = 2 * batch * group * rows * keys * (width + LATENT)
        o = pl.pallas_call(
            functools.partial(kernel, group, rounds // 2 - 1),
            out_shape=jax.ShapeDtypeStruct((chunks, CHUNK, rows, LATENT), bf),
            in_specs=[pl.BlockSpec(memory_space=pltpu.HBM)] * 3,
            out_specs=pl.BlockSpec(memory_space=pltpu.VMEM),
            scratch_shapes=scratch,
            compiler_params=pltpu.CompilerParams(collective_id=0, has_side_effects=True, vmem_limit_bytes=50 * 2**20),
            cost_estimate=pl.CostEstimate(flops=flops, bytes_accessed=kv_blk.size * 2, transcendentals=batch * group * rows * keys),
        )(pltpu.with_memory_space_constraint(len_blk, pltpu.HBM), pltpu.with_memory_space_constraint(q_blk.reshape(chunks, CHUNK, rows, width), pltpu.HBM), kv_blk.reshape(batch, keys, width))
        return o.reshape(batch, tokens, heads, LATENT)

    return jax.shard_map(local_step, mesh=mesh, in_specs=(P('dp', None, 'dcp', None), P('dp', None, 'dcp', None, None), P('dp')), out_specs=P('dp', None, 'dcp', None), check_vma=False)
```

```python
import functools
import math

import jax
import jax.numpy as jnp
from jax import lax
from jax.experimental import pallas as pl
from jax.experimental.pallas import tpu as pltpu
from jax.sharding import PartitionSpec as P

LATENT = 512
ROPE = 64
NOPE = 128
PAGE = 64
TOKENS = 2
CORES = 2
CHUNK = 4
KV_SLOTS = 3
AHEAD = 2
KEPT = 3
SENDS = 4
STRAIGHT = 1
LANES = 128


def wide(col, n):
    return jnp.concatenate([col] * (n // LANES), axis=1)


def merge(o_a, l_a, o_b, l_b):
    top = jnp.maximum(l_a, l_b)
    e_a = jnp.exp(l_a - top)
    e_b = jnp.exp(l_b - top)
    total = e_a + e_b
    inv = 1.0 / total
    n = o_a.shape[1]
    return o_a * wide(e_a * inv, n) + o_b * wide(e_b * inv, n), top + jnp.log(total)


def kernel(group, min_rounds, len_hbm, q_hbm, kv_hbm, out_ref, q_raw, q_all, kv_buf, rank, own, sib, got, chip_o, chip_l, hop_o, hop_l, mid_o, mid_l, fin_o, fin_l,
           len_ref, load_sem, len_sem, kv_sem, q_send, q_recv, s_send, s_recv, h_send, h_recv, f_send, f_recv):
    chunks, per, rows, width = q_raw.shape
    half = per // 2
    heads = rows // TOKENS
    tiles = LATENT // LANES
    keys = kv_buf.shape[2]
    chips = group // CORES
    side = chips * rows
    block = per * rows
    relayed = chunks - STRAIGHT
    lot = LANES // block
    me = lax.axis_index('dcp')
    chip, core = me // CORES, me % CORES
    right = lax.rem(chip + 1, chips) * CORES + core
    left = lax.rem(chip + chips - 1, chips) * CORES + core
    far = lax.rem(chip + 2, chips) * CORES + core
    twin = chip * CORES + (CORES - 1 - core)
    scale = (NOPE + ROPE) ** -0.5

    def remote(src, dst, send, recv, to):
        return pltpu.make_async_remote_copy(src_ref=src, dst_ref=dst, send_sem=send, recv_sem=recv,
                                            device_id={'dcp': to}, device_id_type=pl.DeviceIdType.MESH)

    def way(c):
        return lax.rem(c, 2)

    def toward(d):
        return jnp.where(d == 0, right, left)

    def q_copy(c, kind):
        if kind == 0:
            src, dst, to = q_all.at[c, 0], q_all.at[c, 1], right
        elif kind == 1:
            src, dst, to = q_all.at[c, 0], q_all.at[c, 2], left
        elif kind == 2:
            src, dst, to = q_all.at[c, 1, 0], q_all.at[c, 3, 0], right
        elif kind == 3:
            src, dst, to = q_all.at[c, 2, 1], q_all.at[c, 3, 1], left
        else:
            src, dst, to = q_all.at[c, pl.ds(0, chips)], q_all.at[c, pl.ds(chips, chips)], twin
        return remote(src, dst, q_send.at[lax.rem(c, SENDS), kind], q_recv.at[c, kind], to)

    def part_twin(c):
        return remote(sib.at[c], got.at[c], s_send.at[lax.rem(c, SENDS)], s_recv.at[c], twin)

    def hop_copy(c, what):
        src = (chip_o.at[c, 3], chip_l.at[c, 3 // lot])[what]
        dst = (hop_o.at[c], hop_l.at[c])[what]
        return remote(src, dst, h_send.at[lax.rem(c, SENDS), what], h_recv.at[c, what], jnp.where(c >= relayed, far, toward(way(c))))

    def fin_copy(c, kind, what):
        if kind == 0:
            src, to = (mid_o.at[c], mid_l.at[c])[what], toward(way(c))
        else:
            slot = 1 + way(c)
            src, to = (chip_o.at[c, slot], chip_l.at[c, slot // lot])[what], toward(1 - way(c))
        dst = (fin_o.at[c, kind], fin_l.at[c, kind])[what]
        return remote(src, dst, f_send.at[lax.rem(c, SENDS), kind, what], f_recv.at[c, kind, what], to)

    def fin_straight(c, what):
        slot = 2 - way(c)
        src = (chip_o.at[c, slot], chip_l.at[c, slot // lot])[what]
        dst = (fin_o.at[c, 0], fin_l.at[c, 0])[what]
        return remote(src, dst, f_send.at[lax.rem(c, SENDS), 0, what], f_recv.at[c, 0, what], toward(way(c)))

    def kv_copy(c, b):
        slot = lax.rem(c, KV_SLOTS)
        return pltpu.make_async_copy(kv_hbm.at[c * per + b], kv_buf.at[slot, b], kv_sem.at[slot, b])

    def go(make, c, *which):
        @pl.when(c >= SENDS)
        def _():
            make(c - SENDS, *which).wait_send()

        make(c, *which).start()

    def pack(c):
        for b in range(per):
            h, n = b // half, b % half
            for k in range(tiles):
                at = (k * half + n) * rows
                q_all[c, 0, h, at:at + rows] = q_raw[c, b, :, k * LANES:(k + 1) * LANES]
            turn = q_raw[c, b, :, LATENT:].astype(jnp.float32)
            at = tiles * half * rows + n * heads
            both = jnp.concatenate([turn[t * heads:(t + 1) * heads] for t in range(TOKENS)], axis=1)
            q_all[c, 0, h, at:at + heads] = both.astype(jnp.bfloat16)

    def send_own(c):
        for kind in (0, 1):
            go(q_copy, c, kind)

    load = pltpu.make_async_copy(q_hbm, q_raw, load_sem)
    load.start()
    lengths = pltpu.make_async_copy(len_hbm, len_ref, len_sem)
    lengths.start()
    barrier = pltpu.get_barrier_semaphore()
    for peer in (left, right, twin):
        pl.semaphore_signal(barrier, inc=1, device_id={'dcp': peer}, device_id_type=pl.DeviceIdType.MESH)

    r_id = lax.broadcasted_iota(jnp.int32, (rows, keys), 0)
    k_id = lax.broadcasted_iota(jnp.int32, (rows, keys), 1)
    rank[...] = (k_id // PAGE * group + me) * PAGE + k_id % PAGE - r_id // heads

    load.wait()
    for c in range(min(AHEAD, chunks)):
        pack(c)
    pl.semaphore_wait(barrier, 3)
    for c in range(min(AHEAD, chunks)):
        send_own(jnp.int32(c))
    for c in range(min(KV_SLOTS, chunks)):
        for b in range(per):
            kv_copy(c, b).start()
    for c in range(min(AHEAD, chunks), chunks):
        pack(c)

    free_keys = (min_rounds * PAGE) // LANES * LANES

    def scores(c, b):
        h, n = b // half, b % half
        latent = [q_all[c, :, h, (k * half + n) * rows:(k * half + n + 1) * rows] for k in range(tiles)]
        latent = jnp.concatenate([x.reshape(group * rows, LANES) for x in latent], axis=1)
        at = tiles * half * rows + n * heads
        both = q_all[c, :, h, at:at + heads].astype(jnp.float32).reshape(group * heads, LANES)
        turn = jnp.stack([both.reshape(group, heads, LANES), pltpu.roll(both, ROPE, 1).reshape(group, heads, LANES)], axis=1)
        turn = turn.reshape(group * rows, LANES).astype(jnp.bfloat16)[:, :ROPE]
        kv = kv_buf.at[lax.rem(c, KV_SLOTS), b]
        over = (((1,), (1,)), ((), ()))
        s = lax.dot_general(latent, kv[:, :LATENT], over, preferred_element_type=jnp.float32)
        s = s + lax.dot_general(turn, kv[:, LATENT:], over, preferred_element_type=jnp.float32)
        tail = s[:, free_keys:].reshape(group, rows, keys - free_keys)
        limit = len_ref[c * per + b] - TOKENS
        seen = jnp.broadcast_to(rank[:, free_keys:][None], tail.shape) <= limit
        tail = jnp.where(seen, tail, -jnp.inf).reshape(group * rows, keys - free_keys)
        return jnp.concatenate([s[:, :free_keys], tail], axis=1)

    def values(c, b, s):
        top = jnp.max(s, axis=1, keepdims=True)
        p = jnp.exp2((s - top) * (scale * math.log2(math.e)))
        total = jnp.sum(p, axis=1, keepdims=True)
        o = jnp.dot(p.astype(jnp.bfloat16), kv_buf[lax.rem(c, KV_SLOTS), b, :, :LATENT], preferred_element_type=jnp.float32)
        o = o * (1.0 / total)
        lse = jnp.broadcast_to(top * scale + jnp.log(total), (group * rows, LANES))
        keep = lax.rem(c, KEPT)
        own[keep, b, :, :LATENT] = o[:side]
        own[keep, b, :, LATENT:] = lse[:side]
        sib[c, b, :, :LATENT] = o[side:]
        sib[c, b, :, LATENT:] = lse[side:]

    def attend(c):
        ahead = scores(c, 0)
        for b in range(per):
            now = ahead
            if b + 1 < per:
                ahead = scores(c, b + 1)
            values(c, b, now)

    lane_s = lax.broadcasted_iota(jnp.int32, (lot * rows, LANES), 1)
    row_s = lax.broadcasted_iota(jnp.int32, (lot * rows, LANES), 0)
    lane_b = lax.broadcasted_iota(jnp.int32, (block, LANES), 1)
    row_b = lax.broadcasted_iota(jnp.int32, (block, LANES), 0)

    def column(row, slot):
        picked = jnp.where(lane_b == row_b + lax.rem(slot, lot) * block, jnp.broadcast_to(row, (block, LANES)), 0.0)
        return jnp.broadcast_to(jnp.sum(picked, axis=1, keepdims=True), (block, LANES))

    def join_cores(c):
        packed = [jnp.zeros((1, LANES), jnp.float32) for _ in range(chips // lot)]
        keep = lax.rem(c, KEPT)
        for b in range(per):
            o, lse = merge(own[keep, b, :, :LATENT], own[keep, b, :, LATENT:], got[c, b, :, :LATENT], got[c, b, :, LATENT:])
            o = o.astype(jnp.bfloat16)
            for slot in range(chips):
                chip_o[c, slot, b * rows:(b + 1) * rows] = o[slot * rows:(slot + 1) * rows]
            at = row_s // rows * block + b * rows + row_s % rows
            for j in range(chips // lot):
                part = lse[j * lot * rows:(j + 1) * lot * rows]
                packed[j] = packed[j] + jnp.sum(jnp.where(lane_s == at, part, 0.0), axis=0, keepdims=True)
        for j in range(chips // lot):
            chip_l[c, j] = packed[j]

    def join_hop(c):
        slot = 2 - way(c)
        o, lse = merge(chip_o[c, slot].astype(jnp.float32), column(chip_l[c, slot // lot], slot),
                       hop_o[c].astype(jnp.float32), column(hop_l[c], jnp.int32(3)))
        mid_o[c] = o.astype(jnp.bfloat16)
        mid_l[c] = jnp.sum(jnp.where(lane_b == row_b, lse, 0.0), axis=0, keepdims=True)

    def finish(c, parts):
        top = functools.reduce(jnp.maximum, [l for _, l in parts])
        weights = [jnp.exp(l - top) for _, l in parts]
        inv = 1.0 / functools.reduce(jnp.add, weights)
        o = functools.reduce(jnp.add, [part.astype(jnp.float32) * wide(w * inv, LATENT) for (part, _), w in zip(parts, weights)])
        o = o.astype(jnp.bfloat16)
        for b in range(per):
            out_ref[c, b] = o[b * rows:(b + 1) * rows]

    def join_last(c):
        finish(c, [(chip_o[c, 0], column(chip_l[c, 0], jnp.int32(0))), (fin_o[c, 0], column(fin_l[c, 0], jnp.int32(0))),
                   (fin_o[c, 1], column(fin_l[c, 1], 1 + way(c)))])

    def join_straight(c):
        finish(c, [(chip_o[c, 0], column(chip_l[c, 0], jnp.int32(0))), (fin_o[c, 0], column(fin_l[c, 0], 2 - way(c))),
                   (fin_o[c, 1], column(fin_l[c, 1], 1 + way(c))), (hop_o[c], column(hop_l[c], jnp.int32(3)))])

    def stage(t, lag, fn, start=0, stop=chunks):
        c = t - lag

        @pl.when(jnp.logical_and(c >= start, c < stop))
        def _():
            fn(c)

    def spread(c):
        for kind in (0, 1):
            q_copy(c, kind).wait_recv()
        for kind in (2, 3):
            go(q_copy, c, kind)

    def to_twin(c):
        for kind in (2, 3):
            q_copy(c, kind).wait_recv()
        go(q_copy, c, 4)

    def cores_in(c):
        part_twin(c).wait_recv()

    def cores_out(c):
        for what in range(2):
            go(hop_copy, c, what)
            go(fin_copy, c, 1, what)

    def hop_in(c):
        for what in range(2):
            hop_copy(c, what).wait_recv()

    def hop_out(c):
        for what in range(2):
            go(fin_copy, c, 0, what)

    def last_in(c):
        for what in range(2):
            for kind in range(2):
                fin_copy(c, kind, what).wait_recv()

    lag = 3
    joins = ((8, hop_in, join_hop, hop_out), (5, cores_in, join_cores, cores_out))
    final = chunks + lag

    def step(t, carry):
        stage(t, -AHEAD, send_own)
        stage(t, 0, spread)
        stage(t, 2, to_twin)
        c = t - lag
        busy = jnp.logical_and(c >= 0, c < chunks)

        @pl.when(busy)
        def _():
            for late, ready, _, _ in joins:
                stage(t, late, ready)
            q_copy(c, 4).wait_recv()
            for b in range(per):
                kv_copy(c, b).wait()
            for late, _, join, _ in joins:
                old = t - late
                join(jnp.where(old >= 0, old, chunks))
            attend(c)
            go(part_twin, c)
            for late, _, _, pass_on in joins:
                stage(t, late, pass_on)

            @pl.when(c + KV_SLOTS < chunks)
            def _():
                for b in range(per):
                    kv_copy(c + KV_SLOTS, b).start()

        @pl.when(jnp.logical_not(busy))
        def _():
            def cores(c):
                cores_in(c)
                join_cores(c)
                cores_out(c)

            def cores_straight(c):
                cores(c)
                for what in range(2):
                    go(fin_straight, c, what)

            def hop(c):
                hop_in(c)
                join_hop(c)
                hop_out(c)

            def last(c):
                last_in(c)
                join_last(c)

            def last_straight(c):
                last_in(c)
                hop_in(c)
                join_straight(c)

            stage(t, joins[1][0], cores, stop=relayed)
            stage(t, joins[1][0], cores_straight, start=relayed)
            stage(t, joins[0][0], hop, stop=relayed)
            stage(t, final, last, stop=relayed)
            stage(t, final, last_straight, start=relayed)

        return carry

    lengths.wait()
    lax.fori_loop(0, chunks + final, step, 0)
    for c in range(max(chunks - SENDS, 0), chunks):
        c = jnp.int32(c)
        for kind in range(5):
            q_copy(c, kind).wait_send()
        part_twin(c).wait_send()
        for what in range(2):
            hop_copy(c, what).wait_send()
            for kind in range(2):
                fin_copy(c, kind, what).wait_send()


def solution(mesh):
    group = mesh.shape['dcp']
    chips = group // CORES

    def local_step(q_blk, kv_blk, len_blk):
        batch, tokens, heads, width = q_blk.shape
        rounds = kv_blk.shape[1]
        keys = rounds * PAGE
        rows = tokens * heads
        chunks = batch // CHUNK
        block = CHUNK * rows
        side = chips * rows
        bf, f32 = jnp.bfloat16, jnp.float32
        scratch = [
            pltpu.VMEM((chunks, CHUNK, rows, width), bf),
            pltpu.VMEM((chunks, group, 2, CHUNK // 2 * rows * width // LANES, LANES), bf),
            pltpu.VMEM((KV_SLOTS, CHUNK, keys, width), bf),
            pltpu.VMEM((rows, keys), jnp.int32),
            pltpu.VMEM((KEPT, CHUNK, side, LATENT + LANES), f32),
            pltpu.VMEM((chunks, CHUNK, side, LATENT + LANES), f32),
            pltpu.VMEM((chunks + 1, CHUNK, side, LATENT + LANES), f32),
            pltpu.VMEM((chunks + 1, chips, block, LATENT), bf),
            pltpu.VMEM((chunks + 1, chips * block // LANES, 1, LANES), f32),
            pltpu.VMEM((chunks + 1, block, LATENT), bf),
            pltpu.VMEM((chunks + 1, 1, LANES), f32),
            pltpu.VMEM((chunks + 1, block, LATENT), bf),
            pltpu.VMEM((chunks + 1, 1, LANES), f32),
            pltpu.VMEM((chunks + 1, 2, block, LATENT), bf),
            pltpu.VMEM((chunks + 1, 2, 1, LANES), f32),
            pltpu.SMEM((batch,), jnp.int32),
            pltpu.SemaphoreType.DMA,
            pltpu.SemaphoreType.DMA,
            pltpu.SemaphoreType.DMA((KV_SLOTS, CHUNK)),
        ]
        for shape in ((5,), (), (2,), (2, 2)):
            scratch += [pltpu.SemaphoreType.DMA((SENDS, *shape)), pltpu.SemaphoreType.DMA((chunks, *shape))]
        flops = 2 * batch * group * rows * keys * (width + LATENT)
        o = pl.pallas_call(
            functools.partial(kernel, group, rounds // 2 - 1),
            out_shape=jax.ShapeDtypeStruct((chunks, CHUNK, rows, LATENT), bf),
            in_specs=[pl.BlockSpec(memory_space=pltpu.HBM)] * 3,
            out_specs=pl.BlockSpec(memory_space=pltpu.VMEM),
            scratch_shapes=scratch,
            compiler_params=pltpu.CompilerParams(collective_id=0, has_side_effects=True, vmem_limit_bytes=50 * 2**20),
            cost_estimate=pl.CostEstimate(flops=flops, bytes_accessed=kv_blk.size * 2, transcendentals=batch * group * rows * keys),
        )(pltpu.with_memory_space_constraint(len_blk, pltpu.HBM), pltpu.with_memory_space_constraint(q_blk.reshape(chunks, CHUNK, rows, width), pltpu.HBM), kv_blk.reshape(batch, keys, width))
        return o.reshape(batch, tokens, heads, LATENT)

    return jax.shard_map(local_step, mesh=mesh, in_specs=(P('dp', None, 'dcp', None), P('dp', None, 'dcp', None, None), P('dp')), out_specs=P('dp', None, 'dcp', None), check_vma=False)
```

```python
import functools
import math

import jax
import jax.numpy as jnp
from jax import lax
from jax.experimental import pallas as pl
from jax.experimental.pallas import tpu as pltpu
from jax.sharding import PartitionSpec as P

LATENT = 512
ROPE = 64
NOPE = 128
PAGE = 64
TOKENS = 2
CORES = 2
CHUNK = 4
KV_SLOTS = 3
AHEAD = 2
KEPT = 3
SENDS = 4
STRAIGHT = 1
LANES = 128


def wide(col, n):
    return jnp.concatenate([col] * (n // LANES), axis=1)


def merge(o_a, l_a, o_b, l_b):
    top = jnp.maximum(l_a, l_b)
    e_a = jnp.exp(l_a - top)
    e_b = jnp.exp(l_b - top)
    total = e_a + e_b
    inv = 1.0 / total
    n = o_a.shape[1]
    return o_a * wide(e_a * inv, n) + o_b * wide(e_b * inv, n), top + jnp.log(total)


def kernel(group, min_rounds, len_hbm, q_hbm, kv_hbm, out_ref, q_raw, q_all, kv_buf, rank, own, sib, got, chip_o, chip_l, hop_o, hop_l, mid_o, mid_l, fin_o, fin_l,
           turned, len_ref, load_sem, len_sem, kv_sem, q_send, q_recv, s_send, s_recv, h_send, h_recv, f_send, f_recv):
    chunks, per, rows, width = q_raw.shape
    half = per // 2
    heads = rows // TOKENS
    tiles = LATENT // LANES
    keys = kv_buf.shape[2]
    chips = group // CORES
    side = chips * rows
    block = per * rows
    relayed = chunks - STRAIGHT
    lot = LANES // block
    me = lax.axis_index('dcp')
    chip, core = me // CORES, me % CORES
    right = lax.rem(chip + 1, chips) * CORES + core
    left = lax.rem(chip + chips - 1, chips) * CORES + core
    far = lax.rem(chip + 2, chips) * CORES + core
    twin = chip * CORES + (CORES - 1 - core)
    scale = (NOPE + ROPE) ** -0.5

    def remote(src, dst, send, recv, to):
        return pltpu.make_async_remote_copy(src_ref=src, dst_ref=dst, send_sem=send, recv_sem=recv,
                                            device_id={'dcp': to}, device_id_type=pl.DeviceIdType.MESH)

    def way(c):
        return lax.rem(c, 2)

    def toward(d):
        return jnp.where(d == 0, right, left)

    def q_copy(c, kind):
        if kind == 0:
            src, dst, to = q_all.at[c, 0], q_all.at[c, 1], right
        elif kind == 1:
            src, dst, to = q_all.at[c, 0], q_all.at[c, 2], left
        elif kind == 2:
            src, dst, to = q_all.at[c, 1, 0], q_all.at[c, 3, 0], right
        elif kind == 3:
            src, dst, to = q_all.at[c, 2, 1], q_all.at[c, 3, 1], left
        else:
            src, dst, to = q_all.at[c, pl.ds(0, chips)], q_all.at[c, pl.ds(chips, chips)], twin
        return remote(src, dst, q_send.at[lax.rem(c, SENDS), kind], q_recv.at[c, kind], to)

    def part_twin(c):
        return remote(sib.at[c], got.at[c], s_send.at[lax.rem(c, SENDS)], s_recv.at[c], twin)

    def hop_copy(c, what):
        src = (chip_o.at[c, 3], chip_l.at[c, 3 // lot])[what]
        dst = (hop_o.at[c], hop_l.at[c])[what]
        return remote(src, dst, h_send.at[lax.rem(c, SENDS), what], h_recv.at[c, what], jnp.where(c >= relayed, far, toward(way(c))))

    def fin_copy(c, kind, what):
        if kind == 0:
            src, to = (mid_o.at[c], mid_l.at[c])[what], toward(way(c))
        else:
            slot = 1 + way(c)
            src, to = (chip_o.at[c, slot], chip_l.at[c, slot // lot])[what], toward(1 - way(c))
        dst = (fin_o.at[c, kind], fin_l.at[c, kind])[what]
        return remote(src, dst, f_send.at[lax.rem(c, SENDS), kind, what], f_recv.at[c, kind, what], to)

    def fin_straight(c, what):
        slot = 2 - way(c)
        src = (chip_o.at[c, slot], chip_l.at[c, slot // lot])[what]
        dst = (fin_o.at[c, 0], fin_l.at[c, 0])[what]
        return remote(src, dst, f_send.at[lax.rem(c, SENDS), 0, what], f_recv.at[c, 0, what], toward(way(c)))

    def kv_copy(c, b):
        slot = lax.rem(c, KV_SLOTS)
        return pltpu.make_async_copy(kv_hbm.at[c * per + b], kv_buf.at[slot, b], kv_sem.at[slot, b])

    def go(make, c, *which):
        @pl.when(c >= SENDS)
        def _():
            make(c - SENDS, *which).wait_send()

        make(c, *which).start()

    def pack(c):
        for b in range(per):
            h, n = b // half, b % half
            for k in range(tiles):
                at = (k * half + n) * rows
                q_all[c, 0, h, at:at + rows] = q_raw[c, b, :, k * LANES:(k + 1) * LANES]
            turn = q_raw[c, b, :, LATENT:].astype(jnp.float32)
            at = tiles * half * rows + n * heads
            both = jnp.concatenate([turn[t * heads:(t + 1) * heads] for t in range(TOKENS)], axis=1)
            q_all[c, 0, h, at:at + heads] = both.astype(jnp.bfloat16)

    def send_own(c):
        for kind in (0, 1):
            go(q_copy, c, kind)

    load = pltpu.make_async_copy(q_hbm, q_raw, load_sem)
    load.start()
    lengths = pltpu.make_async_copy(len_hbm, len_ref, len_sem)
    lengths.start()
    barrier = pltpu.get_barrier_semaphore()
    for peer in (left, right, twin):
        pl.semaphore_signal(barrier, inc=1, device_id={'dcp': peer}, device_id_type=pl.DeviceIdType.MESH)

    r_id = lax.broadcasted_iota(jnp.int32, (rows, keys), 0)
    k_id = lax.broadcasted_iota(jnp.int32, (rows, keys), 1)
    rank[...] = (k_id // PAGE * group + me) * PAGE + k_id % PAGE - r_id // heads

    load.wait()
    for c in range(min(AHEAD, chunks)):
        pack(c)
    pl.semaphore_wait(barrier, 3)
    for c in range(min(AHEAD, chunks)):
        send_own(jnp.int32(c))
    for c in range(min(KV_SLOTS, chunks)):
        for b in range(per):
            kv_copy(c, b).start()
    for c in range(min(AHEAD, chunks), chunks):
        pack(c)

    free_keys = (min_rounds * PAGE) // LANES * LANES

    def scores(c, b):
        h, n = b // half, b % half
        latent = [q_all[c, :, h, (k * half + n) * rows:(k * half + n + 1) * rows] for k in range(tiles)]
        latent = jnp.concatenate([x.reshape(group * rows, LANES) for x in latent], axis=1)
        at = tiles * half * rows + n * heads
        both = q_all[c, :, h, at:at + heads].astype(jnp.float32).reshape(group * heads, LANES)
        turn = jnp.stack([both.reshape(group, heads, LANES), pltpu.roll(both, ROPE, 1).reshape(group, heads, LANES)], axis=1)
        turn = turn.reshape(group * rows, LANES).astype(jnp.bfloat16)[:, :ROPE]
        kv = kv_buf.at[lax.rem(c, KV_SLOTS), b]
        over = (((1,), (1,)), ((), ()))
        flat = keys - turned.shape[2]
        turned[b % 3] = kv[flat:, :LATENT].T
        s = lax.dot_general(latent, kv[:flat, :LATENT], over, preferred_element_type=jnp.float32)
        s2 = jnp.dot(latent, turned[b % 3], preferred_element_type=jnp.float32)
        s = jnp.concatenate([s, s2], axis=1)
        s = s + lax.dot_general(turn, kv[:, LATENT:], over, preferred_element_type=jnp.float32)
        tail = s[:, free_keys:].reshape(group, rows, keys - free_keys)
        limit = len_ref[c * per + b] - TOKENS
        seen = jnp.broadcast_to(rank[:, free_keys:][None], tail.shape) <= limit
        tail = jnp.where(seen, tail, -jnp.inf).reshape(group * rows, keys - free_keys)
        return jnp.concatenate([s[:, :free_keys], tail], axis=1)

    def values(c, b, s):
        top = jnp.max(s, axis=1, keepdims=True)
        p = jnp.exp2((s - top) * (scale * math.log2(math.e)))
        total = jnp.sum(p, axis=1, keepdims=True)
        o = jnp.dot(p.astype(jnp.bfloat16), kv_buf[lax.rem(c, KV_SLOTS), b, :, :LATENT], preferred_element_type=jnp.float32)
        o = o * (1.0 / total)
        lse = jnp.broadcast_to(top * scale + jnp.log(total), (group * rows, LANES))
        keep = lax.rem(c, KEPT)
        own[keep, b, :, :LATENT] = o[:side]
        own[keep, b, :, LATENT:] = lse[:side]
        sib[c, b, :, :LATENT] = o[side:]
        sib[c, b, :, LATENT:] = lse[side:]

    def attend(c):
        queue = [scores(c, 0), scores(c, 1)]
        for b in range(per):
            if b + 2 < per:
                queue.append(scores(c, b + 2))
            values(c, b, queue[b])

    lane_s = lax.broadcasted_iota(jnp.int32, (lot * rows, LANES), 1)
    row_s = lax.broadcasted_iota(jnp.int32, (lot * rows, LANES), 0)
    lane_b = lax.broadcasted_iota(jnp.int32, (block, LANES), 1)
    row_b = lax.broadcasted_iota(jnp.int32, (block, LANES), 0)

    def column(row, slot):
        picked = jnp.where(lane_b == row_b + lax.rem(slot, lot) * block, jnp.broadcast_to(row, (block, LANES)), 0.0)
        return jnp.broadcast_to(jnp.sum(picked, axis=1, keepdims=True), (block, LANES))

    def join_cores(c):
        packed = [jnp.zeros((1, LANES), jnp.float32) for _ in range(chips // lot)]
        keep = lax.rem(c, KEPT)
        for b in range(per):
            o, lse = merge(own[keep, b, :, :LATENT], own[keep, b, :, LATENT:], got[c, b, :, :LATENT], got[c, b, :, LATENT:])
            o = o.astype(jnp.bfloat16)
            for slot in range(chips):
                chip_o[c, slot, b * rows:(b + 1) * rows] = o[slot * rows:(slot + 1) * rows]
            at = row_s // rows * block + b * rows + row_s % rows
            for j in range(chips // lot):
                part = lse[j * lot * rows:(j + 1) * lot * rows]
                packed[j] = packed[j] + jnp.sum(jnp.where(lane_s == at, part, 0.0), axis=0, keepdims=True)
        for j in range(chips // lot):
            chip_l[c, j] = packed[j]

    def join_hop(c):
        slot = 2 - way(c)
        o, lse = merge(chip_o[c, slot].astype(jnp.float32), column(chip_l[c, slot // lot], slot),
                       hop_o[c].astype(jnp.float32), column(hop_l[c], jnp.int32(3)))
        mid_o[c] = o.astype(jnp.bfloat16)
        mid_l[c] = jnp.sum(jnp.where(lane_b == row_b, lse, 0.0), axis=0, keepdims=True)

    def finish(c, parts):
        top = functools.reduce(jnp.maximum, [l for _, l in parts])
        weights = [jnp.exp(l - top) for _, l in parts]
        inv = 1.0 / functools.reduce(jnp.add, weights)
        o = functools.reduce(jnp.add, [part.astype(jnp.float32) * wide(w * inv, LATENT) for (part, _), w in zip(parts, weights)])
        o = o.astype(jnp.bfloat16)
        for b in range(per):
            out_ref[c, b] = o[b * rows:(b + 1) * rows]

    def join_last(c):
        finish(c, [(chip_o[c, 0], column(chip_l[c, 0], jnp.int32(0))), (fin_o[c, 0], column(fin_l[c, 0], jnp.int32(0))),
                   (fin_o[c, 1], column(fin_l[c, 1], 1 + way(c)))])

    def join_straight(c):
        finish(c, [(chip_o[c, 0], column(chip_l[c, 0], jnp.int32(0))), (fin_o[c, 0], column(fin_l[c, 0], 2 - way(c))),
                   (fin_o[c, 1], column(fin_l[c, 1], 1 + way(c))), (hop_o[c], column(hop_l[c], jnp.int32(3)))])

    def stage(t, lag, fn, start=0, stop=chunks):
        c = t - lag

        @pl.when(jnp.logical_and(c >= start, c < stop))
        def _():
            fn(c)

    def spread(c):
        for kind in (0, 1):
            q_copy(c, kind).wait_recv()
        for kind in (2, 3):
            go(q_copy, c, kind)

    def to_twin(c):
        for kind in (2, 3):
            q_copy(c, kind).wait_recv()
        go(q_copy, c, 4)

    def cores_in(c):
        part_twin(c).wait_recv()

    def cores_out(c):
        for what in range(2):
            go(hop_copy, c, what)
            go(fin_copy, c, 1, what)

    def hop_in(c):
        for what in range(2):
            hop_copy(c, what).wait_recv()

    def hop_out(c):
        for what in range(2):
            go(fin_copy, c, 0, what)

    def last_in(c):
        for what in range(2):
            for kind in range(2):
                fin_copy(c, kind, what).wait_recv()

    lag = 3
    joins = ((8, hop_in, join_hop, hop_out), (5, cores_in, join_cores, cores_out))
    final = chunks + lag

    def step(t, carry):
        stage(t, -AHEAD, send_own)
        stage(t, 0, spread)
        stage(t, 2, to_twin)
        c = t - lag
        busy = jnp.logical_and(c >= 0, c < chunks)

        @pl.when(busy)
        def _():
            for late, ready, _, _ in joins:
                stage(t, late, ready)
            q_copy(c, 4).wait_recv()
            for b in range(per):
                kv_copy(c, b).wait()
            for late, _, join, _ in joins:
                old = t - late
                join(jnp.where(old >= 0, old, chunks))
            attend(c)
            go(part_twin, c)
            for late, _, _, pass_on in joins:
                stage(t, late, pass_on)

            @pl.when(c + KV_SLOTS < chunks)
            def _():
                for b in range(per):
                    kv_copy(c + KV_SLOTS, b).start()

        @pl.when(jnp.logical_not(busy))
        def _():
            def cores(c):
                cores_in(c)
                join_cores(c)
                cores_out(c)

            def cores_straight(c):
                cores(c)
                for what in range(2):
                    go(fin_straight, c, what)

            def hop(c):
                hop_in(c)
                join_hop(c)
                hop_out(c)

            def last(c):
                last_in(c)
                join_last(c)

            def last_straight(c):
                last_in(c)
                hop_in(c)
                join_straight(c)

            stage(t, joins[1][0], cores, stop=relayed)
            stage(t, joins[1][0], cores_straight, start=relayed)
            stage(t, joins[0][0], hop, stop=relayed)
            stage(t, final, last, stop=relayed)
            stage(t, final, last_straight, start=relayed)

        return carry

    lengths.wait()
    lax.fori_loop(0, chunks + final, step, 0)
    for c in range(max(chunks - SENDS, 0), chunks):
        c = jnp.int32(c)
        for kind in range(5):
            q_copy(c, kind).wait_send()
        part_twin(c).wait_send()
        for what in range(2):
            hop_copy(c, what).wait_send()
            for kind in range(2):
                fin_copy(c, kind, what).wait_send()


def solution(mesh):
    group = mesh.shape['dcp']
    chips = group // CORES

    def local_step(q_blk, kv_blk, len_blk):
        batch, tokens, heads, width = q_blk.shape
        rounds = kv_blk.shape[1]
        keys = rounds * PAGE
        rows = tokens * heads
        chunks = batch // CHUNK
        block = CHUNK * rows
        side = chips * rows
        bf, f32 = jnp.bfloat16, jnp.float32
        scratch = [
            pltpu.VMEM((chunks, CHUNK, rows, width), bf),
            pltpu.VMEM((chunks, group, 2, CHUNK // 2 * rows * width // LANES, LANES), bf),
            pltpu.VMEM((KV_SLOTS, CHUNK, keys, width), bf),
            pltpu.VMEM((rows, keys), jnp.int32),
            pltpu.VMEM((KEPT, CHUNK, side, LATENT + LANES), f32),
            pltpu.VMEM((chunks, CHUNK, side, LATENT + LANES), f32),
            pltpu.VMEM((chunks + 1, CHUNK, side, LATENT + LANES), f32),
            pltpu.VMEM((chunks + 1, chips, block, LATENT), bf),
            pltpu.VMEM((chunks + 1, chips * block // LANES, 1, LANES), f32),
            pltpu.VMEM((chunks + 1, block, LATENT), bf),
            pltpu.VMEM((chunks + 1, 1, LANES), f32),
            pltpu.VMEM((chunks + 1, block, LATENT), bf),
            pltpu.VMEM((chunks + 1, 1, LANES), f32),
            pltpu.VMEM((chunks + 1, 2, block, LATENT), bf),
            pltpu.VMEM((chunks + 1, 2, 1, LANES), f32),
            pltpu.VMEM((3, LATENT, keys // 2), bf),
            pltpu.SMEM((batch,), jnp.int32),
            pltpu.SemaphoreType.DMA,
            pltpu.SemaphoreType.DMA,
            pltpu.SemaphoreType.DMA((KV_SLOTS, CHUNK)),
        ]
        for shape in ((5,), (), (2,), (2, 2)):
            scratch += [pltpu.SemaphoreType.DMA((SENDS, *shape)), pltpu.SemaphoreType.DMA((chunks, *shape))]
        flops = 2 * batch * group * rows * keys * (width + LATENT)
        o = pl.pallas_call(
            functools.partial(kernel, group, rounds // 2 - 1),
            out_shape=jax.ShapeDtypeStruct((chunks, CHUNK, rows, LATENT), bf),
            in_specs=[pl.BlockSpec(memory_space=pltpu.HBM)] * 3,
            out_specs=pl.BlockSpec(memory_space=pltpu.VMEM),
            scratch_shapes=scratch,
            compiler_params=pltpu.CompilerParams(collective_id=0, has_side_effects=True, vmem_limit_bytes=50 * 2**20),
            cost_estimate=pl.CostEstimate(flops=flops, bytes_accessed=kv_blk.size * 2, transcendentals=batch * group * rows * keys),
        )(pltpu.with_memory_space_constraint(len_blk, pltpu.HBM), pltpu.with_memory_space_constraint(q_blk.reshape(chunks, CHUNK, rows, width), pltpu.HBM), kv_blk.reshape(batch, keys, width))
        return o.reshape(batch, tokens, heads, LATENT)

    return jax.shard_map(local_step, mesh=mesh, in_specs=(P('dp', None, 'dcp', None), P('dp', None, 'dcp', None, None), P('dp')), out_specs=P('dp', None, 'dcp', None), check_vma=False)
```

```python
import functools
import math

import jax
import jax.numpy as jnp
from jax import lax
from jax.experimental import pallas as pl
from jax.experimental.pallas import tpu as pltpu
from jax.sharding import PartitionSpec as P

LATENT = 512
ROPE = 64
NOPE = 128
PAGE = 64
TOKENS = 2
CORES = 2
CHUNK = 4
KV_SLOTS = 3
AHEAD = 2
KEPT = 3
SENDS = 4
STRAIGHT = 0
LANES = 128


def wide(col, n):
    return jnp.concatenate([col] * (n // LANES), axis=1)


def merge(o_a, l_a, o_b, l_b):
    top = jnp.maximum(l_a, l_b)
    e_a = jnp.exp(l_a - top)
    e_b = jnp.exp(l_b - top)
    total = e_a + e_b
    inv = 1.0 / total
    n = o_a.shape[1]
    return o_a * wide(e_a * inv, n) + o_b * wide(e_b * inv, n), top + jnp.log(total)


def kernel(group, min_rounds, len_hbm, q_hbm, kv_hbm, out_ref, q_raw, q_all, kv_buf, rank, own, sib, got, chip_o, chip_l, hop_o, hop_l, mid_o, mid_l, fin_o, fin_l,
           turned, len_ref, load_sem, len_sem, kv_sem, q_send, q_recv, s_send, s_recv, h_send, h_recv, f_send, f_recv):
    chunks, per, rows, width = q_raw.shape
    half = per // 2
    heads = rows // TOKENS
    tiles = LATENT // LANES
    keys = kv_buf.shape[2]
    chips = group // CORES
    side = chips * rows
    block = per * rows
    relayed = chunks - STRAIGHT
    lot = LANES // block
    me = lax.axis_index('dcp')
    chip, core = me // CORES, me % CORES
    right = lax.rem(chip + 1, chips) * CORES + core
    left = lax.rem(chip + chips - 1, chips) * CORES + core
    far = lax.rem(chip + 2, chips) * CORES + core
    twin = chip * CORES + (CORES - 1 - core)
    scale = (NOPE + ROPE) ** -0.5

    def remote(src, dst, send, recv, to):
        return pltpu.make_async_remote_copy(src_ref=src, dst_ref=dst, send_sem=send, recv_sem=recv,
                                            device_id={'dcp': to}, device_id_type=pl.DeviceIdType.MESH)

    def way(c):
        return lax.rem(c, 2)

    def toward(d):
        return jnp.where(d == 0, right, left)

    def q_copy(c, kind):
        if kind == 0:
            src, dst, to = q_all.at[c, 0], q_all.at[c, 1], right
        elif kind == 1:
            src, dst, to = q_all.at[c, 0], q_all.at[c, 2], left
        elif kind == 2:
            src, dst, to = q_all.at[c, 1, 0], q_all.at[c, 3, 0], right
        elif kind == 3:
            src, dst, to = q_all.at[c, 2, 1], q_all.at[c, 3, 1], left
        else:
            src, dst, to = q_all.at[c, pl.ds(0, chips)], q_all.at[c, pl.ds(chips, chips)], twin
        return remote(src, dst, q_send.at[lax.rem(c, SENDS), kind], q_recv.at[c, kind], to)

    def part_twin(c):
        return remote(sib.at[c], got.at[c], s_send.at[lax.rem(c, SENDS)], s_recv.at[c], twin)

    def hop_copy(c, what):
        src = (chip_o.at[c, 3], chip_l.at[c, 3 // lot])[what]
        dst = (hop_o.at[c], hop_l.at[c])[what]
        return remote(src, dst, h_send.at[lax.rem(c, SENDS), what], h_recv.at[c, what], jnp.where(c >= relayed, far, toward(way(c))))

    def fin_copy(c, kind, what):
        if kind == 0:
            src, to = (mid_o.at[c], mid_l.at[c])[what], toward(way(c))
        else:
            slot = 1 + way(c)
            src, to = (chip_o.at[c, slot], chip_l.at[c, slot // lot])[what], toward(1 - way(c))
        dst = (fin_o.at[c, kind], fin_l.at[c, kind])[what]
        return remote(src, dst, f_send.at[lax.rem(c, SENDS), kind, what], f_recv.at[c, kind, what], to)

    def fin_straight(c, what):
        slot = 2 - way(c)
        src = (chip_o.at[c, slot], chip_l.at[c, slot // lot])[what]
        dst = (fin_o.at[c, 0], fin_l.at[c, 0])[what]
        return remote(src, dst, f_send.at[lax.rem(c, SENDS), 0, what], f_recv.at[c, 0, what], toward(way(c)))

    def kv_copy(c, b):
        slot = lax.rem(c, KV_SLOTS)
        return pltpu.make_async_copy(kv_hbm.at[c * per + b], kv_buf.at[slot, b], kv_sem.at[slot, b])

    def go(make, c, *which):
        @pl.when(c >= SENDS)
        def _():
            make(c - SENDS, *which).wait_send()

        make(c, *which).start()

    def pack(c):
        for b in range(per):
            h, n = b // half, b % half
            for k in range(tiles):
                at = (k * half + n) * rows
                q_all[c, 0, h, at:at + rows] = q_raw[c, b, :, k * LANES:(k + 1) * LANES]
            turn = q_raw[c, b, :, LATENT:].astype(jnp.float32)
            at = tiles * half * rows + n * heads
            both = jnp.concatenate([turn[t * heads:(t + 1) * heads] for t in range(TOKENS)], axis=1)
            q_all[c, 0, h, at:at + heads] = both.astype(jnp.bfloat16)

    def send_own(c):
        for kind in (0, 1):
            go(q_copy, c, kind)

    load = pltpu.make_async_copy(q_hbm, q_raw, load_sem)
    load.start()
    lengths = pltpu.make_async_copy(len_hbm, len_ref, len_sem)
    lengths.start()
    barrier = pltpu.get_barrier_semaphore()
    for peer in (left, right, twin):
        pl.semaphore_signal(barrier, inc=1, device_id={'dcp': peer}, device_id_type=pl.DeviceIdType.MESH)

    r_id = lax.broadcasted_iota(jnp.int32, (rows, keys), 0)
    k_id = lax.broadcasted_iota(jnp.int32, (rows, keys), 1)
    rank[...] = (k_id // PAGE * group + me) * PAGE + k_id % PAGE - r_id // heads

    load.wait()
    for c in range(min(AHEAD, chunks)):
        pack(c)
    pl.semaphore_wait(barrier, 3)
    for c in range(min(AHEAD, chunks)):
        send_own(jnp.int32(c))
    for c in range(min(KV_SLOTS, chunks)):
        for b in range(per):
            kv_copy(c, b).start()
    for c in range(min(AHEAD, chunks), chunks):
        pack(c)

    free_keys = (min_rounds * PAGE) // LANES * LANES

    def scores(c, b):
        h, n = b // half, b % half
        latent = [q_all[c, :, h, (k * half + n) * rows:(k * half + n + 1) * rows] for k in range(tiles)]
        latent = jnp.concatenate([x.reshape(group * rows, LANES) for x in latent], axis=1)
        at = tiles * half * rows + n * heads
        both = q_all[c, :, h, at:at + heads].astype(jnp.float32).reshape(group * heads, LANES)
        turn = jnp.stack([both.reshape(group, heads, LANES), pltpu.roll(both, ROPE, 1).reshape(group, heads, LANES)], axis=1)
        turn = turn.reshape(group * rows, LANES).astype(jnp.bfloat16)[:, :ROPE]
        kv = kv_buf.at[lax.rem(c, KV_SLOTS), b]
        over = (((1,), (1,)), ((), ()))
        flat = keys - turned.shape[2]
        turned[b % 3] = kv[flat:, :LATENT].T
        s = lax.dot_general(latent, kv[:flat, :LATENT], over, preferred_element_type=jnp.float32)
        s2 = jnp.dot(latent, turned[b % 3], preferred_element_type=jnp.float32)
        s = jnp.concatenate([s, s2], axis=1)
        s = s + lax.dot_general(turn, kv[:, LATENT:], over, preferred_element_type=jnp.float32)
        tail = s[:, free_keys:].reshape(group, rows, keys - free_keys)
        limit = len_ref[c * per + b] - TOKENS
        seen = jnp.broadcast_to(rank[:, free_keys:][None], tail.shape) <= limit
        tail = jnp.where(seen, tail, -jnp.inf).reshape(group * rows, keys - free_keys)
        return jnp.concatenate([s[:, :free_keys], tail], axis=1)

    def values(c, b, s):
        top = jnp.max(s, axis=1, keepdims=True)
        p = jnp.exp2((s - top) * (scale * math.log2(math.e)))
        total = jnp.sum(p, axis=1, keepdims=True)
        o = jnp.dot(p.astype(jnp.bfloat16), kv_buf[lax.rem(c, KV_SLOTS), b, :, :LATENT], preferred_element_type=jnp.float32)
        o = o * (1.0 / total)
        lse = jnp.broadcast_to(top * scale + jnp.log(total), (group * rows, LANES))
        keep = lax.rem(c, KEPT)
        own[keep, b, :, :LATENT] = o[:side]
        own[keep, b, :, LATENT:] = lse[:side]
        sib[c, b, :, :LATENT] = o[side:]
        sib[c, b, :, LATENT:] = lse[side:]

    def attend(c):
        queue = [scores(c, 0), scores(c, 1)]
        for b in range(per):
            if b + 2 < per:
                queue.append(scores(c, b + 2))
            values(c, b, queue[b])

    lane_s = lax.broadcasted_iota(jnp.int32, (lot * rows, LANES), 1)
    row_s = lax.broadcasted_iota(jnp.int32, (lot * rows, LANES), 0)
    lane_b = lax.broadcasted_iota(jnp.int32, (block, LANES), 1)
    row_b = lax.broadcasted_iota(jnp.int32, (block, LANES), 0)

    def column(row, slot):
        picked = jnp.where(lane_b == row_b + lax.rem(slot, lot) * block, jnp.broadcast_to(row, (block, LANES)), 0.0)
        return jnp.broadcast_to(jnp.sum(picked, axis=1, keepdims=True), (block, LANES))

    def join_cores(c):
        packed = [jnp.zeros((1, LANES), jnp.float32) for _ in range(chips // lot)]
        keep = lax.rem(c, KEPT)
        for b in range(per):
            o, lse = merge(own[keep, b, :, :LATENT], own[keep, b, :, LATENT:], got[c, b, :, :LATENT], got[c, b, :, LATENT:])
            o = o.astype(jnp.bfloat16)
            for slot in range(chips):
                chip_o[c, slot, b * rows:(b + 1) * rows] = o[slot * rows:(slot + 1) * rows]
            at = row_s // rows * block + b * rows + row_s % rows
            for j in range(chips // lot):
                part = lse[j * lot * rows:(j + 1) * lot * rows]
                packed[j] = packed[j] + jnp.sum(jnp.where(lane_s == at, part, 0.0), axis=0, keepdims=True)
        for j in range(chips // lot):
            chip_l[c, j] = packed[j]

    def join_hop(c):
        slot = 2 - way(c)
        o, lse = merge(chip_o[c, slot].astype(jnp.float32), column(chip_l[c, slot // lot], slot),
                       hop_o[c].astype(jnp.float32), column(hop_l[c], jnp.int32(3)))
        mid_o[c] = o.astype(jnp.bfloat16)
        mid_l[c] = jnp.sum(jnp.where(lane_b == row_b, lse, 0.0), axis=0, keepdims=True)

    def finish(c, parts):
        top = functools.reduce(jnp.maximum, [l for _, l in parts])
        weights = [jnp.exp(l - top) for _, l in parts]
        inv = 1.0 / functools.reduce(jnp.add, weights)
        o = functools.reduce(jnp.add, [part.astype(jnp.float32) * wide(w * inv, LATENT) for (part, _), w in zip(parts, weights)])
        o = o.astype(jnp.bfloat16)
        for b in range(per):
            out_ref[c, b] = o[b * rows:(b + 1) * rows]

    def join_last(c):
        finish(c, [(chip_o[c, 0], column(chip_l[c, 0], jnp.int32(0))), (fin_o[c, 0], column(fin_l[c, 0], jnp.int32(0))),
                   (fin_o[c, 1], column(fin_l[c, 1], 1 + way(c)))])

    def join_straight(c):
        finish(c, [(chip_o[c, 0], column(chip_l[c, 0], jnp.int32(0))), (fin_o[c, 0], column(fin_l[c, 0], 2 - way(c))),
                   (fin_o[c, 1], column(fin_l[c, 1], 1 + way(c))), (hop_o[c], column(hop_l[c], jnp.int32(3)))])

    def stage(t, lag, fn, start=0, stop=chunks):
        c = t - lag

        @pl.when(jnp.logical_and(c >= start, c < stop))
        def _():
            fn(c)

    def spread(c):
        for kind in (0, 1):
            q_copy(c, kind).wait_recv()
        for kind in (2, 3):
            go(q_copy, c, kind)

    def to_twin(c):
        for kind in (2, 3):
            q_copy(c, kind).wait_recv()
        go(q_copy, c, 4)

    def cores_in(c):
        part_twin(c).wait_recv()

    def cores_out(c):
        for what in range(2):
            go(hop_copy, c, what)
            go(fin_copy, c, 1, what)

    def hop_in(c):
        for what in range(2):
            hop_copy(c, what).wait_recv()

    def hop_out(c):
        for what in range(2):
            go(fin_copy, c, 0, what)

    def last_in(c):
        for what in range(2):
            for kind in range(2):
                fin_copy(c, kind, what).wait_recv()

    lag = 3
    joins = ((8, hop_in, join_hop, hop_out), (5, cores_in, join_cores, cores_out))
    final = max(chunks + lag, joins[0][0] + 3)

    def step(t, carry):
        stage(t, -AHEAD, send_own)
        stage(t, 0, spread)
        stage(t, 2, to_twin)
        c = t - lag
        busy = jnp.logical_and(c >= 0, c < chunks)

        @pl.when(busy)
        def _():
            for late, ready, _, _ in joins:
                stage(t, late, ready)
            q_copy(c, 4).wait_recv()
            for b in range(per):
                kv_copy(c, b).wait()
            for late, _, join, _ in joins:
                old = t - late
                join(jnp.where(old >= 0, old, chunks))
            attend(c)
            go(part_twin, c)
            for late, _, _, pass_on in joins:
                stage(t, late, pass_on)

            @pl.when(c + KV_SLOTS < chunks)
            def _():
                for b in range(per):
                    kv_copy(c + KV_SLOTS, b).start()

        @pl.when(jnp.logical_not(busy))
        def _():
            def cores(c):
                cores_in(c)
                join_cores(c)
                cores_out(c)

            def cores_straight(c):
                cores(c)
                for what in range(2):
                    go(fin_straight, c, what)

            def hop(c):
                hop_in(c)
                join_hop(c)
                hop_out(c)

            def last(c):
                last_in(c)
                join_last(c)

            def last_straight(c):
                last_in(c)
                hop_in(c)
                join_straight(c)

            stage(t, joins[1][0], cores, stop=relayed)
            stage(t, joins[1][0], cores_straight, start=relayed)
            stage(t, joins[0][0], hop, stop=relayed)
            stage(t, final, last, stop=relayed)
            stage(t, final, last_straight, start=relayed)

        return carry

    lengths.wait()
    lax.fori_loop(0, chunks + final, step, 0)
    for c in range(max(chunks - SENDS, 0), chunks):
        c = jnp.int32(c)
        for kind in range(5):
            q_copy(c, kind).wait_send()
        part_twin(c).wait_send()
        for what in range(2):
            hop_copy(c, what).wait_send()
            for kind in range(2):
                fin_copy(c, kind, what).wait_send()


def solution(mesh):
    group = mesh.shape['dcp']
    chips = group // CORES

    def local_step(q_blk, kv_blk, len_blk):
        batch, tokens, heads, width = q_blk.shape
        rounds = kv_blk.shape[1]
        keys = rounds * PAGE
        rows = tokens * heads
        chunks = batch // CHUNK
        block = CHUNK * rows
        side = chips * rows
        bf, f32 = jnp.bfloat16, jnp.float32
        scratch = [
            pltpu.VMEM((chunks, CHUNK, rows, width), bf),
            pltpu.VMEM((chunks, group, 2, CHUNK // 2 * rows * width // LANES, LANES), bf),
            pltpu.VMEM((KV_SLOTS, CHUNK, keys, width), bf),
            pltpu.VMEM((rows, keys), jnp.int32),
            pltpu.VMEM((KEPT, CHUNK, side, LATENT + LANES), f32),
            pltpu.VMEM((chunks, CHUNK, side, LATENT + LANES), f32),
            pltpu.VMEM((chunks + 1, CHUNK, side, LATENT + LANES), f32),
            pltpu.VMEM((chunks + 1, chips, block, LATENT), bf),
            pltpu.VMEM((chunks + 1, chips * block // LANES, 1, LANES), f32),
            pltpu.VMEM((chunks + 1, block, LATENT), bf),
            pltpu.VMEM((chunks + 1, 1, LANES), f32),
            pltpu.VMEM((chunks + 1, block, LATENT), bf),
            pltpu.VMEM((chunks + 1, 1, LANES), f32),
            pltpu.VMEM((chunks + 1, 2, block, LATENT), bf),
            pltpu.VMEM((chunks + 1, 2, 1, LANES), f32),
            pltpu.VMEM((3, LATENT, keys // 2), bf),
            pltpu.SMEM((batch,), jnp.int32),
            pltpu.SemaphoreType.DMA,
            pltpu.SemaphoreType.DMA,
            pltpu.SemaphoreType.DMA((KV_SLOTS, CHUNK)),
        ]
        for shape in ((5,), (), (2,), (2, 2)):
            scratch += [pltpu.SemaphoreType.DMA((SENDS, *shape)), pltpu.SemaphoreType.DMA((chunks, *shape))]
        flops = 2 * batch * group * rows * keys * (width + LATENT)
        o = pl.pallas_call(
            functools.partial(kernel, group, rounds // 2 - 1),
            out_shape=jax.ShapeDtypeStruct((chunks, CHUNK, rows, LATENT), bf),
            in_specs=[pl.BlockSpec(memory_space=pltpu.HBM)] * 3,
            out_specs=pl.BlockSpec(memory_space=pltpu.VMEM),
            scratch_shapes=scratch,
            compiler_params=pltpu.CompilerParams(collective_id=0, has_side_effects=True, vmem_limit_bytes=50 * 2**20),
            cost_estimate=pl.CostEstimate(flops=flops, bytes_accessed=kv_blk.size * 2, transcendentals=batch * group * rows * keys),
        )(pltpu.with_memory_space_constraint(len_blk, pltpu.HBM), pltpu.with_memory_space_constraint(q_blk.reshape(chunks, CHUNK, rows, width), pltpu.HBM), kv_blk.reshape(batch, keys, width))
        return o.reshape(batch, tokens, heads, LATENT)

    return jax.shard_map(local_step, mesh=mesh, in_specs=(P('dp', None, 'dcp', None), P('dp', None, 'dcp', None, None), P('dp')), out_specs=P('dp', None, 'dcp', None), check_vma=False)
```

```python
import functools
import math

import jax
import jax.numpy as jnp
from jax import lax
from jax.experimental import pallas as pl
from jax.experimental.pallas import tpu as pltpu
from jax.sharding import PartitionSpec as P

LATENT = 512
ROPE = 64
NOPE = 128
PAGE = 64
TOKENS = 2
CORES = 2
CHUNK = 4
KV_SLOTS = 3
AHEAD = 2
KEPT = 3
SENDS = 4
LANES = 128


def wide(col, n):
    return jnp.concatenate([col] * (n // LANES), axis=1)


def merge(o_a, l_a, o_b, l_b):
    top = jnp.maximum(l_a, l_b)
    e_a = jnp.exp(l_a - top)
    e_b = jnp.exp(l_b - top)
    total = e_a + e_b
    inv = 1.0 / total
    n = o_a.shape[1]
    return o_a * wide(e_a * inv, n) + o_b * wide(e_b * inv, n), top + jnp.log(total)


def kernel(group, min_rounds, len_hbm, q_hbm, kv_hbm, out_ref, q_raw, q_all, kv_buf, rank, own, sib, got, chip_o, chip_l, hop_o, hop_l, mid_o, mid_l, fin_o, fin_l,
           turned, len_ref, load_sem, len_sem, kv_sem, q_send, q_recv, s_send, s_recv, h_send, h_recv, f_send, f_recv):
    chunks, per, rows, width = q_raw.shape
    half = per // 2
    heads = rows // TOKENS
    tiles = LATENT // LANES
    keys = kv_buf.shape[2]
    chips = group // CORES
    side = chips * rows
    block = per * rows
    lot = LANES // block
    me = lax.axis_index('dcp')
    chip, core = me // CORES, me % CORES
    right = lax.rem(chip + 1, chips) * CORES + core
    left = lax.rem(chip + chips - 1, chips) * CORES + core
    twin = chip * CORES + (CORES - 1 - core)
    scale = (NOPE + ROPE) ** -0.5

    def remote(src, dst, send, recv, to):
        return pltpu.make_async_remote_copy(src_ref=src, dst_ref=dst, send_sem=send, recv_sem=recv,
                                            device_id={'dcp': to}, device_id_type=pl.DeviceIdType.MESH)

    def way(c):
        return lax.rem(c, 2)

    def toward(d):
        return jnp.where(d == 0, right, left)

    def q_copy(c, kind):
        if kind == 0:
            src, dst, to = q_all.at[c, 0], q_all.at[c, 1], right
        elif kind == 1:
            src, dst, to = q_all.at[c, 0], q_all.at[c, 2], left
        elif kind == 2:
            src, dst, to = q_all.at[c, 1, 0], q_all.at[c, 3, 0], right
        elif kind == 3:
            src, dst, to = q_all.at[c, 2, 1], q_all.at[c, 3, 1], left
        else:
            src, dst, to = q_all.at[c, pl.ds(0, chips)], q_all.at[c, pl.ds(chips, chips)], twin
        return remote(src, dst, q_send.at[lax.rem(c, SENDS), kind], q_recv.at[c, kind], to)

    def part_twin(c):
        return remote(sib.at[c], got.at[c], s_send.at[lax.rem(c, SENDS)], s_recv.at[c], twin)

    def hop_copy(c, what):
        src = (chip_o.at[c, 3], chip_l.at[c, 3 // lot])[what]
        dst = (hop_o.at[c], hop_l.at[c])[what]
        return remote(src, dst, h_send.at[lax.rem(c, SENDS), what], h_recv.at[c, what], toward(way(c)))

    def fin_copy(c, kind, what):
        if kind == 0:
            src, to = (mid_o.at[c], mid_l.at[c])[what], toward(way(c))
        else:
            slot = 1 + way(c)
            src, to = (chip_o.at[c, slot], chip_l.at[c, slot // lot])[what], toward(1 - way(c))
        dst = (fin_o.at[c, kind], fin_l.at[c, kind])[what]
        return remote(src, dst, f_send.at[lax.rem(c, SENDS), kind, what], f_recv.at[c, kind, what], to)

    def kv_copy(c, b):
        slot = lax.rem(c, KV_SLOTS)
        return pltpu.make_async_copy(kv_hbm.at[c * per + b], kv_buf.at[slot, b], kv_sem.at[slot])

    def go(make, c, *which):
        @pl.when(c >= SENDS)
        def _():
            make(c - SENDS, *which).wait_send()

        make(c, *which).start()

    def pack(c):
        for b in range(per):
            h, n = b // half, b % half
            for k in range(tiles):
                at = (k * half + n) * rows
                q_all[c, 0, h, at:at + rows] = q_raw[c, b, :, k * LANES:(k + 1) * LANES]
            turn = q_raw[c, b, :, LATENT:].astype(jnp.float32)
            at = tiles * half * rows + n * heads
            both = jnp.concatenate([turn[t * heads:(t + 1) * heads] for t in range(TOKENS)], axis=1)
            q_all[c, 0, h, at:at + heads] = both.astype(jnp.bfloat16)

    def send_own(c):
        for kind in (0, 1):
            go(q_copy, c, kind)

    load = pltpu.make_async_copy(q_hbm, q_raw, load_sem)
    load.start()
    lengths = pltpu.make_async_copy(len_hbm, len_ref, len_sem)
    lengths.start()
    barrier = pltpu.get_barrier_semaphore()
    for peer in (left, right, twin):
        pl.semaphore_signal(barrier, inc=1, device_id={'dcp': peer}, device_id_type=pl.DeviceIdType.MESH)

    r_id = lax.broadcasted_iota(jnp.int32, (rows, keys), 0)
    k_id = lax.broadcasted_iota(jnp.int32, (rows, keys), 1)
    rank[...] = (k_id // PAGE * group + me) * PAGE + k_id % PAGE - r_id // heads

    load.wait()
    for c in range(min(AHEAD, chunks)):
        pack(c)
    pl.semaphore_wait(barrier, 3)
    for c in range(min(AHEAD, chunks)):
        send_own(jnp.int32(c))
    for c in range(min(KV_SLOTS, chunks)):
        for b in range(per):
            kv_copy(c, b).start()
    for c in range(min(AHEAD, chunks), chunks):
        pack(c)

    free_keys = (min_rounds * PAGE) // LANES * LANES

    def scores(c, b):
        h, n = b // half, b % half
        latent = [q_all[c, :, h, (k * half + n) * rows:(k * half + n + 1) * rows] for k in range(tiles)]
        latent = jnp.concatenate([x.reshape(group * rows, LANES) for x in latent], axis=1)
        at = tiles * half * rows + n * heads
        both = q_all[c, :, h, at:at + heads].astype(jnp.float32).reshape(group * heads, LANES)
        turn = jnp.stack([both.reshape(group, heads, LANES), pltpu.roll(both, ROPE, 1).reshape(group, heads, LANES)], axis=1)
        turn = turn.reshape(group * rows, LANES).astype(jnp.bfloat16)[:, :ROPE]
        kv = kv_buf.at[lax.rem(c, KV_SLOTS), b]
        over = (((1,), (1,)), ((), ()))
        flat = keys - turned.shape[2]
        turned[b % 3] = kv[flat:, :LATENT].T
        s = lax.dot_general(latent, kv[:flat, :LATENT], over, preferred_element_type=jnp.float32)
        s2 = jnp.dot(latent, turned[b % 3], preferred_element_type=jnp.float32)
        s = jnp.concatenate([s, s2], axis=1)
        s = s + lax.dot_general(turn, kv[:, LATENT:], over, preferred_element_type=jnp.float32)
        tail = s[:, free_keys:].reshape(group, rows, keys - free_keys)
        limit = len_ref[c * per + b] - TOKENS
        seen = jnp.broadcast_to(rank[:, free_keys:][None], tail.shape) <= limit
        tail = jnp.where(seen, tail, -jnp.inf).reshape(group * rows, keys - free_keys)
        return jnp.concatenate([s[:, :free_keys], tail], axis=1)

    def values(c, b, s):
        top = jnp.max(s, axis=1, keepdims=True)
        p = jnp.exp2((s - top) * (scale * math.log2(math.e)))
        total = jnp.sum(p, axis=1, keepdims=True)
        o = jnp.dot(p.astype(jnp.bfloat16), kv_buf[lax.rem(c, KV_SLOTS), b, :, :LATENT], preferred_element_type=jnp.float32)
        o = o * (1.0 / total)
        lse = jnp.broadcast_to(top * scale + jnp.log(total), (group * rows, LANES))
        keep = lax.rem(c, KEPT)
        own[keep, b, :, :LATENT] = o[:side]
        own[keep, b, :, LATENT:] = lse[:side]
        sib[c, b, :, :LATENT] = o[side:]
        sib[c, b, :, LATENT:] = lse[side:]

    def attend(c):
        queue = [scores(c, 0), scores(c, 1)]
        for b in range(per):
            if b + 2 < per:
                queue.append(scores(c, b + 2))
            values(c, b, queue[b])

    lane_s = lax.broadcasted_iota(jnp.int32, (lot * rows, LANES), 1)
    row_s = lax.broadcasted_iota(jnp.int32, (lot * rows, LANES), 0)
    lane_b = lax.broadcasted_iota(jnp.int32, (block, LANES), 1)
    row_b = lax.broadcasted_iota(jnp.int32, (block, LANES), 0)

    def column(row, slot):
        picked = jnp.where(lane_b == row_b + lax.rem(slot, lot) * block, jnp.broadcast_to(row, (block, LANES)), 0.0)
        return jnp.broadcast_to(jnp.sum(picked, axis=1, keepdims=True), (block, LANES))

    def join_cores(c):
        packed = [jnp.zeros((1, LANES), jnp.float32) for _ in range(chips // lot)]
        keep = lax.rem(c, KEPT)
        for b in range(per):
            o, lse = merge(own[keep, b, :, :LATENT], own[keep, b, :, LATENT:], got[c, b, :, :LATENT], got[c, b, :, LATENT:])
            o = o.astype(jnp.bfloat16)
            for slot in range(chips):
                chip_o[c, slot, b * rows:(b + 1) * rows] = o[slot * rows:(slot + 1) * rows]
            at = row_s // rows * block + b * rows + row_s % rows
            for j in range(chips // lot):
                part = lse[j * lot * rows:(j + 1) * lot * rows]
                packed[j] = packed[j] + jnp.sum(jnp.where(lane_s == at, part, 0.0), axis=0, keepdims=True)
        for j in range(chips // lot):
            chip_l[c, j] = packed[j]

    def join_hop(c):
        slot = 2 - way(c)
        o, lse = merge(chip_o[c, slot].astype(jnp.float32), column(chip_l[c, slot // lot], slot),
                       hop_o[c].astype(jnp.float32), column(hop_l[c], jnp.int32(3)))
        mid_o[c] = o.astype(jnp.bfloat16)
        mid_l[c] = jnp.sum(jnp.where(lane_b == row_b, lse, 0.0), axis=0, keepdims=True)

    def finish(c, parts):
        top = functools.reduce(jnp.maximum, [l for _, l in parts])
        weights = [jnp.exp(l - top) for _, l in parts]
        inv = 1.0 / functools.reduce(jnp.add, weights)
        o = functools.reduce(jnp.add, [part.astype(jnp.float32) * wide(w * inv, LATENT) for (part, _), w in zip(parts, weights)])
        o = o.astype(jnp.bfloat16)
        for b in range(per):
            out_ref[c, b] = o[b * rows:(b + 1) * rows]

    def join_last(c):
        finish(c, [(chip_o[c, 0], column(chip_l[c, 0], jnp.int32(0))), (fin_o[c, 0], column(fin_l[c, 0], jnp.int32(0))),
                   (fin_o[c, 1], column(fin_l[c, 1], 1 + way(c)))])

    def stage(t, lag, fn):
        c = t - lag

        @pl.when(jnp.logical_and(c >= 0, c < chunks))
        def _():
            fn(c)

    def spread(c):
        for kind in (0, 1):
            q_copy(c, kind).wait_recv()
        for kind in (2, 3):
            go(q_copy, c, kind)

    def to_twin(c):
        for kind in (2, 3):
            q_copy(c, kind).wait_recv()
        go(q_copy, c, 4)

    def cores_in(c):
        part_twin(c).wait_recv()

    def cores_out(c):
        for what in range(2):
            go(hop_copy, c, what)
            go(fin_copy, c, 1, what)

    def hop_in(c):
        for what in range(2):
            hop_copy(c, what).wait_recv()

    def hop_out(c):
        for what in range(2):
            go(fin_copy, c, 0, what)

    def last_in(c):
        for what in range(2):
            for kind in range(2):
                fin_copy(c, kind, what).wait_recv()

    lag = 3
    joins = ((8, hop_in, join_hop, hop_out), (5, cores_in, join_cores, cores_out))
    final = max(chunks + lag, joins[0][0] + 3)

    def step(t, carry):
        stage(t, -AHEAD, send_own)
        stage(t, 0, spread)
        stage(t, 2, to_twin)
        c = t - lag
        busy = jnp.logical_and(c >= 0, c < chunks)

        @pl.when(busy)
        def _():
            for late, ready, _, _ in joins:
                stage(t, late, ready)
            q_copy(c, 4).wait_recv()
            slot = lax.rem(c, KV_SLOTS)
            pltpu.make_async_copy(kv_hbm.at[pl.ds(c * per, per)], kv_buf.at[slot], kv_sem.at[slot]).wait()
            for late, _, join, _ in joins:
                old = t - late
                join(jnp.where(old >= 0, old, chunks))
            attend(c)
            go(part_twin, c)
            for late, _, _, pass_on in joins:
                stage(t, late, pass_on)

            @pl.when(c + KV_SLOTS < chunks)
            def _():
                for b in range(per):
                    kv_copy(c + KV_SLOTS, b).start()

        @pl.when(jnp.logical_not(busy))
        def _():
            def cores(c):
                cores_in(c)
                join_cores(c)
                cores_out(c)

            def hop(c):
                hop_in(c)
                join_hop(c)
                hop_out(c)

            def last(c):
                last_in(c)
                join_last(c)

            stage(t, joins[1][0], cores)
            stage(t, joins[0][0], hop)
            stage(t, final, last)

        return carry

    lengths.wait()
    lax.fori_loop(0, chunks + final, step, 0)
    for c in range(max(chunks - SENDS, 0), chunks):
        c = jnp.int32(c)
        for kind in range(5):
            q_copy(c, kind).wait_send()
        part_twin(c).wait_send()
        for what in range(2):
            hop_copy(c, what).wait_send()
            for kind in range(2):
                fin_copy(c, kind, what).wait_send()


def solution(mesh):
    group = mesh.shape['dcp']
    chips = group // CORES

    def local_step(q_blk, kv_blk, len_blk):
        batch, tokens, heads, width = q_blk.shape
        rounds = kv_blk.shape[1]
        keys = rounds * PAGE
        rows = tokens * heads
        chunks = batch // CHUNK
        block = CHUNK * rows
        side = chips * rows
        bf, f32 = jnp.bfloat16, jnp.float32
        scratch = [
            pltpu.VMEM((chunks, CHUNK, rows, width), bf),
            pltpu.VMEM((chunks, group, 2, CHUNK // 2 * rows * width // LANES, LANES), bf),
            pltpu.VMEM((KV_SLOTS, CHUNK, keys, width), bf),
            pltpu.VMEM((rows, keys), jnp.int32),
            pltpu.VMEM((KEPT, CHUNK, side, LATENT + LANES), f32),
            pltpu.VMEM((chunks, CHUNK, side, LATENT + LANES), f32),
            pltpu.VMEM((chunks + 1, CHUNK, side, LATENT + LANES), f32),
            pltpu.VMEM((chunks + 1, chips, block, LATENT), bf),
            pltpu.VMEM((chunks + 1, chips * block // LANES, 1, LANES), f32),
            pltpu.VMEM((chunks + 1, block, LATENT), bf),
            pltpu.VMEM((chunks + 1, 1, LANES), f32),
            pltpu.VMEM((chunks + 1, block, LATENT), bf),
            pltpu.VMEM((chunks + 1, 1, LANES), f32),
            pltpu.VMEM((chunks + 1, 2, block, LATENT), bf),
            pltpu.VMEM((chunks + 1, 2, 1, LANES), f32),
            pltpu.VMEM((3, LATENT, keys // 2), bf),
            pltpu.SMEM((batch,), jnp.int32),
            pltpu.SemaphoreType.DMA,
            pltpu.SemaphoreType.DMA,
            pltpu.SemaphoreType.DMA((KV_SLOTS,)),
        ]
        for shape in ((5,), (), (2,), (2, 2)):
            scratch += [pltpu.SemaphoreType.DMA((SENDS, *shape)), pltpu.SemaphoreType.DMA((chunks, *shape))]
        flops = 2 * batch * group * rows * keys * (width + LATENT)
        o = pl.pallas_call(
            functools.partial(kernel, group, rounds // 2 - 1),
            out_shape=jax.ShapeDtypeStruct((chunks, CHUNK, rows, LATENT), bf),
            in_specs=[pl.BlockSpec(memory_space=pltpu.HBM)] * 3,
            out_specs=pl.BlockSpec(memory_space=pltpu.VMEM),
            scratch_shapes=scratch,
            compiler_params=pltpu.CompilerParams(collective_id=0, has_side_effects=True, vmem_limit_bytes=50 * 2**20),
            cost_estimate=pl.CostEstimate(flops=flops, bytes_accessed=kv_blk.size * 2, transcendentals=batch * group * rows * keys),
        )(pltpu.with_memory_space_constraint(len_blk, pltpu.HBM), pltpu.with_memory_space_constraint(q_blk.reshape(chunks, CHUNK, rows, width), pltpu.HBM), kv_blk.reshape(batch, keys, width))
        return o.reshape(batch, tokens, heads, LATENT)

    return jax.shard_map(local_step, mesh=mesh, in_specs=(P('dp', None, 'dcp', None), P('dp', None, 'dcp', None, None), P('dp')), out_specs=P('dp', None, 'dcp', None), check_vma=False)
```
